128 devices in a mesh: seq: 16 (over z_hi, y, core), tensor: 8 (over z_lo, x).
Axes of the slice: x: 4, y: 4, z: 4 (z_hi: 2, z_lo: 2; z = z_hi * 2 + z_lo), core: 2. Of those that a mesh axis runs over, the one named last changes fastest.
Arguments:
- tokens: bfloat16 [11520, 1536], P('seq'), may hold values from -6 to 6
- norm_gain: float32 [1536], replicated, may hold values from 0.1 to 1.9
- w_qkv: bfloat16 [1536, 3, 1536], P(None, None, 'tensor'), may hold values from -8 to 8
- w_out: bfloat16 [1536, 1536], P('tensor'), may hold values from -0.15625 to 0.15625
- post_gain: float32 [1536], replicated, may hold values from 0.1 to 1.9
- w_up: bfloat16 [1536, 6144], P(None, 'tensor'), may hold values from -0.15625 to 0.15625
- w_down: bfloat16 [6144, 1536], P('tensor'), may hold values from -0.078125 to 0.078125
Outputs:
- layer_out: bfloat16 [11520, 1536], P('seq')
The draws below stay inside these ranges and needn't reach their ends.
All inputs are finite; a program needn't handle non-finite values.
Results may differ from the reference program's by a relative error of at most 0.015.
Values may be sent and summed in bfloat16 or wider, within the bound.
A program may use at most 128 MiB of HBM per device.

```python
import math
import jax
import jax.numpy as jnp
from jax import lax

D = 1536
HEADS = 32
HD = 48
FF = 6144
TOK_DEV = 720
TOKENS = 11520
N_TENSOR = 8


def draw_w_qkv(key, part):
    base = jax.random.normal(key, (D, 3, HEADS * HD), jnp.float32) * D ** (-0.5)
    levels = jax.random.uniform(jax.random.fold_in(key, 3), (HEADS,), jnp.float32, math.log(1.5), math.log(3.5))
    sharpness = jnp.repeat(jnp.exp(levels), HD)
    query = base[:, 0, :] * sharpness[None, :]
    stacked = jnp.stack([query, base[:, 1, :], base[:, 2, :]], axis=1)
    return jnp.clip(stacked, -8.0, 8.0).astype(jnp.bfloat16)


def level_of(stream_key, shape, cuts, least, top_value):
    def one(dim, parts):
        steps = jax.random.uniform(jax.random.fold_in(jax.random.fold_in(stream_key, 6), dim), (parts,), jnp.float32, least / len(cuts), top_value / len(cuts))
        return jnp.repeat(jnp.exp(steps), shape[dim] // parts).reshape((-1,) + (1,) * (len(shape) - dim - 1))

    level = one(*cuts[0])
    for cut in cuts[1:]:
        level = level * one(*cut)
    return level


def scatter_about(rng, extent, scale, bound, split=(), dtype=jnp.bfloat16):
    loudness = level_of(rng, extent, split, -0.22, 0.18) if split else 1.0
    array = jax.random.normal(rng, extent, jnp.float32) * scale * loudness
    return jnp.minimum(jnp.maximum(array, -bound), bound).astype(dtype)


def setup_inputs(seed: int = 0) -> dict:
    key_list = jax.random.split(jax.random.key(seed), 8)
    return {
        "tokens": scatter_about(key_list[0], (TOKENS, D), 1.0, 6.0, ((0, 16),)),
        "norm_gain": jnp.clip(1.0 + 0.18 * jax.random.normal(key_list[1], (D,), jnp.float32), 0.1, 1.9),
        "w_qkv": draw_w_qkv(jax.random.fold_in(key_list[7], 71), 0),
        "w_out": scatter_about(key_list[3], (HEADS * HD, D), (HEADS * HD) ** -0.5, 0.15625, ((0, 8),)),
        "post_gain": jnp.clip(1.0 + 0.18 * jax.random.normal(key_list[4], (D,), jnp.float32), 0.1, 1.9),
        "w_up": scatter_about(key_list[5], (D, FF), D ** -0.5, 0.15625, ((1, 8),)),
        "w_down": scatter_about(key_list[6], (FF, D), FF ** -0.5, 0.078125, ((0, 8),)),
    }


def layer_norm(values, gain):
    mean = lax.optimization_barrier(jnp.mean(values, axis=-1, keepdims=True))
    centred = values - mean
    var = lax.optimization_barrier(jnp.mean(centred * centred, axis=-1, keepdims=True))
    return centred * lax.rsqrt(var + 1e-05) * gain

def one_head(operands):
    query, key, value = operands
    scale = 1.0 / HD ** 0.5

    def block(query_block):
        scores = jnp.dot(query_block, key.T, preferred_element_type=jnp.float32) * scale
        peak = lax.optimization_barrier(jnp.max(scores, axis=-1, keepdims=True))
        weights = jnp.exp(scores - peak)
        total = lax.optimization_barrier(jnp.sum(weights, axis=-1, keepdims=True))
        return jnp.dot(weights.astype(jnp.bfloat16), value, preferred_element_type=jnp.float32) / total
    blocks = query.reshape(TOKENS // TOK_DEV, TOK_DEV, HD)
    return lax.map(block, blocks).reshape(TOKENS, HD)

def grouped_sum(left, right):
    width = left.shape[1] // N_TENSOR
    result = jnp.zeros((left.shape[0], right.shape[1]), jnp.float32)
    for group in range(N_TENSOR):
        term = jnp.dot(left[:, group * width:(group + 1) * width], right[group * width:(group + 1) * width], preferred_element_type=jnp.float32)
        term = lax.optimization_barrier(term.astype(jnp.bfloat16))
        result = result + term.astype(jnp.float32)
    return result

def reference(tokens, norm_gain, w_qkv, w_out, post_gain, w_up, w_down):
    base = tokens.astype(jnp.float32)
    normed = layer_norm(base, norm_gain).astype(jnp.bfloat16)
    qkv = jnp.dot(normed, w_qkv.reshape(D, 3 * HEADS * HD), preferred_element_type=jnp.float32).astype(jnp.bfloat16)
    qkv = qkv.reshape(TOKENS, 3, HEADS, HD)
    query = jnp.transpose(qkv[:, 0], (1, 0, 2))
    key = jnp.transpose(qkv[:, 1], (1, 0, 2))
    value = jnp.transpose(qkv[:, 2], (1, 0, 2))
    heads = lax.map(one_head, (query, key, value))
    attended = jnp.transpose(heads, (1, 0, 2)).reshape(TOKENS, HEADS * HD).astype(jnp.bfloat16)
    mixed = base + grouped_sum(attended, w_out)
    post = layer_norm(mixed, post_gain).astype(jnp.bfloat16)
    hidden = jax.nn.gelu(jnp.dot(post, w_up, preferred_element_type=jnp.float32), approximate=True).astype(jnp.bfloat16)
    return (mixed + grouped_sum(hidden, w_down)).astype(jnp.bfloat16)
```

```python
import jax
import jax.numpy as jnp
from jax import lax
from jax.experimental import pallas as pl
from jax.experimental.pallas import tpu as pltpu
from jax.sharding import PartitionSpec as P

HD = 48
PAD = 768
WIDE = 1024
MESH = pl.DeviceIdType.MESH
LOG2E = 1.4426950408889634
LIMIT = 2.0**90
FLOOR = 2.0**-20
FULL = pl.BlockSpec(memory_space=pltpu.VMEM)


def layer_norm(values, gain):
    mean = jnp.mean(values, axis=-1, keepdims=True)
    centred = values - mean
    var = jnp.mean(centred * centred, axis=-1, keepdims=True)
    return centred * lax.rsqrt(var + 1e-05) * gain


def load_blocks(rows, refs, keys, vals):
    lane = lax.broadcasted_iota(jnp.int32, (16, PAD), 1)
    sub = lax.broadcasted_iota(jnp.int32, (16, PAD), 0)
    count = ((sub == 0) & (lane < rows)).astype(jnp.float32).astype(jnp.bfloat16)
    shift = (sub == 0).astype(jnp.float32).astype(jnp.bfloat16)
    zeros = jnp.zeros((64, PAD), jnp.bfloat16)
    for g, ref in enumerate(refs):

        def one(j, _, g=g, ref=ref):
            full = jnp.concatenate([ref[j, 0], shift, zeros], axis=0)
            keys[g * 4 + j] = full.T
            vals[g * 4 + j, 0:HD] = ref[j, 1]
            vals[g * 4 + j, HD : HD + 16] = count
            return 0

        lax.fori_loop(0, 4, one, 0)


def sweep(rows, blocks, queries, keys, vals, acc, probs, unroll):
    chunks = queries.shape[1] // WIDE
    total = blocks * chunks

    def place(i):
        return i // chunks, pl.ds(pl.multiple_of(lax.rem(i, chunks) * WIDE, WIDE), WIDE)

    def scores(i, slot):
        b, cols = place(i)
        s = jnp.dot(keys[b, 0:rows], queries[:, cols], preferred_element_type=jnp.float32)
        probs[slot, 0:rows, :] = jnp.exp2(s).astype(jnp.bfloat16)

    def product(i, slot):
        b, cols = place(i)
        acc[:, cols] += jnp.dot(vals[b], probs[slot], preferred_element_type=jnp.float32)

    scores(0, 0)

    def body(j, _):
        for u in range(unroll):
            i = unroll * j + u
            ahead = i + 1 if u < unroll - 1 else jnp.minimum(i + 1, total - 1)
            scores(ahead, (u + 1) % 2)
            product(i, u % 2)
        return 0

    lax.fori_loop(0, total // unroll, body, 0)


def fill_queries(q_ref, queries):
    queries[HD:128, :] = jnp.zeros((128 - HD, queries.shape[1]), jnp.bfloat16)
    for d in range(4):
        queries[0:HD, d * PAD : (d + 1) * PAD] = q_ref[d]


def set_shift(queries, peak):
    width = queries.shape[1]
    first = lax.broadcasted_iota(jnp.int32, (16, width), 0) == 0
    rows = jnp.where(first, jnp.broadcast_to(-peak, (16, width)), 0.0)
    queries[HD : HD + 16, :] = rows.astype(jnp.bfloat16)


def attend_first(rows, q_ref, own, core, acc, peak_ref, queries, keys, vals, probs):
    width = queries.shape[1]
    fill_queries(q_ref, queries)
    load_blocks(rows, (own, core), keys, vals)
    acc[...] = jnp.zeros_like(acc)
    probs[:, rows:PAD, :] = jnp.zeros((2, PAD - rows, WIDE), jnp.bfloat16)
    for c in range(width // WIDE):
        cols = slice(c * WIDE, (c + 1) * WIDE)
        s = jnp.dot(keys[0, 0:rows], queries[:, cols], preferred_element_type=jnp.float32)
        top = jnp.max(s.reshape(rows // 8, 8, WIDE), axis=0)
        top = jnp.max(top, axis=0, keepdims=True)
        peak_ref[:, cols] = jnp.broadcast_to(top, (8, WIDE))
    set_shift(queries, peak_ref[0:1, :])
    sweep(rows, 8, queries, keys, vals, acc, probs, 6)


def attend_rest(rows, q_ref, own, core, far, farcore, acc_in, peak_in, o_ref, queries, keys, vals, probs, acc):
    width = queries.shape[1]
    fill_queries(q_ref, queries)
    load_blocks(rows, (far, farcore), keys, vals)
    probs[:, rows:PAD, :] = jnp.zeros((2, PAD - rows, WIDE), jnp.bfloat16)
    acc[...] = acc_in[...]
    set_shift(queries, peak_in[0:1, :])
    sweep(rows, 8, queries, keys, vals, acc, probs, 6)

    total = acc[HD : HD + 1, :]
    fits = jnp.where((total < LIMIT) & (total > FLOOR), 0.0, 1.0)

    @pl.when(jnp.max(fits) > 0.5)
    def _():
        set_shift(queries, jnp.zeros((1, width), jnp.float32))
        acc[...] = jnp.zeros_like(acc)
        for group in ((own, core), (far, farcore)):
            load_blocks(rows, group, keys, vals)
            first_group = group[0] is own

            def chunk(c, _):
                cols = pl.ds(pl.multiple_of(c * 256, 256), 256)

                def block(b, carry):
                    peak, sums = carry
                    s = jnp.dot(keys[b, 0:rows], queries[:, cols], preferred_element_type=jnp.float32)
                    fresh = jnp.maximum(peak, jnp.max(s, axis=0, keepdims=True))
                    probs[0, 0:rows, 0:256] = jnp.exp2(s - fresh).astype(jnp.bfloat16)
                    part = jnp.dot(vals[b], probs[0, :, 0:256], preferred_element_type=jnp.float32)
                    return fresh, sums * jnp.exp2(peak - fresh) + part

                if first_group:
                    start = jnp.full((1, 256), -1e30, jnp.float32)
                else:
                    start = acc[HD + 8 : HD + 9, cols]
                peak, sums = lax.fori_loop(0, 8, block, (start, acc[:, cols]))
                acc[:, cols] = sums
                acc[HD + 8 : HD + 9, cols] = peak
                return 0

            lax.fori_loop(0, width // 256, chunk, 0)

    for d in range(4):
        cols = slice(d * PAD, (d + 1) * PAD)
        o_ref[d] = (acc[0:HD, cols] / acc[HD : HD + 1, cols]).astype(jnp.bfloat16)


def attention(rows, q, own, core, far, farcore):
    import functools

    width = 4 * PAD
    scratch = [
        pltpu.VMEM((128, width), jnp.bfloat16),
        pltpu.VMEM((8, PAD, 128), jnp.bfloat16),
        pltpu.VMEM((8, HD + 16, PAD), jnp.bfloat16),
        pltpu.VMEM((2, PAD, WIDE), jnp.bfloat16),
    ]
    cost = pl.CostEstimate(flops=8 * 4 * PAD * PAD * 128 * 4, bytes_accessed=2**22, transcendentals=8 * 4 * PAD * PAD)
    acc, peak = pl.pallas_call(
        functools.partial(attend_first, rows),
        out_shape=(
            jax.ShapeDtypeStruct((HD + 16, width), jnp.float32),
            jax.ShapeDtypeStruct((8, width), jnp.float32),
        ),
        in_specs=[FULL] * 3,
        out_specs=(FULL, FULL),
        scratch_shapes=scratch,
        cost_estimate=cost,
        compiler_params=pltpu.CompilerParams(vmem_limit_bytes=40 * 2**20),
        name="attend_first",
    )(q, own, core)
    return pl.pallas_call(
        functools.partial(attend_rest, rows),
        out_shape=jax.ShapeDtypeStruct((4, HD, PAD), jnp.bfloat16),
        in_specs=[FULL] * 7,
        out_specs=FULL,
        scratch_shapes=scratch + [pltpu.VMEM((HD + 16, width), jnp.float32)],
        cost_estimate=cost,
        compiler_params=pltpu.CompilerParams(vmem_limit_bytes=40 * 2**20),
        name="attend_rest",
    )(q, own, core, far, farcore, acc, peak)


class Links:
    def __init__(self, send, recv):
        me = lax.axis_index("tensor")
        self.seq = lax.axis_index("seq")
        self.z, self.x = me // 4, lax.rem(me, 4)
        self.me = me
        self.send, self.recv = send, recv
        self.count = 0
        self.open = []

    def slot(self, dz, dx):
        z = lax.rem(self.z + dz, 2)
        return z * 4 + lax.rem(self.x + dx, 4)

    def barrier(self):
        sem = pltpu.get_barrier_semaphore()
        for dz, dx in ((1, 0), (0, 1), (0, 3)):
            pl.semaphore_signal(sem, inc=1, device_id=(self.seq, self.slot(dz, dx)), device_id_type=MESH)
        pl.semaphore_wait(sem, 3)

    def put(self, src, dst, dz, dx):
        i = self.count
        self.count += 1
        copy = pltpu.make_async_remote_copy(
            src_ref=src,
            dst_ref=dst,
            send_sem=self.send.at[i],
            recv_sem=self.recv.at[i],
            device_id=(self.seq, self.slot(dz, dx)),
            device_id_type=MESH,
        )
        copy.start()
        self.open.append(copy)
        return copy

    def drain(self):
        for copy in self.open:
            copy.wait_send()
        self.open = []


def gather_tensor(links, piece):
    s = links.slot
    put = links.put

    def pass_on(slot, lo, hi, dz, dx):
        ref = piece(slot, lo, hi)
        return put(ref, ref, dz, dx)

    me = s(0, 0)
    a_z = pass_on(me, 0, 2, 1, 0)
    b_up = pass_on(me, 2, 4, 0, 1)
    b_down = pass_on(me, 2, 4, 0, 3)
    b_z = pass_on(me, 2, 4, 1, 0)
    a_up = pass_on(me, 0, 2, 0, 1)
    a_down = pass_on(me, 0, 2, 0, 3)
    b_up.wait_recv()
    r2 = pass_on(s(0, 3), 2, 3, 0, 1)
    bz_lo = pass_on(s(0, 3), 2, 4, 1, 0)
    b_down.wait_recv()
    r3 = pass_on(s(0, 1), 3, 4, 0, 3)
    bz_hi = pass_on(s(0, 1), 2, 4, 1, 0)
    a_z.wait_recv()
    az_up = pass_on(s(1, 0), 0, 2, 0, 1)
    az_down = pass_on(s(1, 0), 0, 2, 0, 3)
    a_up.wait_recv()
    r0 = pass_on(s(0, 3), 0, 1, 0, 1)
    a_down.wait_recv()
    r1 = pass_on(s(0, 1), 1, 2, 0, 3)
    r2.wait_recv()
    bz_2 = pass_on(s(0, 2), 2, 3, 1, 0)
    r3.wait_recv()
    bz_3 = pass_on(s(0, 2), 3, 4, 1, 0)
    az_up.wait_recv()
    q0 = pass_on(s(1, 3), 0, 1, 0, 1)
    az_down.wait_recv()
    q1 = pass_on(s(1, 1), 1, 2, 0, 3)
    for copy in (b_z, bz_lo, bz_hi, r0, r1, bz_2, bz_3, q0, q1):
        copy.wait_recv()
    links.drain()


GATHER_COPIES = 18


def gather_heads_kernel(block_ref, out_ref, send, recv):
    links = Links(send, recv)
    links.barrier()
    out_ref[links.me] = block_ref[...]
    gather_tensor(links, lambda slot, lo, hi: out_ref.at[slot, lo:hi])


def gather_heads(block):
    return pl.pallas_call(
        gather_heads_kernel,
        out_shape=jax.ShapeDtypeStruct((8,) + block.shape, block.dtype),
        in_specs=[FULL],
        out_specs=FULL,
        scratch_shapes=[pltpu.SemaphoreType.DMA((GATHER_COPIES,)), pltpu.SemaphoreType.DMA((GATHER_COPIES,))],
        compiler_params=pltpu.CompilerParams(collective_id=1, has_side_effects=True, vmem_limit_bytes=32 * 2**20),
        name="gather_heads",
    )(block)


def reduce_tensor(links, term, stage, rows, cols):
    quarter = cols // 4
    s = links.slot
    put = links.put

    def q(slot, lo, hi):
        return term.at[slot, :, lo * quarter : hi * quarter]

    def val(slot, lo, hi):
        return term[slot, :, lo * quarter : hi * quarter].astype(jnp.float32)

    def land(i, n):
        return stage.at[i, :, 0 : n * quarter]

    def got(i, lo, hi):
        return stage[i, :, lo * quarter : hi * quarter].astype(jnp.float32)

    def add_into(slot, lo, hi, *parts):
        total = val(slot, lo, hi)
        for part in parts:
            total = total + part
        term[slot, :, lo * quarter : hi * quarter] = total.astype(jnp.bfloat16)

    zb = {}
    for i, dx in enumerate((2, 1, 3, 0)):
        zb[dx] = put(q(s(1, dx), 2, 4), land(i, 2), 1, 0)
    fa = {}
    for j, dz in enumerate((1, 0)):
        fa[dz, 0] = put(q(s(dz, 2), 0, 1), land(4 + j, 1), 0, 3)
        fa[dz, 1] = put(q(s(dz, 2), 1, 2), land(6 + j, 1), 0, 1)
    near = {}
    for j, dz in enumerate((1, 0)):
        fa[dz, 0].wait_recv()
        add_into(s(dz, 3), 0, 1, got(4 + j, 0, 1))
        near[dz, 3] = put(q(s(dz, 3), 0, 2), land(8 + j, 2), 0, 3)
        fa[dz, 1].wait_recv()
        add_into(s(dz, 1), 1, 2, got(6 + j, 0, 1))
        near[dz, 1] = put(q(s(dz, 1), 0, 2), land(10 + j, 2), 0, 1)
    zb[2].wait_recv()
    add_into(s(0, 2), 2, 4, got(0, 0, 2))
    fb0 = put(q(s(0, 2), 2, 3), land(12, 1), 0, 3)
    fb1 = put(q(s(0, 2), 3, 4), land(13, 1), 0, 1)
    zb[1].wait_recv()
    zb[3].wait_recv()
    near[1, 3].wait_recv()
    near[1, 1].wait_recv()
    add_into(s(1, 0), 0, 2, got(8, 0, 2), got(10, 0, 2))
    za = put(q(s(1, 0), 0, 2), land(14, 2), 1, 0)
    fb0.wait_recv()
    add_into(s(0, 3), 2, 3, got(2, 0, 1), got(12, 0, 1))
    add_into(s(0, 3), 3, 4, got(2, 1, 2))
    nb3 = put(q(s(0, 3), 2, 4), land(15, 2), 0, 3)
    fb1.wait_recv()
    add_into(s(0, 1), 3, 4, got(1, 1, 2), got(13, 0, 1))
    add_into(s(0, 1), 2, 3, got(1, 0, 1))
    nb1 = put(q(s(0, 1), 2, 4), land(16, 2), 0, 1)
    near[0, 3].wait_recv()
    near[0, 1].wait_recv()
    za.wait_recv()
    first = val(s(0, 0), 0, 2) + got(9, 0, 2) + got(11, 0, 2) + got(14, 0, 2)
    zb[0].wait_recv()
    nb3.wait_recv()
    nb1.wait_recv()
    second = val(s(0, 0), 2, 4) + got(3, 0, 2) + got(15, 0, 2) + got(16, 0, 2)
    links.drain()
    return first, second


def finish_kernel(term_in, mixed_ref, out_ref, term, stage, send, recv):
    rows, cols = mixed_ref.shape
    quarter = cols // 4
    links = Links(send, recv)
    links.barrier()
    term[...] = term_in[...]
    first, second = reduce_tensor(links, term, stage, rows, cols)
    out_ref[links.me, :, 0 : 2 * quarter] = (mixed_ref[:, 0 : 2 * quarter] + first).astype(jnp.bfloat16)
    out_ref[links.me, :, 2 * quarter :] = (mixed_ref[:, 2 * quarter :] + second).astype(jnp.bfloat16)
    gather_tensor(links, lambda slot, lo, hi: out_ref.at[slot, :, lo * quarter : hi * quarter])


def finish(term, mixed):
    parts, rows, cols = term.shape
    copies = 40
    return pl.pallas_call(
        finish_kernel,
        out_shape=jax.ShapeDtypeStruct(term.shape, jnp.bfloat16),
        in_specs=[FULL, FULL],
        out_specs=FULL,
        scratch_shapes=[
            pltpu.VMEM(term.shape, jnp.bfloat16),
            pltpu.VMEM((17, rows, cols // 2), jnp.bfloat16),
            pltpu.SemaphoreType.DMA((copies,)),
            pltpu.SemaphoreType.DMA((copies,)),
        ],
        compiler_params=pltpu.CompilerParams(collective_id=2, has_side_effects=True, vmem_limit_bytes=40 * 2**20),
        name="finish",
    )(term, mixed)


def seq_pairs(move):
    pairs = []
    for s in range(16):
        z, y, c = s // 8, (s // 2) % 4, s % 2
        z2, y2, c2 = move(z, y, c)
        pairs.append((s, (z2 * 4 + y2) * 2 + c2))
    return pairs


def shift_y(value, d):
    return lax.ppermute(value, "seq", seq_pairs(lambda z, y, c: (z, (y + d) % 4, c)))


def other_core(value):
    return lax.ppermute(value, "seq", seq_pairs(lambda z, y, c: (z, y, 1 - c)))


def other_z(value):
    return lax.ppermute(value, "seq", seq_pairs(lambda z, y, c: (1 - z, y, c)))


def gather_weight(w, core):
    half = w.shape[0] // 2
    mine = lax.dynamic_slice_in_dim(w, core * half, half, 0)
    found = [mine]
    for d in range(1, 8):
        found.append(lax.ppermute(mine, "tensor", [(t, (t + d) % 8) for t in range(8)]))
    mine_all = jnp.stack(found)
    other = other_core(mine_all)
    t = lax.axis_index("tensor")
    low = jnp.where(core == 0, mine_all, other)
    high = jnp.where(core == 0, other, mine_all)
    both = jnp.stack([low, high], axis=1)
    order = lax.rem(t - jnp.arange(8) + 8, 8)
    return jnp.take(both, order, axis=0).reshape(16 * half, w.shape[1])


def per_device(tokens, norm_gain, w_qkv, w_out, post_gain, w_up, w_down):
    rows, width = tokens.shape
    heads = w_qkv.shape[2] // HD
    seq = lax.axis_index("seq")
    t = lax.axis_index("tensor")
    y, core = lax.rem(seq // 2, 4), lax.rem(seq, 2)
    w_out_all = gather_weight(w_out, core)
    base = tokens.astype(jnp.float32)
    normed = layer_norm(base, norm_gain).astype(jnp.bfloat16)
    qkv = lax.dot_general(w_qkv, normed, (((0,), (1,)), ((), ())), preferred_element_type=jnp.float32)
    factor = jnp.array([LOG2E / HD**0.5, 1.0, 1.0], jnp.float32)[:, None, None]
    qkv = (qkv * factor).astype(jnp.bfloat16)
    qkv = jnp.pad(qkv, ((0, 0), (0, 0), (0, PAD - rows))).reshape(3, heads, HD, PAD)

    def head_for(d):
        return lax.dynamic_index_in_dim(qkv, lax.rem(y + d, 4), 1, keepdims=False)

    parts = [head_for(0)] + [shift_y(head_for(d), d) for d in range(1, 4)]
    both = jnp.stack(parts)
    q = both[:, 0]
    own = both[:, 1:]
    core_kv = other_core(own)
    far = other_z(own)
    far_core = other_core(far)
    o = attention(rows, q, own, core_kv, far, far_core)
    back = [o[0]] + [shift_y(o[d], -d) for d in range(1, 4)]
    attended = jnp.take(jnp.stack(back), lax.rem(jnp.arange(4) - y + 4, 4), axis=0)
    every = gather_heads(attended).reshape(8 * heads * HD, PAD)
    padded = jnp.pad(base, ((0, PAD - rows), (0, 0)))
    mixed = padded + lax.dot_general(
        every, w_out_all, (((0,), (0,)), ((), ())), preferred_element_type=jnp.float32
    )
    post = layer_norm(mixed, post_gain).astype(jnp.bfloat16)
    hidden = jax.nn.gelu(
        jnp.dot(post, w_up, preferred_element_type=jnp.float32), approximate=True
    ).astype(jnp.bfloat16)
    term = jnp.dot(hidden, w_down, preferred_element_type=jnp.float32).astype(jnp.bfloat16)
    share = PAD // 8
    mine = lax.dynamic_slice_in_dim(mixed, t * share, share, 0)
    out = finish(term.reshape(8, share, width), mine)
    return out.reshape(PAD, width)[:rows]


def solution(mesh):
    placed = (
        P("seq", None),
        P(),
        P(None, None, "tensor"),
        P("tensor", None),
        P(),
        P(None, "tensor"),
        P("tensor", None),
    )
    return jax.shard_map(
        per_device, mesh=mesh, in_specs=placed, out_specs=P("seq", None), check_vma=False
    )
```

```python
import functools

import jax
import jax.numpy as jnp
from jax import lax
from jax.experimental import pallas as pl
from jax.experimental.pallas import tpu as pltpu
from jax.sharding import PartitionSpec as P

HD = 48
PAD = 768
WIDE = 1024
MESH = pl.DeviceIdType.MESH
LOG2E = 1.4426950408889634
LIMIT = 2.0**90
FLOOR = 2.0**-20
FULL = pl.BlockSpec(memory_space=pltpu.VMEM)


def layer_norm(values, gain):
    mean = jnp.mean(values, axis=-1, keepdims=True)
    centred = values - mean
    var = jnp.mean(centred * centred, axis=-1, keepdims=True)
    return centred * lax.rsqrt(var + 1e-05) * gain


def sweep(rows, blocks, queries, keys, vals, acc, probs, unroll, stage):
    chunks = queries.shape[1] // WIDE
    total = blocks * chunks

    def place(i):
        return i // chunks, pl.ds(pl.multiple_of(lax.rem(i, chunks) * WIDE, WIDE), WIDE)

    def scores(i, slot):
        b, cols = place(i)
        s = jnp.dot(keys[b, 0:rows], queries[:, cols], preferred_element_type=jnp.float32)
        probs[slot, 0:rows, :] = jnp.exp2(s).astype(jnp.bfloat16)

    def product(i, slot):
        b, cols = place(i)
        acc[:, cols] += jnp.dot(vals[b], probs[slot], preferred_element_type=jnp.float32)

    scores(0, 0)

    def body(j, _):
        for k in range(total // unroll):

            @pl.when(j == k)
            def _(k=k):
                stage(k)

        for u in range(unroll):
            i = unroll * j + u
            ahead = i + 1 if u < unroll - 1 else jnp.minimum(i + 1, total - 1)
            scores(ahead, (u + 1) % 2)
            product(i, u % 2)
        return 0

    lax.fori_loop(0, total // unroll, body, 0)


ORDER = (0, 1, 3, 2)


def load_block(rows, kv, b, keys, vals):
    lane = lax.broadcasted_iota(jnp.int32, (16, PAD), 1)
    sub = lax.broadcasted_iota(jnp.int32, (16, PAD), 0)
    count = ((sub == 0) & (lane < rows)).astype(jnp.float32).astype(jnp.bfloat16)
    shift = (sub == 0).astype(jnp.float32).astype(jnp.bfloat16)
    zeros = jnp.zeros((64, PAD), jnp.bfloat16)
    keys[b] = jnp.concatenate([kv[0], shift, zeros], axis=0).T
    vals[b, 0:HD] = kv[1]
    vals[b, HD : HD + 16] = count


def attend_kernel(rows, qkv, w_ref, acc, land, kvx, w_all, queries, keys, vals, probs, w_own, send, recv, local):
    width = queries.shape[1]
    seq, me = lax.axis_index("seq"), lax.axis_index("tensor")
    z, y, core = seq // 8, lax.rem(seq // 2, 4), lax.rem(seq, 2)
    links = Links(send, recv)

    def on_seq(dz, dy, dc):
        return ((lax.rem(z + dz, 2) * 4 + lax.rem(y + dy, 4)) * 2 + lax.rem(core + dc, 2), me)

    barrier = pltpu.get_barrier_semaphore()
    peers = [on_seq(0, d, 0) for d in (1, 2, 3)] + [on_seq(0, 0, 1), on_seq(1, 0, 0)]
    peers += [(seq, links.slot(1, 0)), (seq, links.slot(0, 1)), (seq, links.slot(0, 3))]
    for peer in peers:
        pl.semaphore_signal(barrier, inc=1, device_id=peer, device_id_type=MESH)
    pl.semaphore_wait(barrier, 8)

    by_y = {}
    for d in (2, 1, 3):
        by_y[d] = links.start(lambda d=d: (qkv.at[:, lax.rem(y + d, 4)], land.at[d], on_seq(0, d, 0)))
    to_core, to_far, far_core = {}, {}, {}
    to_core[0] = links.start(lambda: (qkv.at[1:3, y], kvx.at[0, 0], on_seq(0, 0, 1)))
    to_far[0] = links.start(lambda: (qkv.at[1:3, y], kvx.at[1, 0], on_seq(1, 0, 0)))

    fetch = pltpu.make_async_copy(w_ref, w_own, local.at[0])
    fetch.start()
    land[0] = qkv[:, y]
    load_block(rows, land.at[0, 1:3], 0, keys, vals)
    fetch.wait()
    keep = pltpu.make_async_copy(w_own, w_all.at[me], local.at[1])
    keep.start()
    w_cols = w_own.shape[2] // 2

    def tensor_at(dz, dx):
        return (seq, links.slot(dz, dx))

    def own_w(dz, dx):
        return links.start(lambda: (w_own.at[core], w_all.at[me, core], tensor_at(dz, dx)))

    def pass_w(slot, lo, hi, dz, dx):
        def ends():
            ref = w_all.at[links.slot(*slot), core, :, lo * w_cols : hi * w_cols]
            return ref, ref, tensor_at(dz, dx)

        return links.start(ends)

    def swap_w(slot):
        def ends():
            ref = w_all.at[links.slot(*slot), core]
            return ref, ref, on_seq(0, 0, 1)

        return links.start(ends)

    wz, wup, wdown = own_w(1, 0), own_w(0, 1), own_w(0, 3)

    acc[...] = jnp.zeros_like(acc)
    probs[:, rows:PAD, :] = jnp.zeros((2, PAD - rows, WIDE), jnp.bfloat16)
    queries[HD:128, :] = jnp.zeros((128 - HD, width), jnp.bfloat16)
    queries[0:HD, 0:PAD] = land[0, 0]
    for i in (1, 2, 3):
        d = ORDER[i]
        by_y[d].wait_recv()
        to_core[d] = links.start(lambda d=d: (land.at[d, 1:3], kvx.at[0, d], on_seq(0, 0, 1)))
        to_far[d] = links.start(lambda d=d: (land.at[d, 1:3], kvx.at[1, d], on_seq(1, 0, 0)))
        load_block(rows, land.at[d, 1:3], i, keys, vals)
        queries[0:HD, d * PAD : (d + 1) * PAD] = land[d, 0]

    for c in range(width // WIDE):
        cols = slice(c * WIDE, (c + 1) * WIDE)
        s = jnp.dot(keys[0, 0:rows], queries[:, cols], preferred_element_type=jnp.float32)
        top = jnp.max(s.reshape(rows // 8, 8, WIDE), axis=0)
        top = jnp.max(top, axis=0, keepdims=True)
        first = lax.broadcasted_iota(jnp.int32, (16, WIDE), 0) == 0
        shift = jnp.where(first, jnp.broadcast_to(-top, (16, WIDE)), 0.0)
        queries[HD : HD + 16, cols] = shift.astype(jnp.bfloat16)

    more = {}

    def take(block):
        group, d = block // 4, ORDER[block % 4]
        if group == 1:
            to_core[d].wait_recv()
        elif group == 2:
            to_far[d].wait_recv()
            far_core[d] = links.start(lambda d=d: (kvx.at[1, d], kvx.at[2, d], on_seq(0, 0, 1)))
        elif group == 3:
            far_core[d].wait_recv()
        load_block(rows, kvx.at[group - 1, d], block, keys, vals)

    others = [(0, 1), (0, 2), (0, 3), (1, 0), (1, 1), (1, 2), (1, 3)]

    def stage(j):
        for block in (2 * j + 1, 2 * j + 2):
            if 4 <= block < 16:
                take(block)
        if j == 1:
            wz.wait_recv()
            more["zup"] = pass_w((1, 0), 0, 2, 0, 1)
            more["zdown"] = pass_w((1, 0), 0, 2, 0, 3)
            wup.wait_recv()
            more["r0"] = pass_w((0, 3), 0, 1, 0, 1)
            wdown.wait_recv()
            more["r1"] = pass_w((0, 1), 1, 2, 0, 3)
        if j == 3:
            more["zup"].wait_recv()
            more["q0"] = pass_w((1, 3), 0, 1, 0, 1)
            more["zdown"].wait_recv()
            more["q1"] = pass_w((1, 1), 1, 2, 0, 3)
        if j == 6:
            for name in ("r0", "r1", "q0", "q1"):
                more[name].wait_recv()
            for dz, dx in others:
                more[dz, dx] = swap_w((dz, dx))

    sweep(rows, 16, queries, keys, vals, acc, probs, 6, stage)
    keep.wait()
    for pair in others:
        more[pair].wait_recv()
    links.drain()


def settle_kernel(rows, acc_in, land, kvx, o_ref, queries, keys, vals, probs, acc):
    width = acc_in.shape[1]
    total = acc_in[HD : HD + 1, :]
    fits = jnp.where((total < LIMIT) & (total > FLOOR), 0.0, 1.0)
    again = jnp.max(fits) > 0.5

    def write(sums):
        for d in range(4):
            cols = slice(d * PAD, (d + 1) * PAD)
            o_ref[d] = (sums[0:HD, cols] / sums[HD : HD + 1, cols]).astype(jnp.bfloat16)

    @pl.when(jnp.logical_not(again))
    def _():
        write(acc_in)

    @pl.when(again)
    def _():
        queries[HD:128, :] = jnp.zeros((128 - HD, width), jnp.bfloat16)
        for d in range(4):
            queries[0:HD, d * PAD : (d + 1) * PAD] = land[d, 0]
        probs[rows:PAD, :] = jnp.zeros((PAD - rows, 256), jnp.bfloat16)
        acc[...] = jnp.zeros_like(acc)

        def fill(d, _):
            load_block(rows, land.at[d, 1:3], d, keys, vals)
            for g in range(3):
                load_block(rows, kvx.at[g, d], 4 * g + 4 + d, keys, vals)
            return 0

        lax.fori_loop(0, 4, fill, 0)

        def chunk(c, _):
            cols = pl.ds(pl.multiple_of(c * 256, 256), 256)

            def block(b, carry):
                peak, sums = carry
                s = jnp.dot(keys[b, 0:rows], queries[:, cols], preferred_element_type=jnp.float32)
                fresh = jnp.maximum(peak, jnp.max(s, axis=0, keepdims=True))
                probs[0:rows, :] = jnp.exp2(s - fresh).astype(jnp.bfloat16)
                part = jnp.dot(vals[b], probs[...], preferred_element_type=jnp.float32)
                return fresh, sums * jnp.exp2(peak - fresh) + part

            start = (jnp.full((1, 256), -1e30, jnp.float32), jnp.zeros((HD + 16, 256), jnp.float32))
            _, sums = lax.fori_loop(0, 16, block, start)
            acc[:, cols] = sums
            return 0

        lax.fori_loop(0, width // 256, chunk, 0)
        write(acc)


def attention(rows, qkv, w_out):
    width = 4 * PAD
    bf16 = jnp.bfloat16
    half, cols = w_out.shape[0] // 2, w_out.shape[1]
    n = 48
    tables = [
        pltpu.VMEM((128, width), bf16),
        pltpu.VMEM((16, PAD, 128), bf16),
        pltpu.VMEM((16, HD + 16, PAD), bf16),
    ]
    anywhere = pl.BlockSpec(memory_space=pl.ANY)
    acc, land, kvx, w_all = pl.pallas_call(
        functools.partial(attend_kernel, rows),
        out_shape=(
            jax.ShapeDtypeStruct((HD + 16, width), jnp.float32),
            jax.ShapeDtypeStruct((4, 3, HD, PAD), bf16),
            jax.ShapeDtypeStruct((3, 4, 2, HD, PAD), bf16),
            jax.ShapeDtypeStruct((8, 2, half, cols), bf16),
        ),
        in_specs=[FULL, anywhere],
        out_specs=(FULL, FULL, FULL, anywhere),
        scratch_shapes=tables
        + [
            pltpu.VMEM((2, PAD, WIDE), bf16),
            pltpu.VMEM((2, half, cols), bf16),
            pltpu.SemaphoreType.DMA((n,)),
            pltpu.SemaphoreType.DMA((n,)),
            pltpu.SemaphoreType.DMA((2,)),
        ],
        compiler_params=pltpu.CompilerParams(collective_id=0, has_side_effects=True, vmem_limit_bytes=48 * 2**20),
        name="attend",
    )(qkv, w_out.reshape(2, half, cols))
    o = pl.pallas_call(
        functools.partial(settle_kernel, rows),
        out_shape=jax.ShapeDtypeStruct((4, HD, PAD), bf16),
        in_specs=[FULL] * 3,
        out_specs=FULL,
        scratch_shapes=tables + [pltpu.VMEM((PAD, 256), bf16), pltpu.VMEM((HD + 16, width), jnp.float32)],
        compiler_params=pltpu.CompilerParams(vmem_limit_bytes=40 * 2**20),
        name="settle",
    )(acc, land, kvx)
    return o, w_all.reshape(16 * half, cols)


class Links:
    def __init__(self, send, recv):
        me = lax.axis_index("tensor")
        self.seq = lax.axis_index("seq")
        self.z, self.x = me // 4, lax.rem(me, 4)
        self.me = me
        self.send, self.recv = send, recv
        self.count = 0
        self.open = []

    def slot(self, dz, dx):
        z = lax.rem(self.z + dz, 2)
        return z * 4 + lax.rem(self.x + dx, 4)

    def barrier(self, more=0):
        sem = pltpu.get_barrier_semaphore()
        for dz, dx in ((1, 0), (0, 1), (0, 3)):
            pl.semaphore_signal(sem, inc=1, device_id=(self.seq, self.slot(dz, dx)), device_id_type=MESH)
        pl.semaphore_wait(sem, 3 + more)

    def put(self, src, dst, dz, dx):
        device = (self.seq, self.slot(dz, dx))
        return self.start(lambda: (src, dst, device))

    def start(self, ends):
        copy = Copy(self, self.count, ends)
        self.count += 1
        self.open.append(copy)
        copy.make().start()
        return copy

    def drain(self):
        for copy in self.open:
            copy.make().wait_send()
        self.open = []


class Copy:
    def __init__(self, links, index, ends):
        self.links, self.index, self.ends = links, index, ends

    def make(self):
        src, dst, device = self.ends()
        return pltpu.make_async_remote_copy(
            src_ref=src,
            dst_ref=dst,
            send_sem=self.links.send.at[self.index],
            recv_sem=self.links.recv.at[self.index],
            device_id=device,
            device_id_type=MESH,
        )

    def wait_recv(self):
        self.make().wait_recv()


def gather_tensor(links, piece):
    s = links.slot
    put = links.put

    def pass_on(slot, lo, hi, dz, dx):
        ref = piece(slot, lo, hi)
        return put(ref, ref, dz, dx)

    me = s(0, 0)
    a_z = pass_on(me, 0, 2, 1, 0)
    b_up = pass_on(me, 2, 4, 0, 1)
    b_down = pass_on(me, 2, 4, 0, 3)
    b_z = pass_on(me, 2, 4, 1, 0)
    a_up = pass_on(me, 0, 2, 0, 1)
    a_down = pass_on(me, 0, 2, 0, 3)
    b_up.wait_recv()
    r2 = pass_on(s(0, 3), 2, 3, 0, 1)
    bz_lo = pass_on(s(0, 3), 2, 4, 1, 0)
    b_down.wait_recv()
    r3 = pass_on(s(0, 1), 3, 4, 0, 3)
    bz_hi = pass_on(s(0, 1), 2, 4, 1, 0)
    a_z.wait_recv()
    az_up = pass_on(s(1, 0), 0, 2, 0, 1)
    az_down = pass_on(s(1, 0), 0, 2, 0, 3)
    a_up.wait_recv()
    r0 = pass_on(s(0, 3), 0, 1, 0, 1)
    a_down.wait_recv()
    r1 = pass_on(s(0, 1), 1, 2, 0, 3)
    r2.wait_recv()
    bz_2 = pass_on(s(0, 2), 2, 3, 1, 0)
    r3.wait_recv()
    bz_3 = pass_on(s(0, 2), 3, 4, 1, 0)
    az_up.wait_recv()
    q0 = pass_on(s(1, 3), 0, 1, 0, 1)
    az_down.wait_recv()
    q1 = pass_on(s(1, 1), 1, 2, 0, 3)
    for copy in (b_z, bz_lo, bz_hi, r0, r1, bz_2, bz_3, q0, q1):
        copy.wait_recv()
    links.drain()


GATHER_COPIES = 18


def gather_heads_kernel(o_ref, out_ref, send, recv):
    links = Links(send, recv)
    seq = links.seq
    y = lax.rem(seq // 2, 4)

    def at_y(dy):
        return ((seq // 8 * 4 + lax.rem(y + dy, 4)) * 2 + lax.rem(seq, 2), links.me)

    sem = pltpu.get_barrier_semaphore()
    for d in (1, 2, 3):
        pl.semaphore_signal(sem, inc=1, device_id=at_y(d), device_id_type=MESH)
    links.barrier(3)
    back = [links.start(lambda d=d: (o_ref.at[d], out_ref.at[links.me, y], at_y(4 - d))) for d in (2, 1, 3)]
    out_ref[links.me, y] = o_ref[0]
    for copy in back:
        copy.wait_recv()
    gather_tensor(links, lambda slot, lo, hi: out_ref.at[slot, lo:hi])


def gather_heads(o):
    copies = GATHER_COPIES + 3
    return pl.pallas_call(
        gather_heads_kernel,
        out_shape=jax.ShapeDtypeStruct((8,) + o.shape, o.dtype),
        in_specs=[FULL],
        out_specs=FULL,
        scratch_shapes=[pltpu.SemaphoreType.DMA((copies,)), pltpu.SemaphoreType.DMA((copies,))],
        compiler_params=pltpu.CompilerParams(collective_id=1, has_side_effects=True, vmem_limit_bytes=32 * 2**20),
        name="gather_heads",
    )(o)


def reduce_tensor(links, term, stage, rows, cols):
    quarter = cols // 4
    s = links.slot
    put = links.put

    def q(slot, lo, hi):
        return term.at[slot, :, lo * quarter : hi * quarter]

    def val(slot, lo, hi):
        return term[slot, :, lo * quarter : hi * quarter].astype(jnp.float32)

    def land(i, n):
        return stage.at[i, :, 0 : n * quarter]

    def got(i, lo, hi):
        return stage[i, :, lo * quarter : hi * quarter].astype(jnp.float32)

    def add_into(slot, lo, hi, *parts):
        total = val(slot, lo, hi)
        for part in parts:
            total = total + part
        term[slot, :, lo * quarter : hi * quarter] = total.astype(jnp.bfloat16)

    zb = {}
    for i, dx in enumerate((2, 1, 3, 0)):
        zb[dx] = put(q(s(1, dx), 2, 4), land(i, 2), 1, 0)
    fa = {}
    for j, dz in enumerate((1, 0)):
        fa[dz, 0] = put(q(s(dz, 2), 0, 1), land(4 + j, 1), 0, 3)
        fa[dz, 1] = put(q(s(dz, 2), 1, 2), land(6 + j, 1), 0, 1)
    near = {}
    for j, dz in enumerate((1, 0)):
        fa[dz, 0].wait_recv()
        add_into(s(dz, 3), 0, 1, got(4 + j, 0, 1))
        near[dz, 3] = put(q(s(dz, 3), 0, 2), land(8 + j, 2), 0, 3)
        fa[dz, 1].wait_recv()
        add_into(s(dz, 1), 1, 2, got(6 + j, 0, 1))
        near[dz, 1] = put(q(s(dz, 1), 0, 2), land(10 + j, 2), 0, 1)
    zb[2].wait_recv()
    add_into(s(0, 2), 2, 4, got(0, 0, 2))
    fb0 = put(q(s(0, 2), 2, 3), land(12, 1), 0, 3)
    fb1 = put(q(s(0, 2), 3, 4), land(13, 1), 0, 1)
    zb[1].wait_recv()
    zb[3].wait_recv()
    near[1, 3].wait_recv()
    near[1, 1].wait_recv()
    add_into(s(1, 0), 0, 2, got(8, 0, 2), got(10, 0, 2))
    za = put(q(s(1, 0), 0, 2), land(14, 2), 1, 0)
    fb0.wait_recv()
    add_into(s(0, 3), 2, 3, got(2, 0, 1), got(12, 0, 1))
    add_into(s(0, 3), 3, 4, got(2, 1, 2))
    nb3 = put(q(s(0, 3), 2, 4), land(15, 2), 0, 3)
    fb1.wait_recv()
    add_into(s(0, 1), 3, 4, got(1, 1, 2), got(13, 0, 1))
    add_into(s(0, 1), 2, 3, got(1, 0, 1))
    nb1 = put(q(s(0, 1), 2, 4), land(16, 2), 0, 1)
    near[0, 3].wait_recv()
    near[0, 1].wait_recv()
    za.wait_recv()
    first = val(s(0, 0), 0, 2) + got(9, 0, 2) + got(11, 0, 2) + got(14, 0, 2)
    zb[0].wait_recv()
    nb3.wait_recv()
    nb1.wait_recv()
    second = val(s(0, 0), 2, 4) + got(3, 0, 2) + got(15, 0, 2) + got(16, 0, 2)
    links.drain()
    return first, second


def finish_kernel(term_in, mixed_ref, out_ref, term, stage, send, recv):
    rows, cols = mixed_ref.shape
    quarter = cols // 4
    links = Links(send, recv)
    links.barrier()
    term[...] = term_in[...]
    first, second = reduce_tensor(links, term, stage, rows, cols)
    out_ref[links.me, :, 0 : 2 * quarter] = (mixed_ref[:, 0 : 2 * quarter] + first).astype(jnp.bfloat16)
    out_ref[links.me, :, 2 * quarter :] = (mixed_ref[:, 2 * quarter :] + second).astype(jnp.bfloat16)
    gather_tensor(links, lambda slot, lo, hi: out_ref.at[slot, :, lo * quarter : hi * quarter])


def finish(term, mixed):
    parts, rows, cols = term.shape
    copies = 40
    return pl.pallas_call(
        finish_kernel,
        out_shape=jax.ShapeDtypeStruct(term.shape, jnp.bfloat16),
        in_specs=[FULL, FULL],
        out_specs=FULL,
        scratch_shapes=[
            pltpu.VMEM(term.shape, jnp.bfloat16),
            pltpu.VMEM((17, rows, cols // 2), jnp.bfloat16),
            pltpu.SemaphoreType.DMA((copies,)),
            pltpu.SemaphoreType.DMA((copies,)),
        ],
        compiler_params=pltpu.CompilerParams(collective_id=2, has_side_effects=True, vmem_limit_bytes=40 * 2**20),
        name="finish",
    )(term, mixed)


def per_device(tokens, norm_gain, w_qkv, w_out, post_gain, w_up, w_down):
    rows, width = tokens.shape
    heads = w_qkv.shape[2] // HD
    t = lax.axis_index("tensor")
    base = tokens.astype(jnp.float32)
    normed = layer_norm(base, norm_gain).astype(jnp.bfloat16)
    qkv = lax.dot_general(w_qkv, normed, (((0,), (1,)), ((), ())), preferred_element_type=jnp.float32)
    factor = jnp.array([LOG2E / HD**0.5, 1.0, 1.0], jnp.float32)[:, None, None]
    qkv = (qkv * factor).astype(jnp.bfloat16)
    qkv = jnp.pad(qkv, ((0, 0), (0, 0), (0, PAD - rows))).reshape(3, heads, HD, PAD)

    o, w_out_all = attention(rows, qkv, w_out)
    every = gather_heads(o).reshape(8 * heads * HD, PAD)
    padded = jnp.pad(base, ((0, PAD - rows), (0, 0)))
    mixed = padded + lax.dot_general(
        every, w_out_all, (((0,), (0,)), ((), ())), preferred_element_type=jnp.float32
    )
    post = layer_norm(mixed, post_gain).astype(jnp.bfloat16)
    hidden = jax.nn.gelu(
        jnp.dot(post, w_up, preferred_element_type=jnp.float32), approximate=True
    ).astype(jnp.bfloat16)
    term = jnp.dot(hidden, w_down, preferred_element_type=jnp.float32).astype(jnp.bfloat16)
    share = PAD // 8
    mine = lax.dynamic_slice_in_dim(mixed, t * share, share, 0)
    out = finish(term.reshape(8, share, width), mine)
    return out.reshape(PAD, width)[:rows]


def solution(mesh):
    placed = (
        P("seq", None),
        P(),
        P(None, None, "tensor"),
        P("tensor", None),
        P(),
        P(None, "tensor"),
        P("tensor", None),
    )
    return jax.shard_map(
        per_device, mesh=mesh, in_specs=placed, out_specs=P("seq", None), check_vma=False
    )
```

```python
import functools

import jax
import jax.numpy as jnp
from jax import lax
from jax.experimental import pallas as pl
from jax.experimental.pallas import tpu as pltpu
from jax.sharding import PartitionSpec as P

HD = 48
PAD = 768
WIDE = 1024
MESH = pl.DeviceIdType.MESH
LOG2E = 1.4426950408889634
LIMIT = 2.0**90
FLOOR = 2.0**-20
FULL = pl.BlockSpec(memory_space=pltpu.VMEM)


def layer_norm(values, gain):
    mean = jnp.mean(values, axis=-1, keepdims=True)
    centred = values - mean
    var = jnp.mean(centred * centred, axis=-1, keepdims=True)
    return centred * lax.rsqrt(var + 1e-05) * gain


def sweep(rows, blocks, queries, keys, vals, acc, probs, unroll, stage):
    chunks = queries.shape[1] // WIDE
    total = blocks * chunks

    def place(i):
        return i // chunks, pl.ds(pl.multiple_of(lax.rem(i, chunks) * WIDE, WIDE), WIDE)

    def scores(i, slot):
        b, cols = place(i)
        s = jnp.dot(keys[b, 0:rows], queries[:, cols], preferred_element_type=jnp.float32)
        probs[slot, 0:rows, :] = jnp.exp2(s).astype(jnp.bfloat16)

    def product(i, slot):
        b, cols = place(i)
        acc[:, cols] += jnp.dot(vals[b], probs[slot], preferred_element_type=jnp.float32)

    scores(0, 0)

    def body(j, _):
        for k in range(total // unroll):

            @pl.when(j == k)
            def _(k=k):
                stage(k)

        for u in range(unroll):
            i = unroll * j + u
            ahead = i + 1 if u < unroll - 1 else jnp.minimum(i + 1, total - 1)
            scores(ahead, (u + 1) % 2)
            product(i, u % 2)
        return 0

    lax.fori_loop(0, total // unroll, body, 0)


ORDER = (0, 1, 3, 2)


def load_block(rows, kv, b, keys, vals):
    lane = lax.broadcasted_iota(jnp.int32, (16, PAD), 1)
    sub = lax.broadcasted_iota(jnp.int32, (16, PAD), 0)
    count = ((sub == 0) & (lane < rows)).astype(jnp.float32).astype(jnp.bfloat16)
    shift = (sub == 0).astype(jnp.float32).astype(jnp.bfloat16)
    zeros = jnp.zeros((64, PAD), jnp.bfloat16)
    keys[b] = jnp.concatenate([kv[0], shift, zeros], axis=0).T
    vals[b, 0:HD] = kv[1]
    vals[b, HD : HD + 16] = count


def attend_kernel(rows, qkv, w_ref, acc, land, kvx, w_all, queries, keys, vals, probs, w_own, send, recv, local):
    width = queries.shape[1]
    seq, me = lax.axis_index("seq"), lax.axis_index("tensor")
    z, y, core = seq // 8, lax.rem(seq // 2, 4), lax.rem(seq, 2)
    links = Links(send, recv)

    def on_seq(dz, dy, dc):
        return ((lax.rem(z + dz, 2) * 4 + lax.rem(y + dy, 4)) * 2 + lax.rem(core + dc, 2), me)

    barrier = pltpu.get_barrier_semaphore()
    peers = [on_seq(0, d, 0) for d in (1, 2, 3)] + [on_seq(0, 0, 1), on_seq(1, 0, 0)]
    peers += [(seq, links.slot(1, 0)), (seq, links.slot(0, 1)), (seq, links.slot(0, 3))]
    for peer in peers:
        pl.semaphore_signal(barrier, inc=1, device_id=peer, device_id_type=MESH)
    pl.semaphore_wait(barrier, 8)

    by_y = {}
    for d in (2, 1, 3):
        by_y[d] = links.start(lambda d=d: (qkv.at[:, lax.rem(y + d, 4)], land.at[d], on_seq(0, d, 0)))
    to_core, to_far, far_core = {}, {}, {}
    to_core[0] = links.start(lambda: (qkv.at[1:3, y], kvx.at[0, 0], on_seq(0, 0, 1)))
    to_far[0] = links.start(lambda: (qkv.at[1:3, y], kvx.at[1, 0], on_seq(1, 0, 0)))

    fetch = pltpu.make_async_copy(w_ref, w_own, local.at[0])
    fetch.start()
    land[0] = qkv[:, y]
    load_block(rows, land.at[0, 1:3], 0, keys, vals)
    fetch.wait()
    keep = pltpu.make_async_copy(w_own, w_all.at[me], local.at[1])
    keep.start()
    w_cols = w_own.shape[2] // 2

    def tensor_at(dz, dx):
        return (seq, links.slot(dz, dx))

    def own_w(dz, dx):
        return links.start(lambda: (w_own.at[core], w_all.at[me, core], tensor_at(dz, dx)))

    def pass_w(slot, lo, hi, dz, dx):
        def ends():
            ref = w_all.at[links.slot(*slot), core, :, lo * w_cols : hi * w_cols]
            return ref, ref, tensor_at(dz, dx)

        return links.start(ends)

    def swap_w(slot):
        def ends():
            ref = w_all.at[links.slot(*slot), core]
            return ref, ref, on_seq(0, 0, 1)

        return links.start(ends)

    wz, wup, wdown = own_w(1, 0), own_w(0, 1), own_w(0, 3)

    acc[...] = jnp.zeros_like(acc)
    probs[:, rows:PAD, :] = jnp.zeros((2, PAD - rows, WIDE), jnp.bfloat16)
    queries[HD:128, :] = jnp.zeros((128 - HD, width), jnp.bfloat16)
    queries[0:HD, 0:PAD] = land[0, 0]
    for i in (1, 2, 3):
        d = ORDER[i]
        by_y[d].wait_recv()
        to_core[d] = links.start(lambda d=d: (land.at[d, 1:3], kvx.at[0, d], on_seq(0, 0, 1)))
        to_far[d] = links.start(lambda d=d: (land.at[d, 1:3], kvx.at[1, d], on_seq(1, 0, 0)))
        load_block(rows, land.at[d, 1:3], i, keys, vals)
        queries[0:HD, d * PAD : (d + 1) * PAD] = land[d, 0]

    for c in range(width // WIDE):
        cols = slice(c * WIDE, (c + 1) * WIDE)
        s = jnp.dot(keys[0, 0:rows], queries[:, cols], preferred_element_type=jnp.float32)
        top = jnp.max(s.reshape(rows // 8, 8, WIDE), axis=0)
        top = jnp.max(top, axis=0, keepdims=True)
        first = lax.broadcasted_iota(jnp.int32, (16, WIDE), 0) == 0
        shift = jnp.where(first, jnp.broadcast_to(-top, (16, WIDE)), 0.0)
        queries[HD : HD + 16, cols] = shift.astype(jnp.bfloat16)

    more = {}

    def take(block):
        group, d = block // 4, ORDER[block % 4]
        if group == 1:
            to_core[d].wait_recv()
        elif group == 2:
            to_far[d].wait_recv()
            far_core[d] = links.start(lambda d=d: (kvx.at[1, d], kvx.at[2, d], on_seq(0, 0, 1)))
        elif group == 3:
            far_core[d].wait_recv()
        load_block(rows, kvx.at[group - 1, d], block, keys, vals)

    others = [(0, 1), (0, 2), (0, 3), (1, 0), (1, 1), (1, 2), (1, 3)]

    def stage(j):
        for block in (2 * j + 1, 2 * j + 2):
            if 4 <= block < 16:
                take(block)
        if j == 1:
            wz.wait_recv()
            more["zup"] = pass_w((1, 0), 0, 2, 0, 1)
            more["zdown"] = pass_w((1, 0), 0, 2, 0, 3)
            wup.wait_recv()
            more["r0"] = pass_w((0, 3), 0, 1, 0, 1)
            wdown.wait_recv()
            more["r1"] = pass_w((0, 1), 1, 2, 0, 3)
        if j == 3:
            more["zup"].wait_recv()
            more["q0"] = pass_w((1, 3), 0, 1, 0, 1)
            more["zdown"].wait_recv()
            more["q1"] = pass_w((1, 1), 1, 2, 0, 3)
        if j == 6:
            for name in ("r0", "r1", "q0", "q1"):
                more[name].wait_recv()
            for dz, dx in others:
                more[dz, dx] = swap_w((dz, dx))

    sweep(rows, 16, queries, keys, vals, acc, probs, 6, stage)
    keep.wait()
    for pair in others:
        more[pair].wait_recv()
    links.drain()


def settle_kernel(rows, acc_in, land, kvx, o_ref, queries, keys, vals, probs, acc):
    width = acc_in.shape[1]
    total = acc_in[HD : HD + 1, :]
    fits = jnp.where((total < LIMIT) & (total > FLOOR), 0.0, 1.0)
    again = jnp.max(fits) > 0.5

    def write(sums):
        for d in range(4):
            cols = slice(d * PAD, (d + 1) * PAD)
            o_ref[d] = (sums[0:HD, cols] / sums[HD : HD + 1, cols]).astype(jnp.bfloat16)

    @pl.when(jnp.logical_not(again))
    def _():
        write(acc_in)

    @pl.when(again)
    def _():
        queries[HD:128, :] = jnp.zeros((128 - HD, width), jnp.bfloat16)
        for d in range(4):
            queries[0:HD, d * PAD : (d + 1) * PAD] = land[d, 0]
        probs[rows:PAD, :] = jnp.zeros((PAD - rows, 256), jnp.bfloat16)
        acc[...] = jnp.zeros_like(acc)

        def fill(d, _):
            load_block(rows, land.at[d, 1:3], d, keys, vals)
            for g in range(3):
                load_block(rows, kvx.at[g, d], 4 * g + 4 + d, keys, vals)
            return 0

        lax.fori_loop(0, 4, fill, 0)

        def chunk(c, _):
            cols = pl.ds(pl.multiple_of(c * 256, 256), 256)

            def block(b, carry):
                peak, sums = carry
                s = jnp.dot(keys[b, 0:rows], queries[:, cols], preferred_element_type=jnp.float32)
                fresh = jnp.maximum(peak, jnp.max(s, axis=0, keepdims=True))
                probs[0:rows, :] = jnp.exp2(s - fresh).astype(jnp.bfloat16)
                part = jnp.dot(vals[b], probs[...], preferred_element_type=jnp.float32)
                return fresh, sums * jnp.exp2(peak - fresh) + part

            start = (jnp.full((1, 256), -1e30, jnp.float32), jnp.zeros((HD + 16, 256), jnp.float32))
            _, sums = lax.fori_loop(0, 16, block, start)
            acc[:, cols] = sums
            return 0

        lax.fori_loop(0, width // 256, chunk, 0)
        write(acc)


def attention(rows, qkv, w_out):
    width = 4 * PAD
    bf16 = jnp.bfloat16
    half, cols = w_out.shape[0] // 2, w_out.shape[1]
    n = 48
    tables = [
        pltpu.VMEM((128, width), bf16),
        pltpu.VMEM((16, PAD, 128), bf16),
        pltpu.VMEM((16, HD + 16, PAD), bf16),
    ]
    anywhere = pl.BlockSpec(memory_space=pl.ANY)
    acc, land, kvx, w_all = pl.pallas_call(
        functools.partial(attend_kernel, rows),
        out_shape=(
            jax.ShapeDtypeStruct((HD + 16, width), jnp.float32),
            jax.ShapeDtypeStruct((4, 3, HD, PAD), bf16),
            jax.ShapeDtypeStruct((3, 4, 2, HD, PAD), bf16),
            jax.ShapeDtypeStruct((8, 2, half, cols), bf16),
        ),
        in_specs=[FULL, anywhere],
        out_specs=(FULL, FULL, FULL, anywhere),
        scratch_shapes=tables
        + [
            pltpu.VMEM((2, PAD, WIDE), bf16),
            pltpu.VMEM((2, half, cols), bf16),
            pltpu.SemaphoreType.DMA((n,)),
            pltpu.SemaphoreType.DMA((n,)),
            pltpu.SemaphoreType.DMA((2,)),
        ],
        compiler_params=pltpu.CompilerParams(collective_id=0, has_side_effects=True, vmem_limit_bytes=48 * 2**20),
        name="attend",
    )(qkv, w_out.reshape(2, half, cols))
    o = pl.pallas_call(
        functools.partial(settle_kernel, rows),
        out_shape=jax.ShapeDtypeStruct((4, HD, PAD), bf16),
        in_specs=[FULL] * 3,
        out_specs=FULL,
        scratch_shapes=tables + [pltpu.VMEM((PAD, 256), bf16), pltpu.VMEM((HD + 16, width), jnp.float32)],
        compiler_params=pltpu.CompilerParams(vmem_limit_bytes=40 * 2**20),
        name="settle",
    )(acc, land, kvx)
    return o, w_all.reshape(16 * half, cols)


class Links:
    def __init__(self, send, recv):
        me = lax.axis_index("tensor")
        self.seq = lax.axis_index("seq")
        self.z, self.x = me // 4, lax.rem(me, 4)
        self.me = me
        self.send, self.recv = send, recv
        self.count = 0
        self.open = []

    def slot(self, dz, dx):
        z = lax.rem(self.z + dz, 2)
        return z * 4 + lax.rem(self.x + dx, 4)

    def barrier(self, more=0):
        sem = pltpu.get_barrier_semaphore()
        for dz, dx in ((1, 0), (0, 1), (0, 3)):
            pl.semaphore_signal(sem, inc=1, device_id=(self.seq, self.slot(dz, dx)), device_id_type=MESH)
        pl.semaphore_wait(sem, 3 + more)

    def put(self, src, dst, dz, dx):
        device = (self.seq, self.slot(dz, dx))
        return self.start(lambda: (src, dst, device))

    def start(self, ends):
        copy = Copy(self, self.count, ends)
        self.count += 1
        self.open.append(copy)
        copy.make().start()
        return copy

    def drain(self):
        for copy in self.open:
            copy.make().wait_send()
        self.open = []


class Copy:
    def __init__(self, links, index, ends):
        self.links, self.index, self.ends = links, index, ends

    def make(self):
        src, dst, device = self.ends()
        return pltpu.make_async_remote_copy(
            src_ref=src,
            dst_ref=dst,
            send_sem=self.links.send.at[self.index],
            recv_sem=self.links.recv.at[self.index],
            device_id=device,
            device_id_type=MESH,
        )

    def wait_recv(self):
        self.make().wait_recv()


def gather_tensor(links, piece, ready=lambda dz, dx: None):
    s = links.slot
    put = links.put

    def pass_on(slot, lo, hi, dz, dx):
        ref = piece(slot, lo, hi)
        return put(ref, ref, dz, dx)

    me = s(0, 0)
    a_z = pass_on(me, 0, 2, 1, 0)
    b_up = pass_on(me, 2, 4, 0, 1)
    b_down = pass_on(me, 2, 4, 0, 3)
    b_z = pass_on(me, 2, 4, 1, 0)
    a_up = pass_on(me, 0, 2, 0, 1)
    a_down = pass_on(me, 0, 2, 0, 3)
    ready(0, 0)
    b_up.wait_recv()
    r2 = pass_on(s(0, 3), 2, 3, 0, 1)
    bz_lo = pass_on(s(0, 3), 2, 4, 1, 0)
    b_down.wait_recv()
    r3 = pass_on(s(0, 1), 3, 4, 0, 3)
    bz_hi = pass_on(s(0, 1), 2, 4, 1, 0)
    a_z.wait_recv()
    az_up = pass_on(s(1, 0), 0, 2, 0, 1)
    az_down = pass_on(s(1, 0), 0, 2, 0, 3)
    a_up.wait_recv()
    r0 = pass_on(s(0, 3), 0, 1, 0, 1)
    a_down.wait_recv()
    r1 = pass_on(s(0, 1), 1, 2, 0, 3)
    ready(0, 3)
    r2.wait_recv()
    bz_2 = pass_on(s(0, 2), 2, 3, 1, 0)
    r3.wait_recv()
    bz_3 = pass_on(s(0, 2), 3, 4, 1, 0)
    ready(0, 1)
    az_up.wait_recv()
    q0 = pass_on(s(1, 3), 0, 1, 0, 1)
    az_down.wait_recv()
    q1 = pass_on(s(1, 1), 1, 2, 0, 3)
    b_z.wait_recv()
    ready(1, 0)
    r0.wait_recv()
    r1.wait_recv()
    ready(0, 2)
    bz_lo.wait_recv()
    ready(1, 3)
    bz_hi.wait_recv()
    ready(1, 1)
    for copy in (bz_2, bz_3, q0, q1):
        copy.wait_recv()
    ready(1, 2)
    links.drain()


GATHER_COPIES = 18


def reduce_tensor(links, term, stage, rows, cols, make):
    quarter = cols // 4
    s = links.slot
    put = links.put

    def q(slot, lo, hi):
        return term.at[slot, :, lo * quarter : hi * quarter]

    def val(slot, lo, hi):
        return term[slot, :, lo * quarter : hi * quarter].astype(jnp.float32)

    def land(i, n):
        return stage.at[i, :, 0 : n * quarter]

    def got(i, lo, hi):
        return stage[i, :, lo * quarter : hi * quarter].astype(jnp.float32)

    def add_into(slot, lo, hi, *parts):
        total = val(slot, lo, hi)
        for part in parts:
            total = total + part
        term[slot, :, lo * quarter : hi * quarter] = total.astype(jnp.bfloat16)

    zb, fa, near = {}, {}, {}

    def cross(i, dx):
        zb[dx] = put(q(s(1, dx), 2, 4), land(i, 2), 1, 0)

    def far(j, dz):
        fa[dz, 0] = put(q(s(dz, 2), 0, 1), land(4 + j, 1), 0, 3)
        fa[dz, 1] = put(q(s(dz, 2), 1, 2), land(6 + j, 1), 0, 1)

    def relay(j, dz):
        fa[dz, 0].wait_recv()
        add_into(s(dz, 3), 0, 1, got(4 + j, 0, 1))
        near[dz, 3] = put(q(s(dz, 3), 0, 2), land(8 + j, 2), 0, 3)
        fa[dz, 1].wait_recv()
        add_into(s(dz, 1), 1, 2, got(6 + j, 0, 1))
        near[dz, 1] = put(q(s(dz, 1), 0, 2), land(10 + j, 2), 0, 1)

    make((1, 2), (1, 0))
    cross(0, 2)
    far(0, 1)
    far(1, 0)
    make((1, 1), (0, 2))
    cross(1, 1)
    cross(2, 3)
    relay(0, 1)
    make((0, 1), (0, 2))
    relay(1, 0)
    zb[2].wait_recv()
    add_into(s(0, 2), 2, 4, got(0, 0, 2))
    fb0 = put(q(s(0, 2), 2, 3), land(12, 1), 0, 3)
    fb1 = put(q(s(0, 2), 3, 4), land(13, 1), 0, 1)
    make((1, 0), (1, 0))
    cross(3, 0)
    zb[1].wait_recv()
    zb[3].wait_recv()
    near[1, 3].wait_recv()
    near[1, 1].wait_recv()
    add_into(s(1, 0), 0, 2, got(8, 0, 2), got(10, 0, 2))
    za = put(q(s(1, 0), 0, 2), land(14, 2), 1, 0)
    fb0.wait_recv()
    add_into(s(0, 3), 2, 3, got(2, 0, 1), got(12, 0, 1))
    add_into(s(0, 3), 3, 4, got(2, 1, 2))
    nb3 = put(q(s(0, 3), 2, 4), land(15, 2), 0, 3)
    fb1.wait_recv()
    add_into(s(0, 1), 3, 4, got(1, 1, 2), got(13, 0, 1))
    add_into(s(0, 1), 2, 3, got(1, 0, 1))
    nb1 = put(q(s(0, 1), 2, 4), land(16, 2), 0, 1)
    near[0, 3].wait_recv()
    near[0, 1].wait_recv()
    za.wait_recv()
    first = val(s(0, 0), 0, 2) + got(9, 0, 2) + got(11, 0, 2) + got(14, 0, 2)
    zb[0].wait_recv()
    nb3.wait_recv()
    nb1.wait_recv()
    second = val(s(0, 0), 2, 4) + got(3, 0, 2) + got(15, 0, 2) + got(16, 0, 2)
    links.drain()
    return first, second


def tail_kernel(
    o_ref, w_out, tokens, gain, w_up, w_down, out_ref, every, mixed, post, term, stage, wo, tok, wu, wd, send, recv, local
):
    links = Links(send, recv)
    seq, me = links.seq, links.me
    y = lax.rem(seq // 2, 4)
    share, width = out_ref.shape[1], out_ref.shape[2]
    quarter = width // 4
    rows = tok.shape[0]
    loads = [
        pltpu.make_async_copy(src, dst, local.at[i])
        for i, (src, dst) in enumerate(((tokens, tok), (w_out, wo), (w_up, wu), (w_down, wd)))
    ]
    for load in loads:
        load.start()

    def at_y(dy):
        return ((seq // 8 * 4 + lax.rem(y + dy, 4)) * 2 + lax.rem(seq, 2), me)

    sem = pltpu.get_barrier_semaphore()
    for d in (1, 2, 3):
        pl.semaphore_signal(sem, inc=1, device_id=at_y(d), device_id_type=MESH)
    links.barrier(3)
    back = [links.start(lambda d=d: (o_ref.at[d], every.at[me, y], at_y(4 - d))) for d in (2, 1, 3)]
    every[me, y] = o_ref[0]
    loads[0].wait()
    mixed[0:rows, :] = tok[...].astype(jnp.float32)
    mixed[rows:, :] = jnp.zeros((PAD - rows, width), jnp.float32)
    loads[1].wait()
    for copy in back:
        copy.wait_recv()

    def project(dz, dx):
        slot = links.slot(dz, dx)

        def tile(i, _):
            at = pl.ds(pl.multiple_of(i * 256, 256), 256)
            left = every[slot, :, :, at].reshape(4 * HD, 256)
            mixed[at, :] += lax.dot_general(
                left, wo[slot], (((0,), (0,)), ((), ())), preferred_element_type=jnp.float32
            )
            return 0

        lax.fori_loop(0, PAD // 256, tile, 0)

    gather_tensor(links, lambda slot, lo, hi: every.at[slot, lo:hi], project)
    loads[2].wait()
    loads[3].wait()

    def feed_forward(start, step):
        def block(k, _):
            slot = links.slot(start[0] + step[0] * k, start[1] + step[1] * k)
            at = pl.ds(pl.multiple_of(slot * share, 32), share)
            post[...] = layer_norm(mixed[at, :], gain[...]).astype(jnp.bfloat16)
            up = jnp.dot(post[...], wu[...], preferred_element_type=jnp.float32)
            hidden = jax.nn.gelu(up, approximate=True).astype(jnp.bfloat16)
            down = jnp.dot(hidden, wd[...], preferred_element_type=jnp.float32)
            term[slot] = down.astype(jnp.bfloat16)
            return 0

        lax.fori_loop(0, 2, block, 0)

    first, second = reduce_tensor(links, term, stage, share, width, feed_forward)
    at = pl.ds(pl.multiple_of(me * share, 32), share)
    out_ref[me, :, 0 : 2 * quarter] = (mixed[at, 0 : 2 * quarter] + first).astype(jnp.bfloat16)
    out_ref[me, :, 2 * quarter :] = (mixed[at, 2 * quarter :] + second).astype(jnp.bfloat16)
    gather_tensor(links, lambda slot, lo, hi: out_ref.at[slot, :, lo * quarter : hi * quarter])


def tail(o, w_out, tokens, gain, w_up, w_down):
    rows, cols = tokens.shape
    share = PAD // 8
    copies = 64
    bf16 = jnp.bfloat16
    anywhere = pl.BlockSpec(memory_space=pl.ANY)
    return pl.pallas_call(
        tail_kernel,
        out_shape=jax.ShapeDtypeStruct((8, share, cols), bf16),
        in_specs=[FULL, anywhere, anywhere, FULL, anywhere, anywhere],
        out_specs=FULL,
        scratch_shapes=[
            pltpu.VMEM((8,) + o.shape, bf16),
            pltpu.VMEM((PAD, cols), jnp.float32),
            pltpu.VMEM((share, cols), bf16),
            pltpu.VMEM((8, share, cols), bf16),
            pltpu.VMEM((17, share, cols // 2), bf16),
            pltpu.VMEM(w_out.shape, bf16),
            pltpu.VMEM(tokens.shape, bf16),
            pltpu.VMEM(w_up.shape, bf16),
            pltpu.VMEM(w_down.shape, bf16),
            pltpu.SemaphoreType.DMA((copies,)),
            pltpu.SemaphoreType.DMA((copies,)),
            pltpu.SemaphoreType.DMA((4,)),
        ],
        compiler_params=pltpu.CompilerParams(collective_id=1, has_side_effects=True, vmem_limit_bytes=48 * 2**20),
        name="tail",
    )(o, w_out, tokens, gain, w_up, w_down)


def per_device(tokens, norm_gain, w_qkv, w_out, post_gain, w_up, w_down):
    rows, width = tokens.shape
    heads = w_qkv.shape[2] // HD
    base = tokens.astype(jnp.float32)
    normed = layer_norm(base, norm_gain).astype(jnp.bfloat16)
    qkv = lax.dot_general(w_qkv, normed, (((0,), (1,)), ((), ())), preferred_element_type=jnp.float32)
    factor = jnp.array([LOG2E / HD**0.5, 1.0, 1.0], jnp.float32)[:, None, None]
    qkv = (qkv * factor).astype(jnp.bfloat16)
    qkv = jnp.pad(qkv, ((0, 0), (0, 0), (0, PAD - rows))).reshape(3, heads, HD, PAD)

    o, w_out_all = attention(rows, qkv, w_out)
    out = tail(o, w_out_all.reshape(8, heads * HD, width), tokens, post_gain.reshape(1, width), w_up, w_down)
    return out.reshape(PAD, width)[:rows]


def solution(mesh):
    placed = (
        P("seq", None),
        P(),
        P(None, None, "tensor"),
        P("tensor", None),
        P(),
        P(None, "tensor"),
        P("tensor", None),
    )
    return jax.shard_map(
        per_device, mesh=mesh, in_specs=placed, out_specs=P("seq", None), check_vma=False
    )
```

```python
import functools

import jax
import jax.numpy as jnp
from jax import lax
from jax.experimental import pallas as pl
from jax.experimental.pallas import tpu as pltpu
from jax.sharding import PartitionSpec as P

HD = 48
PAD = 768
WIDE = PAD
MESH = pl.DeviceIdType.MESH
LOG2E = 1.4426950408889634
LIMIT = 2.0**90
FLOOR = 2.0**-20
FULL = pl.BlockSpec(memory_space=pltpu.VMEM)


def layer_norm(values, gain):
    mean = jnp.mean(values, axis=-1, keepdims=True)
    centred = values - mean
    var = jnp.mean(centred * centred, axis=-1, keepdims=True)
    return centred * lax.rsqrt(var + 1e-05) * gain


def unit(i):
    k = i - 9
    b, c = i // 4, lax.rem(i, 4)
    b, c = jnp.where(i < 32, i - 24, b), jnp.where(i < 32, 3, c)
    b, c = jnp.where(i < 24, 7, b), jnp.where(i < 24, i - 21, c)
    b, c = jnp.where(i < 21, 3, b), jnp.where(i < 21, i - 18, c)
    b, c = jnp.where(i < 18, 4 + k // 3, b), jnp.where(i < 18, lax.rem(k, 3), c)
    return jnp.where(i < 9, lax.rem(i, 3), b), jnp.where(i < 9, i // 3, c)


def sweep(rows, queries, keys, vals, acc, probs, unroll, stages):
    total = 64

    def place(i):
        b, c = unit(i)
        return b, pl.ds(pl.multiple_of(c * WIDE, WIDE), WIDE)

    def scores(i, slot):
        b, cols = place(i)
        s = jnp.dot(keys[b, 0:rows], queries[:, cols], preferred_element_type=jnp.float32)
        probs[slot, 0:rows, :] = jnp.exp2(s).astype(jnp.bfloat16)

    def product(i, slot):
        b, cols = place(i)
        acc[:, cols] += jnp.dot(vals[b], probs[slot], preferred_element_type=jnp.float32)

    scores(jnp.int32(0), 0)

    def body(j, _):
        for k, stage in stages.items():

            @pl.when(j == k)
            def _(stage=stage):
                stage()

        for u in range(unroll):
            i = unroll * j + u
            ahead = i + 1 if u < unroll - 1 else jnp.minimum(i + 1, total - 1)
            scores(ahead, (u + 1) % 2)
            product(i, u % 2)
        return 0

    lax.fori_loop(0, total // unroll, body, 0)


ORDER = (0, 1, 3, 2)


def load_block(rows, kv, b, keys, vals):
    lane = lax.broadcasted_iota(jnp.int32, (16, PAD), 1)
    sub = lax.broadcasted_iota(jnp.int32, (16, PAD), 0)
    count = ((sub == 0) & (lane < rows)).astype(jnp.float32).astype(jnp.bfloat16)
    shift = (sub == 0).astype(jnp.float32).astype(jnp.bfloat16)
    zeros = jnp.zeros((64, PAD), jnp.bfloat16)
    keys[b] = jnp.concatenate([kv[0], shift, zeros], axis=0).T
    vals[b, 0:HD] = kv[1]
    vals[b, HD : HD + 16] = count


def attend_kernel(
    tokens, gain, w_in, w_own, acc, land, kvx, w_all, tok, normed, qkv, queries, keys, vals, probs, send, recv, local
):
    rows = tok.shape[0]
    width = queries.shape[1]
    seq, me = lax.axis_index("seq"), lax.axis_index("tensor")
    z, y, core = seq // 8, lax.rem(seq // 2, 4), lax.rem(seq, 2)
    links = Links(send, recv)
    fetch = pltpu.make_async_copy(tokens, tok, local.at[0])
    fetch.start()
    keep = pltpu.make_async_copy(w_own, w_all.at[me], local.at[1])
    keep.start()

    def on_seq(dz, dy, dc):
        return ((lax.rem(z + dz, 2) * 4 + lax.rem(y + dy, 4)) * 2 + lax.rem(core + dc, 2), me)

    barrier = pltpu.get_barrier_semaphore()
    peers = [on_seq(0, d, 0) for d in (1, 2, 3)] + [on_seq(0, 0, 1), on_seq(1, 0, 0)]
    peers += [(seq, links.slot(1, 0)), (seq, links.slot(0, 1)), (seq, links.slot(0, 3))]
    for peer in peers:
        pl.semaphore_signal(barrier, inc=1, device_id=peer, device_id_type=MESH)

    step = rows // 5
    normed[rows:PAD, :] = jnp.zeros((PAD - rows, normed.shape[1]), jnp.bfloat16)
    fetch.wait()

    def norm_rows(i, _):
        at = pl.ds(pl.multiple_of(i * step, 16), step)
        normed[at, :] = layer_norm(tok[at, :].astype(jnp.float32), gain[...]).astype(jnp.bfloat16)
        return 0

    lax.fori_loop(0, 5, norm_rows, 0)
    span = w_in.shape[0] // 3
    wide = lax.dot_general(w_in[...], normed[...], (((1,), (1,)), ((), ())), preferred_element_type=jnp.float32)
    for p in range(3):
        part = wide[p * span : (p + 1) * span]
        if p == 0:
            part = part * (LOG2E / HD**0.5)
        qkv[p] = part.astype(jnp.bfloat16).reshape(4, HD, PAD)
    pl.semaphore_wait(barrier, 8)

    by_y = {}
    for d in (1, 3, 2):
        by_y[d] = links.start(lambda d=d: (qkv.at[:, lax.rem(y + d, 4)], land.at[d], on_seq(0, d, 0)))
    to_core, to_far, far_core, more = {}, {}, {}, {}
    to_core[0] = links.start(lambda: (qkv.at[1:3, y], kvx.at[0, 0], on_seq(0, 0, 1)))
    to_far[0] = links.start(lambda: (qkv.at[1:3, y], kvx.at[1, 0], on_seq(1, 0, 0)))

    w_cols = w_own.shape[2] // 2

    def tensor_at(dz, dx):
        return (seq, links.slot(dz, dx))

    def own_w(dz, dx):
        return links.start(lambda: (w_own.at[core], w_all.at[me, core], tensor_at(dz, dx)))

    def pass_w(slot, lo, hi, dz, dx):
        def ends():
            ref = w_all.at[links.slot(*slot), core, :, lo * w_cols : hi * w_cols]
            return ref, ref, tensor_at(dz, dx)

        return links.start(ends)

    def swap_w(slot):
        def ends():
            ref = w_all.at[links.slot(*slot), core]
            return ref, ref, on_seq(0, 0, 1)

        return links.start(ends)

    wz, wup, wdown = own_w(1, 0), own_w(0, 1), own_w(0, 3)

    def set_queries(i):
        cols = slice(i * PAD, (i + 1) * PAD)
        queries[0:HD, cols] = land[ORDER[i], 0]
        queries[HD:128, cols] = jnp.zeros((128 - HD, PAD), jnp.bfloat16)
        s = jnp.dot(keys[0, 0:rows], queries[:, cols], preferred_element_type=jnp.float32)
        top = jnp.max(s.reshape(rows // 8, 8, PAD), axis=0)
        top = jnp.max(top, axis=0, keepdims=True)
        first = lax.broadcasted_iota(jnp.int32, (16, PAD), 0) == 0
        shift = jnp.where(first, jnp.broadcast_to(-top, (16, PAD)), 0.0)
        queries[HD : HD + 16, cols] = shift.astype(jnp.bfloat16)

    def arrive(i):
        d = ORDER[i]
        by_y[d].wait_recv()
        to_core[d] = links.start(lambda: (land.at[d, 1:3], kvx.at[0, d], on_seq(0, 0, 1)))
        to_far[d] = links.start(lambda: (land.at[d, 1:3], kvx.at[1, d], on_seq(1, 0, 0)))
        load_block(rows, land.at[d, 1:3], i, keys, vals)
        set_queries(i)

    def take(block):
        group, d = block // 4, ORDER[block % 4]
        if group == 1:
            to_core[d].wait_recv()
        elif group == 2:
            to_far[d].wait_recv()
            far_core[d] = links.start(lambda: (kvx.at[1, d], kvx.at[2, d], on_seq(0, 0, 1)))
        elif group == 3:
            far_core[d].wait_recv()
        load_block(rows, kvx.at[group - 1, d], block, keys, vals)

    others = [(0, 1), (0, 2), (0, 3), (1, 0), (1, 1), (1, 2), (1, 3)]

    def w_first():
        wz.wait_recv()
        more["zup"] = pass_w((1, 0), 0, 2, 0, 1)
        more["zdown"] = pass_w((1, 0), 0, 2, 0, 3)
        wup.wait_recv()
        more["r0"] = pass_w((0, 3), 0, 1, 0, 1)
        wdown.wait_recv()
        more["r1"] = pass_w((0, 1), 1, 2, 0, 3)

    def w_second():
        more["zup"].wait_recv()
        more["q0"] = pass_w((1, 3), 0, 1, 0, 1)
        more["zdown"].wait_recv()
        more["q1"] = pass_w((1, 1), 1, 2, 0, 3)

    def w_third():
        for name in ("r0", "r1", "q0", "q1"):
            more[name].wait_recv()
        for pair in others:
            more[pair] = swap_w(pair)

    def both(*steps):
        def run():
            for function, *args in steps:
                function(*args)

        return run

    stages = {
        0: both((arrive, 1), (arrive, 2)),
        2: both((take, 4), (take, 5)),
        3: both((take, 6),),
        4: both((arrive, 3), (w_first,)),
        5: both((take, 7),),
        7: both((take, 8),),
        8: both((take, 9), (w_second,)),
        9: both((take, 10),),
        10: both((take, 11),),
        11: both((take, 12),),
        12: both((take, 13), (w_third,)),
        13: both((take, 14),),
        14: both((take, 15),),
    }
    land[0] = qkv[:, y]
    load_block(rows, land.at[0, 1:3], 0, keys, vals)
    acc[...] = jnp.zeros_like(acc)
    probs[:, rows:PAD, :] = jnp.zeros((2, PAD - rows, WIDE), jnp.bfloat16)
    set_queries(0)
    sweep(rows, queries, keys, vals, acc, probs, 4, stages)
    keep.wait()
    for pair in others:
        more[pair].wait_recv()
    links.drain()


def settle_kernel(rows, acc_in, land, kvx, o_ref, queries, keys, vals, probs, acc):
    width = acc_in.shape[1]
    total = acc_in[HD : HD + 1, :]
    fits = jnp.where((total < LIMIT) & (total > FLOOR), 0.0, 1.0)
    again = jnp.max(fits) > 0.5

    def write(sums):
        for i, d in enumerate(ORDER):
            cols = slice(i * PAD, (i + 1) * PAD)
            o_ref[d] = (sums[0:HD, cols] / sums[HD : HD + 1, cols]).astype(jnp.bfloat16)

    @pl.when(jnp.logical_not(again))
    def _():
        write(acc_in)

    @pl.when(again)
    def _():
        queries[HD:128, :] = jnp.zeros((128 - HD, width), jnp.bfloat16)
        for i, d in enumerate(ORDER):
            queries[0:HD, i * PAD : (i + 1) * PAD] = land[d, 0]
        probs[rows:PAD, :] = jnp.zeros((PAD - rows, 256), jnp.bfloat16)
        acc[...] = jnp.zeros_like(acc)

        def fill(d, _):
            load_block(rows, land.at[d, 1:3], d, keys, vals)
            for g in range(3):
                load_block(rows, kvx.at[g, d], 4 * g + 4 + d, keys, vals)
            return 0

        lax.fori_loop(0, 4, fill, 0)

        def chunk(c, _):
            cols = pl.ds(pl.multiple_of(c * 256, 256), 256)

            def block(b, carry):
                peak, sums = carry
                s = jnp.dot(keys[b, 0:rows], queries[:, cols], preferred_element_type=jnp.float32)
                fresh = jnp.maximum(peak, jnp.max(s, axis=0, keepdims=True))
                probs[0:rows, :] = jnp.exp2(s - fresh).astype(jnp.bfloat16)
                part = jnp.dot(vals[b], probs[...], preferred_element_type=jnp.float32)
                return fresh, sums * jnp.exp2(peak - fresh) + part

            start = (jnp.full((1, 256), -1e30, jnp.float32), jnp.zeros((HD + 16, 256), jnp.float32))
            _, sums = lax.fori_loop(0, 16, block, start)
            acc[:, cols] = sums
            return 0

        lax.fori_loop(0, width // 256, chunk, 0)
        write(acc)


def attention(tokens, gain, w_qkv, w_out):
    rows, features = tokens.shape
    width = 4 * PAD
    bf16 = jnp.bfloat16
    half, cols = w_out.shape[0] // 2, w_out.shape[1]
    n = 48
    tables = [
        pltpu.VMEM((128, width), bf16),
        pltpu.VMEM((16, PAD, 128), bf16),
        pltpu.VMEM((16, HD + 16, PAD), bf16),
    ]
    anywhere = pl.BlockSpec(memory_space=pl.ANY)
    acc, land, kvx, w_all = pl.pallas_call(
        attend_kernel,
        out_shape=(
            jax.ShapeDtypeStruct((HD + 16, width), jnp.float32),
            jax.ShapeDtypeStruct((4, 3, HD, PAD), bf16),
            jax.ShapeDtypeStruct((3, 4, 2, HD, PAD), bf16),
            jax.ShapeDtypeStruct((8, 2, half, cols), bf16),
        ),
        in_specs=[anywhere, FULL, FULL, FULL],
        out_specs=(FULL, FULL, FULL, anywhere),
        scratch_shapes=[
            pltpu.VMEM(tokens.shape, bf16),
            pltpu.VMEM((PAD, features), bf16),
            pltpu.VMEM((3, 4, HD, PAD), bf16),
        ]
        + tables
        + [
            pltpu.VMEM((2, PAD, WIDE), bf16),
            pltpu.SemaphoreType.DMA((n,)),
            pltpu.SemaphoreType.DMA((n,)),
            pltpu.SemaphoreType.DMA((2,)),
        ],
        compiler_params=pltpu.CompilerParams(collective_id=0, has_side_effects=True, vmem_limit_bytes=48 * 2**20),
        name="attend",
    )(
        tokens,
        gain.reshape(1, features),
        jnp.transpose(w_qkv, (1, 2, 0)).reshape(3 * w_qkv.shape[2], features),
        w_out.reshape(2, half, cols),
    )
    o = pl.pallas_call(
        functools.partial(settle_kernel, rows),
        out_shape=jax.ShapeDtypeStruct((4, HD, PAD), bf16),
        in_specs=[FULL] * 3,
        out_specs=FULL,
        scratch_shapes=tables + [pltpu.VMEM((PAD, 256), bf16), pltpu.VMEM((HD + 16, width), jnp.float32)],
        compiler_params=pltpu.CompilerParams(vmem_limit_bytes=40 * 2**20),
        name="settle",
    )(acc, land, kvx)
    return o, w_all.reshape(16 * half, cols)


class Links:
    def __init__(self, send, recv):
        me = lax.axis_index("tensor")
        self.seq = lax.axis_index("seq")
        self.z, self.x = me // 4, lax.rem(me, 4)
        self.me = me
        self.send, self.recv = send, recv
        self.count = 0
        self.open = []

    def slot(self, dz, dx):
        z = lax.rem(self.z + dz, 2)
        return z * 4 + lax.rem(self.x + dx, 4)

    def barrier(self, more=0):
        sem = pltpu.get_barrier_semaphore()
        for dz, dx in ((1, 0), (0, 1), (0, 3)):
            pl.semaphore_signal(sem, inc=1, device_id=(self.seq, self.slot(dz, dx)), device_id_type=MESH)
        pl.semaphore_wait(sem, 3 + more)

    def put(self, src, dst, dz, dx):
        device = (self.seq, self.slot(dz, dx))
        return self.start(lambda: (src, dst, device))

    def start(self, ends):
        copy = Copy(self, self.count, ends)
        self.count += 1
        self.open.append(copy)
        copy.make().start()
        return copy

    def drain(self):
        for copy in self.open:
            copy.make().wait_send()
        self.open = []


class Copy:
    def __init__(self, links, index, ends):
        self.links, self.index, self.ends = links, index, ends

    def make(self):
        src, dst, device = self.ends()
        return pltpu.make_async_remote_copy(
            src_ref=src,
            dst_ref=dst,
            send_sem=self.links.send.at[self.index],
            recv_sem=self.links.recv.at[self.index],
            device_id=device,
            device_id_type=MESH,
        )

    def wait_recv(self):
        self.make().wait_recv()


def gather_tensor(links, piece, ready=lambda dz, dx: None):
    s = links.slot
    put = links.put

    def pass_on(slot, lo, hi, dz, dx):
        ref = piece(slot, lo, hi)
        return put(ref, ref, dz, dx)

    me = s(0, 0)
    a_z = pass_on(me, 0, 2, 1, 0)
    b_up = pass_on(me, 2, 4, 0, 1)
    b_down = pass_on(me, 2, 4, 0, 3)
    b_z = pass_on(me, 2, 4, 1, 0)
    a_up = pass_on(me, 0, 2, 0, 1)
    a_down = pass_on(me, 0, 2, 0, 3)
    ready(0, 0)
    b_up.wait_recv()
    r2 = pass_on(s(0, 3), 2, 3, 0, 1)
    bz_lo = pass_on(s(0, 3), 2, 4, 1, 0)
    b_down.wait_recv()
    r3 = pass_on(s(0, 1), 3, 4, 0, 3)
    bz_hi = pass_on(s(0, 1), 2, 4, 1, 0)
    a_z.wait_recv()
    az_up = pass_on(s(1, 0), 0, 2, 0, 1)
    az_down = pass_on(s(1, 0), 0, 2, 0, 3)
    a_up.wait_recv()
    r0 = pass_on(s(0, 3), 0, 1, 0, 1)
    a_down.wait_recv()
    r1 = pass_on(s(0, 1), 1, 2, 0, 3)
    ready(0, 3)
    r2.wait_recv()
    bz_2 = pass_on(s(0, 2), 2, 3, 1, 0)
    r3.wait_recv()
    bz_3 = pass_on(s(0, 2), 3, 4, 1, 0)
    ready(0, 1)
    az_up.wait_recv()
    q0 = pass_on(s(1, 3), 0, 1, 0, 1)
    az_down.wait_recv()
    q1 = pass_on(s(1, 1), 1, 2, 0, 3)
    b_z.wait_recv()
    ready(1, 0)
    r0.wait_recv()
    r1.wait_recv()
    ready(0, 2)
    bz_lo.wait_recv()
    ready(1, 3)
    bz_hi.wait_recv()
    ready(1, 1)
    for copy in (bz_2, bz_3, q0, q1):
        copy.wait_recv()
    ready(1, 2)
    links.drain()


GATHER_COPIES = 18


def reduce_tensor(links, term, stage, rows, cols, make):
    quarter = cols // 4
    s = links.slot
    put = links.put

    def q(slot, lo, hi):
        return term.at[slot, :, lo * quarter : hi * quarter]

    def val(slot, lo, hi):
        return term[slot, :, lo * quarter : hi * quarter].astype(jnp.float32)

    def land(i, n):
        return stage.at[i, :, 0 : n * quarter]

    def got(i, lo, hi):
        return stage[i, :, lo * quarter : hi * quarter].astype(jnp.float32)

    def add_into(slot, lo, hi, *parts):
        total = val(slot, lo, hi)
        for part in parts:
            total = total + part
        term[slot, :, lo * quarter : hi * quarter] = total.astype(jnp.bfloat16)

    zb, fa, near = {}, {}, {}

    def cross(i, dx):
        zb[dx] = put(q(s(1, dx), 2, 4), land(i, 2), 1, 0)

    def far(j, dz):
        fa[dz, 0] = put(q(s(dz, 2), 0, 1), land(4 + j, 1), 0, 3)
        fa[dz, 1] = put(q(s(dz, 2), 1, 2), land(6 + j, 1), 0, 1)

    def relay(j, dz):
        fa[dz, 0].wait_recv()
        add_into(s(dz, 3), 0, 1, got(4 + j, 0, 1))
        near[dz, 3] = put(q(s(dz, 3), 0, 2), land(8 + j, 2), 0, 3)
        fa[dz, 1].wait_recv()
        add_into(s(dz, 1), 1, 2, got(6 + j, 0, 1))
        near[dz, 1] = put(q(s(dz, 1), 0, 2), land(10 + j, 2), 0, 1)

    make((1, 2), (1, 0))
    cross(0, 2)
    far(0, 1)
    far(1, 0)
    make((1, 1), (0, 2))
    cross(1, 1)
    cross(2, 3)
    relay(0, 1)
    make((0, 1), (0, 2))
    relay(1, 0)
    zb[2].wait_recv()
    add_into(s(0, 2), 2, 4, got(0, 0, 2))
    fb0 = put(q(s(0, 2), 2, 3), land(12, 1), 0, 3)
    fb1 = put(q(s(0, 2), 3, 4), land(13, 1), 0, 1)
    make((1, 0), (1, 0))
    cross(3, 0)
    zb[1].wait_recv()
    zb[3].wait_recv()
    near[1, 3].wait_recv()
    near[1, 1].wait_recv()
    add_into(s(1, 0), 0, 2, got(8, 0, 2), got(10, 0, 2))
    za = put(q(s(1, 0), 0, 2), land(14, 2), 1, 0)
    fb0.wait_recv()
    add_into(s(0, 3), 2, 3, got(2, 0, 1), got(12, 0, 1))
    add_into(s(0, 3), 3, 4, got(2, 1, 2))
    nb3 = put(q(s(0, 3), 2, 4), land(15, 2), 0, 3)
    fb1.wait_recv()
    add_into(s(0, 1), 3, 4, got(1, 1, 2), got(13, 0, 1))
    add_into(s(0, 1), 2, 3, got(1, 0, 1))
    nb1 = put(q(s(0, 1), 2, 4), land(16, 2), 0, 1)
    near[0, 3].wait_recv()
    near[0, 1].wait_recv()
    za.wait_recv()
    first = val(s(0, 0), 0, 2) + got(9, 0, 2) + got(11, 0, 2) + got(14, 0, 2)
    zb[0].wait_recv()
    nb3.wait_recv()
    nb1.wait_recv()
    second = val(s(0, 0), 2, 4) + got(3, 0, 2) + got(15, 0, 2) + got(16, 0, 2)
    links.drain()
    return first, second


def tail_kernel(
    o_ref, w_out, tok, gain, w_up, w_down, out_ref, every, mixed, post, term, stage, wo, wu, wd, send, recv, local
):
    links = Links(send, recv)
    seq, me = links.seq, links.me
    y = lax.rem(seq // 2, 4)
    share, width = out_ref.shape[1], out_ref.shape[2]
    quarter = width // 4
    rows = tok.shape[0]
    loads = [
        pltpu.make_async_copy(src, dst, local.at[i])
        for i, (src, dst) in enumerate(((w_out, wo), (w_up, wu), (w_down, wd)))
    ]
    for load in loads:
        load.start()

    def at_y(dy):
        return ((seq // 8 * 4 + lax.rem(y + dy, 4)) * 2 + lax.rem(seq, 2), me)

    sem = pltpu.get_barrier_semaphore()
    for d in (1, 2, 3):
        pl.semaphore_signal(sem, inc=1, device_id=at_y(d), device_id_type=MESH)
    links.barrier(3)
    back = [links.start(lambda d=d: (o_ref.at[d], every.at[me, y], at_y(4 - d))) for d in (2, 1, 3)]
    every[me, y] = o_ref[0]
    mixed[0:rows, :] = tok[...].astype(jnp.float32)
    mixed[rows:, :] = jnp.zeros((PAD - rows, width), jnp.float32)
    loads[0].wait()
    for copy in back:
        copy.wait_recv()

    def project(dz, dx):
        slot = links.slot(dz, dx)

        def tile(i, _):
            at = pl.ds(pl.multiple_of(i * 256, 256), 256)
            left = every[slot, :, :, at].reshape(4 * HD, 256)
            mixed[at, :] += lax.dot_general(
                left, wo[slot], (((0,), (0,)), ((), ())), preferred_element_type=jnp.float32
            )
            return 0

        lax.fori_loop(0, PAD // 256, tile, 0)

    gather_tensor(links, lambda slot, lo, hi: every.at[slot, lo:hi], project)
    loads[1].wait()
    loads[2].wait()

    def feed_forward(start, step):
        def block(k, _):
            slot = links.slot(start[0] + step[0] * k, start[1] + step[1] * k)
            at = pl.ds(pl.multiple_of(slot * share, 32), share)
            post[...] = layer_norm(mixed[at, :], gain[...]).astype(jnp.bfloat16)
            up = jnp.dot(post[...], wu[...], preferred_element_type=jnp.float32)
            hidden = jax.nn.gelu(up, approximate=True).astype(jnp.bfloat16)
            down = jnp.dot(hidden, wd[...], preferred_element_type=jnp.float32)
            term[slot] = down.astype(jnp.bfloat16)
            return 0

        lax.fori_loop(0, 2, block, 0)

    first, second = reduce_tensor(links, term, stage, share, width, feed_forward)
    at = pl.ds(pl.multiple_of(me * share, 32), share)
    out_ref[me, :, 0 : 2 * quarter] = (mixed[at, 0 : 2 * quarter] + first).astype(jnp.bfloat16)
    out_ref[me, :, 2 * quarter :] = (mixed[at, 2 * quarter :] + second).astype(jnp.bfloat16)
    gather_tensor(links, lambda slot, lo, hi: out_ref.at[slot, :, lo * quarter : hi * quarter])


def tail(o, w_out, tokens, gain, w_up, w_down):
    rows, cols = tokens.shape
    share = PAD // 8
    copies = 64
    bf16 = jnp.bfloat16
    anywhere = pl.BlockSpec(memory_space=pl.ANY)
    return pl.pallas_call(
        tail_kernel,
        out_shape=jax.ShapeDtypeStruct((8, share, cols), bf16),
        in_specs=[FULL, anywhere, FULL, FULL, anywhere, anywhere],
        out_specs=FULL,
        scratch_shapes=[
            pltpu.VMEM((8,) + o.shape, bf16),
            pltpu.VMEM((PAD, cols), jnp.float32),
            pltpu.VMEM((share, cols), bf16),
            pltpu.VMEM((8, share, cols), bf16),
            pltpu.VMEM((17, share, cols // 2), bf16),
            pltpu.VMEM(w_out.shape, bf16),
            pltpu.VMEM(w_up.shape, bf16),
            pltpu.VMEM(w_down.shape, bf16),
            pltpu.SemaphoreType.DMA((copies,)),
            pltpu.SemaphoreType.DMA((copies,)),
            pltpu.SemaphoreType.DMA((3,)),
        ],
        compiler_params=pltpu.CompilerParams(collective_id=1, has_side_effects=True, vmem_limit_bytes=48 * 2**20),
        name="tail",
    )(o, w_out, tokens, gain, w_up, w_down)


def per_device(tokens, norm_gain, w_qkv, w_out, post_gain, w_up, w_down):
    rows, width = tokens.shape
    heads = w_qkv.shape[2] // HD
    o, w_out_all = attention(tokens, norm_gain, w_qkv, w_out)
    out = tail(o, w_out_all.reshape(8, heads * HD, width), tokens, post_gain.reshape(1, width), w_up, w_down)
    return out.reshape(PAD, width)[:rows]


def solution(mesh):
    placed = (
        P("seq", None),
        P(),
        P(None, None, "tensor"),
        P("tensor", None),
        P(),
        P(None, "tensor"),
        P("tensor", None),
    )
    return jax.shard_map(
        per_device, mesh=mesh, in_specs=placed, out_specs=P("seq", None), check_vma=False
    )
```

```python
import functools

import jax
import jax.numpy as jnp
from jax import lax
from jax.experimental import pallas as pl
from jax.experimental.pallas import tpu as pltpu
from jax.sharding import PartitionSpec as P

HD = 48
PAD = 768
WIDE = PAD
MESH = pl.DeviceIdType.MESH
LOG2E = 1.4426950408889634
LIMIT = 2.0**90
FLOOR = 2.0**-20
FULL = pl.BlockSpec(memory_space=pltpu.VMEM)


def layer_norm(values, gain):
    mean = jnp.mean(values, axis=-1, keepdims=True)
    centred = values - mean
    var = jnp.mean(centred * centred, axis=-1, keepdims=True)
    return centred * lax.rsqrt(var + 1e-05) * gain


def wide_row(ref):
    return jnp.concatenate([ref[k : k + 1, :] for k in range(ref.shape[0])], axis=1)


EARLY = [(b, c) for b in (0, 1, 2, 4, 5, 6, 3, 7) for c in range(3)] + [(b, 3) for b in range(8)]


def sweep(rows, queries, keys, vals, acc, probs, early, late):
    def scores(unit, slot):
        b, c = unit
        cols = slice(c * WIDE, (c + 1) * WIDE)
        cut = rows // 32 * 16
        for lo, hi in ((0, cut), (cut, rows)):
            s = jnp.dot(keys[b, lo:hi], queries[:, cols], preferred_element_type=jnp.float32)
            probs[slot, lo:hi, :] = jnp.exp2(s).astype(jnp.bfloat16)

    def product(unit, slot):
        b, c = unit
        cols = slice(c * WIDE, (c + 1) * WIDE)
        acc[:, cols] += jnp.dot(vals[b], probs[slot], preferred_element_type=jnp.float32)

    scores(EARLY[0], 0)
    order = EARLY + [(8, 0)]
    for n, pair in enumerate(EARLY):
        if n + 1 in early:
            early[n + 1]()
        scores(order[n + 1], (n + 1) % 2)
        product(pair, n % 2)

    def body(j, _):
        late(j)
        for c in range(4):
            scores((8 + j, c + 1) if c < 3 else (jnp.minimum(9 + j, 15), 0), (c + 1) % 2)
            product((8 + j, c), c % 2)
        return 0

    lax.fori_loop(0, 8, body, 0)


ORDER = (0, 1, 3, 2)


def load_block(rows, kv, b, keys, vals):
    lane = lax.broadcasted_iota(jnp.int32, (16, PAD), 1)
    sub = lax.broadcasted_iota(jnp.int32, (16, PAD), 0)
    count = ((sub == 0) & (lane < rows)).astype(jnp.float32).astype(jnp.bfloat16)
    shift = (sub == 0).astype(jnp.float32).astype(jnp.bfloat16)
    zeros = jnp.zeros((64, PAD), jnp.bfloat16)
    keys[b] = jnp.concatenate([kv[0], shift, zeros], axis=0).T
    vals[b, 0:HD] = kv[1]
    vals[b, HD : HD + 16] = count


def attend_kernel(
    tokens, gain, w_in, w_ref, acc, land_out, kvx_out, w_all,
    tok, wq, w_own, normed, qkv, land, kvx, queries, keys, vals, probs, send, recv, local,
):
    rows = tok.shape[0]
    width = queries.shape[1]
    seq, me = lax.axis_index("seq"), lax.axis_index("tensor")
    z, y, core = seq // 8, lax.rem(seq // 2, 4), lax.rem(seq, 2)
    links = Links(send, recv)
    fetch = [
        pltpu.make_async_copy(src, dst, local.at[i])
        for i, (src, dst) in enumerate(((tokens, tok), (w_in, wq), (w_ref, w_own)))
    ]
    for copy in fetch:
        copy.start()

    def keep(i):
        src, dst = (
            (w_own, w_all.at[me]),
            (land, land_out),
            (kvx.at[0], kvx_out.at[0]),
            (kvx.at[1], kvx_out.at[1]),
            (kvx.at[2], kvx_out.at[2]),
        )[i]
        return pltpu.make_async_copy(src, dst, local.at[3 + i])


    def on_seq(dz, dy, dc):
        return ((lax.rem(z + dz, 2) * 4 + lax.rem(y + dy, 4)) * 2 + lax.rem(core + dc, 2), me)

    barrier = pltpu.get_barrier_semaphore()
    peers = [on_seq(0, d, 0) for d in (1, 2, 3)] + [on_seq(0, 0, 1), on_seq(1, 0, 0)]
    peers += [(seq, links.slot(1, 0)), (seq, links.slot(0, 1)), (seq, links.slot(0, 3))]
    for peer in peers:
        pl.semaphore_signal(barrier, inc=1, device_id=peer, device_id_type=MESH)

    step = rows // 5
    normed[rows:PAD, :] = jnp.zeros((PAD - rows, normed.shape[1]), jnp.bfloat16)
    fetch[0].wait()

    scale = wide_row(gain)

    def norm_rows(i, _):
        at = pl.ds(pl.multiple_of(i * step, 16), step)
        normed[at, :] = layer_norm(tok[at, :].astype(jnp.float32), scale).astype(jnp.bfloat16)
        return 0

    lax.fori_loop(0, 5, norm_rows, 0)
    fetch[1].wait()
    span = w_in.shape[0] // 3
    wide = lax.dot_general(wq[...], normed[...], (((1,), (1,)), ((), ())), preferred_element_type=jnp.float32)
    for p in range(3):
        part = wide[p * span : (p + 1) * span]
        if p == 0:
            part = part * (LOG2E / HD**0.5)
        qkv[p] = part.astype(jnp.bfloat16).reshape(4, HD, PAD)
    pl.semaphore_wait(barrier, 8)

    by_y = {}
    for d in (1, 3, 2):
        by_y[d] = links.start(lambda d=d: (qkv.at[:, lax.rem(y + d, 4)], land.at[d], on_seq(0, d, 0)))
    to_core, to_far, far_core, more = {}, {}, {}, {}
    to_core[0] = links.start(lambda: (qkv.at[1:3, y], kvx.at[0, 0], on_seq(0, 0, 1)))
    to_far[0] = links.start(lambda: (qkv.at[1:3, y], kvx.at[1, 0], on_seq(1, 0, 0)))

    fetch[2].wait()
    keep(0).start()
    w_cols = w_own.shape[2] // 2

    def tensor_at(dz, dx):
        return (seq, links.slot(dz, dx))

    def own_w(dz, dx):
        return links.start(lambda: (w_own.at[core], w_all.at[me, core], tensor_at(dz, dx)))

    def pass_w(slot, lo, hi, dz, dx):
        def ends():
            ref = w_all.at[links.slot(*slot), core, :, lo * w_cols : hi * w_cols]
            return ref, ref, tensor_at(dz, dx)

        return links.start(ends)

    def swap_w(slot):
        def ends():
            ref = w_all.at[links.slot(*slot), core]
            return ref, ref, on_seq(0, 0, 1)

        return links.start(ends)

    wz, wup, wdown = own_w(1, 0), own_w(0, 1), own_w(0, 3)

    def set_queries(i):
        cols = slice(i * PAD, (i + 1) * PAD)
        queries[0:HD, cols] = land[ORDER[i], 0]
        queries[HD:128, cols] = jnp.zeros((128 - HD, PAD), jnp.bfloat16)
        s = jnp.dot(keys[0, 0:rows], queries[:, cols], preferred_element_type=jnp.float32)
        top = jnp.max(s.reshape(rows // 8, 8, PAD), axis=0)
        top = jnp.max(top, axis=0, keepdims=True)
        first = lax.broadcasted_iota(jnp.int32, (16, PAD), 0) == 0
        shift = jnp.where(first, jnp.broadcast_to(-top, (16, PAD)), 0.0)
        queries[HD : HD + 16, cols] = shift.astype(jnp.bfloat16)

    def arrive(i):
        d = ORDER[i]
        by_y[d].wait_recv()
        to_core[d] = links.start(lambda: (land.at[d, 1:3], kvx.at[0, d], on_seq(0, 0, 1)))
        to_far[d] = links.start(lambda: (land.at[d, 1:3], kvx.at[1, d], on_seq(1, 0, 0)))
        load_block(rows, land.at[d, 1:3], i, keys, vals)
        set_queries(i)

    def take(block):
        group, d = block // 4, ORDER[block % 4]
        if group == 1:
            to_core[d].wait_recv()
        elif group == 2:
            to_far[d].wait_recv()
            far_core[d] = links.start(lambda: (kvx.at[1, d], kvx.at[2, d], on_seq(0, 0, 1)))
        elif group == 3:
            far_core[d].wait_recv()
        load_block(rows, kvx.at[group - 1, d], block, keys, vals)

    others = [(0, 1), (0, 2), (0, 3), (1, 0), (1, 1), (1, 2), (1, 3)]

    def w_first():
        wz.wait_recv()
        more["zup"] = pass_w((1, 0), 0, 2, 0, 1)
        more["zdown"] = pass_w((1, 0), 0, 2, 0, 3)
        wup.wait_recv()
        more["r0"] = pass_w((0, 3), 0, 1, 0, 1)
        wdown.wait_recv()
        more["r1"] = pass_w((0, 1), 1, 2, 0, 3)

    def w_second():
        more["zup"].wait_recv()
        more["q0"] = pass_w((1, 3), 0, 1, 0, 1)
        more["zdown"].wait_recv()
        more["q1"] = pass_w((1, 1), 1, 2, 0, 3)

    def w_third():
        for name in ("r0", "r1", "q0", "q1"):
            more[name].wait_recv()
        for pair in others:
            more[pair] = swap_w(pair)

    def both(*steps):
        def run():
            for function, *args in steps:
                function(*args)

        return run

    def store(i):
        keep(i).start()

    early = {
        1: both((arrive, 1), (arrive, 2)),
        9: both((take, 4),),
        12: both((take, 5),),
        15: both((take, 6),),
        18: both((arrive, 3), (w_first,), (store, 1)),
        21: both((take, 7), (store, 2)),
        32: both((take, 8),),
    }

    def landed(block):
        group, d = block // 4, ORDER[block % 4]
        if group == 2:
            to_far[d].wait_recv()
            far_core[d] = links.start(lambda: (kvx.at[1, d], kvx.at[2, d], on_seq(0, 0, 1)))
        else:
            far_core[d].wait_recv()

    def late(j):
        for k in range(7):

            @pl.when(j == k)
            def _(k=k):
                landed(9 + k)
                if k == 2:
                    store(3)
                if k == 6:
                    store(4)
                if k == 1:
                    w_second()
                if k == 4:
                    w_third()

        block = jnp.minimum(9 + j, 15)
        far = (block >= 12).astype(jnp.int32)
        i = block - 8 - 4 * far
        d = i + (i == 2).astype(jnp.int32) - (i == 3).astype(jnp.int32)
        load_block(rows, kvx.at[1 + far, d], block, keys, vals)

    land[0] = qkv[:, y]
    load_block(rows, land.at[0, 1:3], 0, keys, vals)
    acc[...] = jnp.zeros_like(acc)
    probs[:, rows:PAD, :] = jnp.zeros((2, PAD - rows, WIDE), jnp.bfloat16)
    set_queries(0)
    sweep(rows, queries, keys, vals, acc, probs, early, late)
    for i in range(5):
        keep(i).wait()
    for pair in others:
        more[pair].wait_recv()
    links.drain()


def settle_kernel(rows, acc_in, land_ref, kvx_ref, o_ref, land, kvx, queries, keys, vals, probs, acc, local):
    width = acc_in.shape[1]
    total = acc_in[HD : HD + 1, :]
    fits = jnp.where((total < LIMIT) & (total > FLOOR), 0.0, 1.0)
    again = jnp.max(fits) > 0.5

    def write(sums):
        for i, d in enumerate(ORDER):
            cols = slice(i * PAD, (i + 1) * PAD)
            o_ref[d] = (sums[0:HD, cols] / sums[HD : HD + 1, cols]).astype(jnp.bfloat16)

    @pl.when(jnp.logical_not(again))
    def _():
        write(acc_in)

    @pl.when(again)
    def _():
        loads = [
            pltpu.make_async_copy(land_ref, land, local.at[0]),
            pltpu.make_async_copy(kvx_ref, kvx, local.at[1]),
        ]
        for load in loads:
            load.start()
        for load in loads:
            load.wait()
        queries[HD:128, :] = jnp.zeros((128 - HD, width), jnp.bfloat16)
        for i, d in enumerate(ORDER):
            queries[0:HD, i * PAD : (i + 1) * PAD] = land[d, 0]
        probs[rows:PAD, :] = jnp.zeros((PAD - rows, 256), jnp.bfloat16)
        acc[...] = jnp.zeros_like(acc)

        def fill(d, _):
            load_block(rows, land.at[d, 1:3], d, keys, vals)
            for g in range(3):
                load_block(rows, kvx.at[g, d], 4 * g + 4 + d, keys, vals)
            return 0

        lax.fori_loop(0, 4, fill, 0)

        def chunk(c, _):
            cols = pl.ds(pl.multiple_of(c * 256, 256), 256)

            def block(b, carry):
                peak, sums = carry
                s = jnp.dot(keys[b, 0:rows], queries[:, cols], preferred_element_type=jnp.float32)
                fresh = jnp.maximum(peak, jnp.max(s, axis=0, keepdims=True))
                probs[0:rows, :] = jnp.exp2(s - fresh).astype(jnp.bfloat16)
                part = jnp.dot(vals[b], probs[...], preferred_element_type=jnp.float32)
                return fresh, sums * jnp.exp2(peak - fresh) + part

            start = (jnp.full((1, 256), -1e30, jnp.float32), jnp.zeros((HD + 16, 256), jnp.float32))
            _, sums = lax.fori_loop(0, 16, block, start)
            acc[:, cols] = sums
            return 0

        lax.fori_loop(0, width // 256, chunk, 0)
        write(acc)


def attention(tokens, gain, w_qkv, w_out):
    rows, features = tokens.shape
    width = 4 * PAD
    bf16 = jnp.bfloat16
    half, cols = w_out.shape[0] // 2, w_out.shape[1]
    n = 48
    tables = [
        pltpu.VMEM((128, width), bf16),
        pltpu.VMEM((16, PAD, 128), bf16),
        pltpu.VMEM((16, HD + 16, PAD), bf16),
    ]
    blocks = [pltpu.VMEM((4, 3, HD, PAD), bf16), pltpu.VMEM((3, 4, 2, HD, PAD), bf16)]
    anywhere = pl.BlockSpec(memory_space=pl.ANY)
    acc, land, kvx, w_all = pl.pallas_call(
        attend_kernel,
        out_shape=(
            jax.ShapeDtypeStruct((HD + 16, width), jnp.float32),
            jax.ShapeDtypeStruct((4, 3, HD, PAD), bf16),
            jax.ShapeDtypeStruct((3, 4, 2, HD, PAD), bf16),
            jax.ShapeDtypeStruct((8, 2, half, cols), bf16),
        ),
        in_specs=[anywhere, FULL, anywhere, anywhere],
        out_specs=(FULL, anywhere, anywhere, anywhere),
        scratch_shapes=[
            pltpu.VMEM(tokens.shape, bf16),
            pltpu.VMEM((3 * w_qkv.shape[2], features), bf16),
            pltpu.VMEM((2, half, cols), bf16),
            pltpu.VMEM((PAD, features), bf16),
            pltpu.VMEM((3, 4, HD, PAD), bf16),
        ]
        + blocks
        + tables
        + [
            pltpu.VMEM((2, PAD, WIDE), bf16),
            pltpu.SemaphoreType.DMA((n,)),
            pltpu.SemaphoreType.DMA((n,)),
            pltpu.SemaphoreType.DMA((8,)),
        ],
        compiler_params=pltpu.CompilerParams(collective_id=0, has_side_effects=True, vmem_limit_bytes=60 * 2**20),
        name="attend",
    )(
        tokens,
        gain.reshape(features // 128, 128),
        jnp.transpose(w_qkv, (1, 2, 0)).reshape(3 * w_qkv.shape[2], features),
        w_out.reshape(2, half, cols),
    )
    o = pl.pallas_call(
        functools.partial(settle_kernel, rows),
        out_shape=jax.ShapeDtypeStruct((4, HD, PAD), bf16),
        in_specs=[FULL, anywhere, anywhere],
        out_specs=FULL,
        scratch_shapes=blocks
        + tables
        + [
            pltpu.VMEM((PAD, 256), bf16),
            pltpu.VMEM((HD + 16, width), jnp.float32),
            pltpu.SemaphoreType.DMA((2,)),
        ],
        compiler_params=pltpu.CompilerParams(vmem_limit_bytes=60 * 2**20),
        name="settle",
    )(acc, land, kvx)
    return o, w_all.reshape(16 * half, cols)


class Links:
    def __init__(self, send, recv):
        me = lax.axis_index("tensor")
        self.seq = lax.axis_index("seq")
        self.z, self.x = me // 4, lax.rem(me, 4)
        self.me = me
        self.send, self.recv = send, recv
        self.count = 0
        self.open = []

    def slot(self, dz, dx):
        z = lax.rem(self.z + dz, 2)
        return z * 4 + lax.rem(self.x + dx, 4)

    def barrier(self, more=0):
        sem = pltpu.get_barrier_semaphore()
        for dz, dx in ((1, 0), (0, 1), (0, 3)):
            pl.semaphore_signal(sem, inc=1, device_id=(self.seq, self.slot(dz, dx)), device_id_type=MESH)
        pl.semaphore_wait(sem, 3 + more)

    def put(self, src, dst, dz, dx):
        device = (self.seq, self.slot(dz, dx))
        return self.start(lambda: (src, dst, device))

    def start(self, ends):
        copy = Copy(self, self.count, ends)
        self.count += 1
        self.open.append(copy)
        copy.make().start()
        return copy

    def drain(self):
        for copy in self.open:
            copy.make().wait_send()
        self.open = []


class Copy:
    def __init__(self, links, index, ends):
        self.links, self.index, self.ends = links, index, ends

    def make(self):
        src, dst, device = self.ends()
        return pltpu.make_async_remote_copy(
            src_ref=src,
            dst_ref=dst,
            send_sem=self.links.send.at[self.index],
            recv_sem=self.links.recv.at[self.index],
            device_id=device,
            device_id_type=MESH,
        )

    def wait_recv(self):
        self.make().wait_recv()


def gather_tensor(links, piece, ready=lambda dz, dx: None, between=lambda: None):
    s = links.slot
    put = links.put

    def pass_on(slot, lo, hi, dz, dx):
        ref = piece(slot, lo, hi)
        return put(ref, ref, dz, dx)

    me = s(0, 0)
    a_z = pass_on(me, 0, 2, 1, 0)
    a_up = pass_on(me, 0, 2, 0, 1)
    a_down = pass_on(me, 0, 2, 0, 3)
    between()
    b_up = pass_on(me, 2, 4, 0, 1)
    b_down = pass_on(me, 2, 4, 0, 3)
    b_z = pass_on(me, 2, 4, 1, 0)
    ready(0, 0)
    b_up.wait_recv()
    r2 = pass_on(s(0, 3), 2, 3, 0, 1)
    bz_lo = pass_on(s(0, 3), 2, 4, 1, 0)
    b_down.wait_recv()
    r3 = pass_on(s(0, 1), 3, 4, 0, 3)
    bz_hi = pass_on(s(0, 1), 2, 4, 1, 0)
    a_z.wait_recv()
    az_up = pass_on(s(1, 0), 0, 2, 0, 1)
    az_down = pass_on(s(1, 0), 0, 2, 0, 3)
    a_up.wait_recv()
    r0 = pass_on(s(0, 3), 0, 1, 0, 1)
    a_down.wait_recv()
    r1 = pass_on(s(0, 1), 1, 2, 0, 3)
    ready(0, 3)
    r2.wait_recv()
    bz_2 = pass_on(s(0, 2), 2, 3, 1, 0)
    r3.wait_recv()
    bz_3 = pass_on(s(0, 2), 3, 4, 1, 0)
    ready(0, 1)
    az_up.wait_recv()
    q0 = pass_on(s(1, 3), 0, 1, 0, 1)
    az_down.wait_recv()
    q1 = pass_on(s(1, 1), 1, 2, 0, 3)
    b_z.wait_recv()
    ready(1, 0)
    r0.wait_recv()
    r1.wait_recv()
    ready(0, 2)
    bz_lo.wait_recv()
    ready(1, 3)
    bz_hi.wait_recv()
    ready(1, 1)
    for copy in (bz_2, bz_3, q0, q1):
        copy.wait_recv()
    ready(1, 2)
    links.drain()


GATHER_COPIES = 18


def reduce_tensor(links, term, stage, rows, cols, make):
    quarter = cols // 4
    s = links.slot
    put = links.put

    def q(slot, lo, hi):
        return term.at[slot, :, lo * quarter : hi * quarter]

    def val(slot, lo, hi):
        return term[slot, :, lo * quarter : hi * quarter].astype(jnp.float32)

    def land(i, n):
        return stage.at[i, :, 0 : n * quarter]

    def got(i, lo, hi):
        return stage[i, :, lo * quarter : hi * quarter].astype(jnp.float32)

    def add_into(slot, lo, hi, *parts):
        total = val(slot, lo, hi)
        for part in parts:
            total = total + part
        term[slot, :, lo * quarter : hi * quarter] = total.astype(jnp.bfloat16)

    zb, fa, near = {}, {}, {}

    def cross(i, dx):
        zb[dx] = put(q(s(1, dx), 2, 4), land(i, 2), 1, 0)

    def far(j, dz):
        fa[dz, 0] = put(q(s(dz, 2), 0, 1), land(4 + j, 1), 0, 3)
        fa[dz, 1] = put(q(s(dz, 2), 1, 2), land(6 + j, 1), 0, 1)

    def relay(j, dz):
        fa[dz, 0].wait_recv()
        add_into(s(dz, 3), 0, 1, got(4 + j, 0, 1))
        near[dz, 3] = put(q(s(dz, 3), 0, 2), land(8 + j, 2), 0, 3)
        fa[dz, 1].wait_recv()
        add_into(s(dz, 1), 1, 2, got(6 + j, 0, 1))
        near[dz, 1] = put(q(s(dz, 1), 0, 2), land(10 + j, 2), 0, 1)

    make((1, 2), (0, 2))
    cross(0, 2)
    far(0, 1)
    far(1, 0)
    make((1, 1), (1, 3))
    cross(1, 1)
    cross(2, 3)
    relay(0, 1)
    make((0, 1), (0, 3))
    relay(1, 0)
    zb[2].wait_recv()
    add_into(s(0, 2), 2, 4, got(0, 0, 2))
    fb0 = put(q(s(0, 2), 2, 3), land(12, 1), 0, 3)
    fb1 = put(q(s(0, 2), 3, 4), land(13, 1), 0, 1)
    make((1, 0), (0, 0))
    cross(3, 0)
    zb[1].wait_recv()
    zb[3].wait_recv()
    near[1, 3].wait_recv()
    near[1, 1].wait_recv()
    add_into(s(1, 0), 0, 2, got(8, 0, 2), got(10, 0, 2))
    za = put(q(s(1, 0), 0, 2), land(14, 2), 1, 0)
    fb0.wait_recv()
    add_into(s(0, 3), 2, 3, got(2, 0, 1), got(12, 0, 1))
    add_into(s(0, 3), 3, 4, got(2, 1, 2))
    nb3 = put(q(s(0, 3), 2, 4), land(15, 2), 0, 3)
    fb1.wait_recv()
    add_into(s(0, 1), 3, 4, got(1, 1, 2), got(13, 0, 1))
    add_into(s(0, 1), 2, 3, got(1, 0, 1))
    nb1 = put(q(s(0, 1), 2, 4), land(16, 2), 0, 1)
    near[0, 3].wait_recv()
    near[0, 1].wait_recv()
    za.wait_recv()
    first = val(s(0, 0), 0, 2) + got(9, 0, 2) + got(11, 0, 2) + got(14, 0, 2)

    def second():
        zb[0].wait_recv()
        nb3.wait_recv()
        nb1.wait_recv()
        return val(s(0, 0), 2, 4) + got(3, 0, 2) + got(15, 0, 2) + got(16, 0, 2)

    return first, second


def tail_kernel(
    o_ref, w_out, tokens, gain, w_up, w_down, out_ref, every, mixed, post, term, stage, tok, wo, wu, wd, send, recv, local
):
    links = Links(send, recv)
    seq, me = links.seq, links.me
    y = lax.rem(seq // 2, 4)
    share, width = out_ref.shape[1], out_ref.shape[2]
    quarter = width // 4
    rows = tok.shape[0]
    loads = [
        pltpu.make_async_copy(src, dst, local.at[i])
        for i, (src, dst) in enumerate(((tokens, tok), (w_out, wo), (w_up, wu), (w_down, wd)))
    ]
    for load in loads:
        load.start()

    def at_y(dy):
        return ((seq // 8 * 4 + lax.rem(y + dy, 4)) * 2 + lax.rem(seq, 2), me)

    sem = pltpu.get_barrier_semaphore()
    for d in (1, 2, 3):
        pl.semaphore_signal(sem, inc=1, device_id=at_y(d), device_id_type=MESH)
    links.barrier(3)
    back = [links.start(lambda d=d: (o_ref.at[d], every.at[me, y], at_y(4 - d))) for d in (2, 1, 3)]
    every[me, y] = o_ref[0]
    loads[0].wait()
    mixed[0:rows, :] = tok[...].astype(jnp.float32)
    mixed[rows:, :] = jnp.zeros((PAD - rows, width), jnp.float32)
    loads[1].wait()
    for copy in back:
        copy.wait_recv()

    def project(dz, dx):
        slot = links.slot(dz, dx)

        def tile(i, _):
            at = pl.ds(pl.multiple_of(i * 256, 256), 256)
            left = every[slot, :, :, at].reshape(4 * HD, 256)
            mixed[at, :] += lax.dot_general(
                left, wo[slot], (((0,), (0,)), ((), ())), preferred_element_type=jnp.float32
            )
            return 0

        lax.fori_loop(0, PAD // 256, tile, 0)

    gather_tensor(links, lambda slot, lo, hi: every.at[slot, lo:hi], project)
    loads[2].wait()
    loads[3].wait()

    scale = wide_row(gain)

    def feed_forward(*pair):
        slots = [links.slot(*block) for block in pair]
        for k, slot in enumerate(slots):
            at = pl.ds(pl.multiple_of(slot * share, 32), share)
            post[k * share : (k + 1) * share, :] = layer_norm(mixed[at, :], scale).astype(jnp.bfloat16)
        up = jnp.dot(post[...], wu[...], preferred_element_type=jnp.float32)
        hidden = jax.nn.gelu(up, approximate=True).astype(jnp.bfloat16)
        for k in range(3):
            cols = slice(k * (width // 3), (k + 1) * (width // 3))
            down = jnp.dot(hidden, wd[:, cols], preferred_element_type=jnp.float32).astype(jnp.bfloat16)
            for i, slot in enumerate(slots):
                term[slot, :, cols] = down[i * share : (i + 1) * share]

    first, second = reduce_tensor(links, term, stage, share, width, feed_forward)
    at = pl.ds(pl.multiple_of(me * share, 32), share)
    out_ref[me, :, 0 : 2 * quarter] = (mixed[at, 0 : 2 * quarter] + first).astype(jnp.bfloat16)

    def rest():
        out_ref[me, :, 2 * quarter :] = (mixed[at, 2 * quarter :] + second()).astype(jnp.bfloat16)

    gather_tensor(links, lambda slot, lo, hi: out_ref.at[slot, :, lo * quarter : hi * quarter], between=rest)


def tail(o, w_out, tokens, gain, w_up, w_down):
    rows, cols = tokens.shape
    share = PAD // 8
    copies = 64
    bf16 = jnp.bfloat16
    anywhere = pl.BlockSpec(memory_space=pl.ANY)
    return pl.pallas_call(
        tail_kernel,
        out_shape=jax.ShapeDtypeStruct((8, share, cols), bf16),
        in_specs=[FULL, anywhere, anywhere, FULL, anywhere, anywhere],
        out_specs=FULL,
        scratch_shapes=[
            pltpu.VMEM((8,) + o.shape, bf16),
            pltpu.VMEM((PAD, cols), jnp.float32),
            pltpu.VMEM((2 * share, cols), bf16),
            pltpu.VMEM((8, share, cols), bf16),
            pltpu.VMEM((17, share, cols // 2), bf16),
            pltpu.VMEM(tokens.shape, bf16),
            pltpu.VMEM(w_out.shape, bf16),
            pltpu.VMEM(w_up.shape, bf16),
            pltpu.VMEM(w_down.shape, bf16),
            pltpu.SemaphoreType.DMA((copies,)),
            pltpu.SemaphoreType.DMA((copies,)),
            pltpu.SemaphoreType.DMA((4,)),
        ],
        compiler_params=pltpu.CompilerParams(collective_id=1, has_side_effects=True, vmem_limit_bytes=54 * 2**20),
        name="tail",
    )(o, w_out, tokens, gain, w_up, w_down)


def per_device(tokens, norm_gain, w_qkv, w_out, post_gain, w_up, w_down):
    rows, width = tokens.shape
    heads = w_qkv.shape[2] // HD
    o, w_out_all = attention(tokens, norm_gain, w_qkv, w_out)
    out = tail(o, w_out_all.reshape(8, heads * HD, width), tokens, post_gain.reshape(width // 128, 128), w_up, w_down)
    return out.reshape(PAD, width)[:rows]


def solution(mesh):
    placed = (
        P("seq", None),
        P(),
        P(None, None, "tensor"),
        P("tensor", None),
        P(),
        P(None, "tensor"),
        P("tensor", None),
    )
    return jax.shard_map(
        per_device, mesh=mesh, in_specs=placed, out_specs=P("seq", None), check_vma=False
    )
```

```python
import functools

import jax
import jax.numpy as jnp
from jax import lax
from jax.experimental import pallas as pl
from jax.experimental.pallas import tpu as pltpu
from jax.sharding import PartitionSpec as P

HD = 48
PAD = 768
WIDE = PAD
MESH = pl.DeviceIdType.MESH
LOG2E = 1.4426950408889634
LIMIT = 2.0**90
FLOOR = 2.0**-20
FULL = pl.BlockSpec(memory_space=pltpu.VMEM)


def layer_norm(values, gain):
    mean = jnp.mean(values, axis=-1, keepdims=True)
    centred = values - mean
    var = jnp.mean(centred * centred, axis=-1, keepdims=True)
    return centred * lax.rsqrt(var + 1e-05) * gain


def wide_row(ref):
    return jnp.concatenate([ref[k : k + 1, :] for k in range(ref.shape[0])], axis=1)


EARLY = [(b, c) for b in (0, 1, 2, 4, 5, 6, 3, 7) for c in range(3)] + [(b, 3) for b in range(8)]


def sweep(rows, queries, keys, vals, acc, probs, early, late):
    def scores(unit, slot):
        b, c = unit
        cols = slice(c * WIDE, (c + 1) * WIDE)
        cut = rows // 32 * 16
        for lo, hi in ((0, cut), (cut, rows)):
            s = jnp.dot(keys[b, lo:hi], queries[:, cols], preferred_element_type=jnp.float32)
            probs[slot, lo:hi, :] = jnp.exp2(s).astype(jnp.bfloat16)

    def product(unit, slot):
        b, c = unit
        cols = slice(c * WIDE, (c + 1) * WIDE)
        acc[:, cols] += jnp.dot(vals[b], probs[slot], preferred_element_type=jnp.float32)

    scores(EARLY[0], 0)
    order = EARLY + [(8, 0)]
    for n, pair in enumerate(EARLY):
        if n + 1 in early:
            early[n + 1]()
        scores(order[n + 1], (n + 1) % 2)
        product(pair, n % 2)

    def body(j, _):
        late(j)
        for c in range(4):
            scores((8 + j, c + 1) if c < 3 else (jnp.minimum(9 + j, 15), 0), (c + 1) % 2)
            product((8 + j, c), c % 2)
        return 0

    lax.fori_loop(0, 8, body, 0)


ORDER = (0, 1, 3, 2)


def load_block(rows, kv, b, keys, vals):
    lane = lax.broadcasted_iota(jnp.int32, (16, PAD), 1)
    sub = lax.broadcasted_iota(jnp.int32, (16, PAD), 0)
    count = ((sub == 0) & (lane < rows)).astype(jnp.float32).astype(jnp.bfloat16)
    shift = (sub == 0).astype(jnp.float32).astype(jnp.bfloat16)
    zeros = jnp.zeros((64, PAD), jnp.bfloat16)
    keys[b] = jnp.concatenate([kv[0], shift, zeros], axis=0).T
    vals[b, 0:HD] = kv[1]
    vals[b, HD : HD + 16] = count


def attend_kernel(
    tokens, gain, w_in, w_ref, o_ref, totals, land_out, kvx_out, w_all,
    tok, wq, w_own, normed, qkv, land, kvx, queries, keys, vals, probs, acc, send, recv, local,
):
    rows = tok.shape[0]
    width = queries.shape[1]
    seq, me = lax.axis_index("seq"), lax.axis_index("tensor")
    z, y, core = seq // 8, lax.rem(seq // 2, 4), lax.rem(seq, 2)
    links = Links(send, recv)
    fetch = [
        pltpu.make_async_copy(src, dst, local.at[i])
        for i, (src, dst) in enumerate(((tokens, tok), (w_in, wq), (w_ref, w_own)))
    ]
    for copy in fetch:
        copy.start()

    def keep(i):
        src, dst = (
            (w_own, w_all.at[me]),
            (land, land_out),
            (kvx.at[0], kvx_out.at[0]),
            (kvx.at[1], kvx_out.at[1]),
            (kvx.at[2], kvx_out.at[2]),
        )[i]
        return pltpu.make_async_copy(src, dst, local.at[3 + i])


    def on_seq(dz, dy, dc):
        return ((lax.rem(z + dz, 2) * 4 + lax.rem(y + dy, 4)) * 2 + lax.rem(core + dc, 2), me)

    barrier = pltpu.get_barrier_semaphore()
    peers = [on_seq(0, d, 0) for d in (1, 2, 3)] + [on_seq(0, 0, 1), on_seq(1, 0, 0)]
    peers += [(seq, links.slot(1, 0)), (seq, links.slot(0, 1)), (seq, links.slot(0, 3))]
    for peer in peers:
        pl.semaphore_signal(barrier, inc=1, device_id=peer, device_id_type=MESH)

    step = rows // 5
    normed[rows:PAD, :] = jnp.zeros((PAD - rows, normed.shape[1]), jnp.bfloat16)
    fetch[0].wait()

    scale = wide_row(gain)

    def norm_rows(i, _):
        at = pl.ds(pl.multiple_of(i * step, 16), step)
        normed[at, :] = layer_norm(tok[at, :].astype(jnp.float32), scale).astype(jnp.bfloat16)
        return 0

    lax.fori_loop(0, 5, norm_rows, 0)
    fetch[1].wait()
    span = w_in.shape[0] // 3
    wide = lax.dot_general(wq[...], normed[...], (((1,), (1,)), ((), ())), preferred_element_type=jnp.float32)
    for p in range(3):
        part = wide[p * span : (p + 1) * span]
        if p == 0:
            part = part * (LOG2E / HD**0.5)
        qkv[p] = part.astype(jnp.bfloat16).reshape(4, HD, PAD)
    pl.semaphore_wait(barrier, 8)

    by_y = {}
    for d in (1, 3, 2):
        by_y[d] = links.start(lambda d=d: (qkv.at[:, lax.rem(y + d, 4)], land.at[d], on_seq(0, d, 0)))
    to_core, to_far, far_core, more = {}, {}, {}, {}
    to_core[0] = links.start(lambda: (qkv.at[1:3, y], kvx.at[0, 0], on_seq(0, 0, 1)))
    to_far[0] = links.start(lambda: (qkv.at[1:3, y], kvx.at[1, 0], on_seq(1, 0, 0)))

    fetch[2].wait()
    keep(0).start()
    w_cols = w_own.shape[2] // 2

    def tensor_at(dz, dx):
        return (seq, links.slot(dz, dx))

    def own_w(dz, dx):
        return links.start(lambda: (w_own.at[core], w_all.at[me, core], tensor_at(dz, dx)))

    def pass_w(slot, lo, hi, dz, dx):
        def ends():
            ref = w_all.at[links.slot(*slot), core, :, lo * w_cols : hi * w_cols]
            return ref, ref, tensor_at(dz, dx)

        return links.start(ends)

    def swap_w(slot):
        def ends():
            ref = w_all.at[links.slot(*slot), core]
            return ref, ref, on_seq(0, 0, 1)

        return links.start(ends)

    wz, wup, wdown = own_w(1, 0), own_w(0, 1), own_w(0, 3)

    def set_queries(i):
        cols = slice(i * PAD, (i + 1) * PAD)
        queries[0:HD, cols] = land[ORDER[i], 0]
        queries[HD:128, cols] = jnp.zeros((128 - HD, PAD), jnp.bfloat16)
        s = jnp.dot(keys[0, 0:rows], queries[:, cols], preferred_element_type=jnp.float32)
        top = jnp.max(s.reshape(rows // 8, 8, PAD), axis=0)
        top = jnp.max(top, axis=0, keepdims=True)
        first = lax.broadcasted_iota(jnp.int32, (16, PAD), 0) == 0
        shift = jnp.where(first, jnp.broadcast_to(-top, (16, PAD)), 0.0)
        queries[HD : HD + 16, cols] = shift.astype(jnp.bfloat16)

    def arrive(i):
        d = ORDER[i]
        by_y[d].wait_recv()
        to_core[d] = links.start(lambda: (land.at[d, 1:3], kvx.at[0, d], on_seq(0, 0, 1)))
        to_far[d] = links.start(lambda: (land.at[d, 1:3], kvx.at[1, d], on_seq(1, 0, 0)))
        load_block(rows, land.at[d, 1:3], i, keys, vals)
        set_queries(i)

    def take(block):
        group, d = block // 4, ORDER[block % 4]
        if group == 1:
            to_core[d].wait_recv()
        elif group == 2:
            to_far[d].wait_recv()
            far_core[d] = links.start(lambda: (kvx.at[1, d], kvx.at[2, d], on_seq(0, 0, 1)))
        elif group == 3:
            far_core[d].wait_recv()
        load_block(rows, kvx.at[group - 1, d], block, keys, vals)

    others = [(0, 1), (0, 2), (0, 3), (1, 0), (1, 1), (1, 2), (1, 3)]

    def w_first():
        wz.wait_recv()
        more["zup"] = pass_w((1, 0), 0, 2, 0, 1)
        more["zdown"] = pass_w((1, 0), 0, 2, 0, 3)
        wup.wait_recv()
        more["r0"] = pass_w((0, 3), 0, 1, 0, 1)
        wdown.wait_recv()
        more["r1"] = pass_w((0, 1), 1, 2, 0, 3)

    def w_second():
        more["zup"].wait_recv()
        more["q0"] = pass_w((1, 3), 0, 1, 0, 1)
        more["zdown"].wait_recv()
        more["q1"] = pass_w((1, 1), 1, 2, 0, 3)

    def w_third():
        for name in ("r0", "r1", "q0", "q1"):
            more[name].wait_recv()
        for pair in others:
            more[pair] = swap_w(pair)

    def both(*steps):
        def run():
            for function, *args in steps:
                function(*args)

        return run

    def store(i):
        keep(i).start()

    early = {
        1: both((arrive, 1), (arrive, 2)),
        9: both((take, 4),),
        12: both((take, 5),),
        15: both((take, 6),),
        18: both((arrive, 3), (w_first,), (store, 1)),
        21: both((take, 7), (store, 2)),
        32: both((take, 8),),
    }

    def landed(block):
        group, d = block // 4, ORDER[block % 4]
        if group == 2:
            to_far[d].wait_recv()
            far_core[d] = links.start(lambda: (kvx.at[1, d], kvx.at[2, d], on_seq(0, 0, 1)))
        else:
            far_core[d].wait_recv()

    def late(j):
        for k in range(7):

            @pl.when(j == k)
            def _(k=k):
                landed(9 + k)
                if k == 2:
                    store(3)
                if k == 6:
                    store(4)
                if k == 1:
                    w_second()
                if k == 4:
                    w_third()

        block = jnp.minimum(9 + j, 15)
        far = (block >= 12).astype(jnp.int32)
        i = block - 8 - 4 * far
        d = i + (i == 2).astype(jnp.int32) - (i == 3).astype(jnp.int32)
        load_block(rows, kvx.at[1 + far, d], block, keys, vals)

    land[0] = qkv[:, y]
    load_block(rows, land.at[0, 1:3], 0, keys, vals)
    acc[...] = jnp.zeros_like(acc)
    probs[:, rows:PAD, :] = jnp.zeros((2, PAD - rows, WIDE), jnp.bfloat16)
    set_queries(0)
    sweep(rows, queries, keys, vals, acc, probs, early, late)
    attended(acc, o_ref)
    totals[...] = jnp.broadcast_to(acc[HD : HD + 1, :], totals.shape)
    for i in range(5):
        keep(i).wait()
    for pair in others:
        more[pair].wait_recv()
    links.drain()


def attended(sums, o_ref):
    for i, d in enumerate(ORDER):
        cols = slice(i * PAD, (i + 1) * PAD)
        o_ref[d] = (sums[0:HD, cols] / sums[HD : HD + 1, cols]).astype(jnp.bfloat16)


def settle_kernel(
    rows, o_in, totals, land_ref, kvx_ref, o_out, o_new, land, kvx, queries, keys, vals, probs, acc, local
):
    width = totals.shape[1]
    fits = jnp.where((totals[...] < LIMIT) & (totals[...] > FLOOR), 0.0, 1.0)

    @pl.when(jnp.max(fits) > 0.5)
    def _():
        loads = [
            pltpu.make_async_copy(land_ref, land, local.at[0]),
            pltpu.make_async_copy(kvx_ref, kvx, local.at[1]),
        ]
        for load in loads:
            load.start()
        for load in loads:
            load.wait()
        queries[HD:128, :] = jnp.zeros((128 - HD, width), jnp.bfloat16)
        for i, d in enumerate(ORDER):
            queries[0:HD, i * PAD : (i + 1) * PAD] = land[d, 0]
        probs[rows:PAD, :] = jnp.zeros((PAD - rows, 256), jnp.bfloat16)
        acc[...] = jnp.zeros_like(acc)

        def fill(d, _):
            load_block(rows, land.at[d, 1:3], d, keys, vals)
            for g in range(3):
                load_block(rows, kvx.at[g, d], 4 * g + 4 + d, keys, vals)
            return 0

        lax.fori_loop(0, 4, fill, 0)

        def chunk(c, _):
            cols = pl.ds(pl.multiple_of(c * 256, 256), 256)

            def block(b, carry):
                peak, sums = carry
                s = jnp.dot(keys[b, 0:rows], queries[:, cols], preferred_element_type=jnp.float32)
                fresh = jnp.maximum(peak, jnp.max(s, axis=0, keepdims=True))
                probs[0:rows, :] = jnp.exp2(s - fresh).astype(jnp.bfloat16)
                part = jnp.dot(vals[b], probs[...], preferred_element_type=jnp.float32)
                return fresh, sums * jnp.exp2(peak - fresh) + part

            start = (jnp.full((1, 256), -1e30, jnp.float32), jnp.zeros((HD + 16, 256), jnp.float32))
            _, sums = lax.fori_loop(0, 16, block, start)
            acc[:, cols] = sums
            return 0

        lax.fori_loop(0, width // 256, chunk, 0)
        attended(acc, o_new)
        store = pltpu.make_async_copy(o_new, o_out, local.at[2])
        store.start()
        store.wait()


def attention(tokens, gain, w_qkv, w_out):
    rows, features = tokens.shape
    width = 4 * PAD
    bf16 = jnp.bfloat16
    half, cols = w_out.shape[0] // 2, w_out.shape[1]
    n = 48
    tables = [
        pltpu.VMEM((128, width), bf16),
        pltpu.VMEM((16, PAD, 128), bf16),
        pltpu.VMEM((16, HD + 16, PAD), bf16),
    ]
    blocks = [pltpu.VMEM((4, 3, HD, PAD), bf16), pltpu.VMEM((3, 4, 2, HD, PAD), bf16)]
    anywhere = pl.BlockSpec(memory_space=pl.ANY)
    o, totals, land, kvx, w_all = pl.pallas_call(
        attend_kernel,
        out_shape=(
            jax.ShapeDtypeStruct((4, HD, PAD), bf16),
            jax.ShapeDtypeStruct((8, width), jnp.float32),
            jax.ShapeDtypeStruct((4, 3, HD, PAD), bf16),
            jax.ShapeDtypeStruct((3, 4, 2, HD, PAD), bf16),
            jax.ShapeDtypeStruct((8, 2, half, cols), bf16),
        ),
        in_specs=[anywhere, FULL, anywhere, anywhere],
        out_specs=(FULL, FULL, anywhere, anywhere, anywhere),
        scratch_shapes=[
            pltpu.VMEM(tokens.shape, bf16),
            pltpu.VMEM((3 * w_qkv.shape[2], features), bf16),
            pltpu.VMEM((2, half, cols), bf16),
            pltpu.VMEM((PAD, features), bf16),
            pltpu.VMEM((3, 4, HD, PAD), bf16),
        ]
        + blocks
        + tables
        + [
            pltpu.VMEM((2, PAD, WIDE), bf16),
            pltpu.VMEM((HD + 16, width), jnp.float32),
            pltpu.SemaphoreType.DMA((n,)),
            pltpu.SemaphoreType.DMA((n,)),
            pltpu.SemaphoreType.DMA((8,)),
        ],
        compiler_params=pltpu.CompilerParams(collective_id=0, has_side_effects=True, vmem_limit_bytes=54 * 2**20),
        name="attend",
    )(
        tokens,
        gain.reshape(features // 128, 128),
        jnp.transpose(w_qkv, (1, 2, 0)).reshape(3 * w_qkv.shape[2], features),
        w_out.reshape(2, half, cols),
    )
    o = pl.pallas_call(
        functools.partial(settle_kernel, rows),
        out_shape=jax.ShapeDtypeStruct((4, HD, PAD), bf16),
        in_specs=[anywhere, FULL, anywhere, anywhere],
        out_specs=anywhere,
        input_output_aliases={0: 0},
        scratch_shapes=[pltpu.VMEM((4, HD, PAD), bf16)]
        + blocks
        + tables
        + [
            pltpu.VMEM((PAD, 256), bf16),
            pltpu.VMEM((HD + 16, width), jnp.float32),
            pltpu.SemaphoreType.DMA((3,)),
        ],
        compiler_params=pltpu.CompilerParams(vmem_limit_bytes=61 * 2**20),
        name="settle",
    )(o, totals, land, kvx)
    return o, w_all.reshape(16 * half, cols)


class Links:
    def __init__(self, send, recv):
        me = lax.axis_index("tensor")
        self.seq = lax.axis_index("seq")
        self.z, self.x = me // 4, lax.rem(me, 4)
        self.me = me
        self.send, self.recv = send, recv
        self.count = 0
        self.open = []

    def slot(self, dz, dx):
        z = lax.rem(self.z + dz, 2)
        return z * 4 + lax.rem(self.x + dx, 4)

    def barrier(self, more=0):
        sem = pltpu.get_barrier_semaphore()
        for dz, dx in ((1, 0), (0, 1), (0, 3)):
            pl.semaphore_signal(sem, inc=1, device_id=(self.seq, self.slot(dz, dx)), device_id_type=MESH)
        pl.semaphore_wait(sem, 3 + more)

    def put(self, src, dst, dz, dx):
        device = (self.seq, self.slot(dz, dx))
        return self.start(lambda: (src, dst, device))

    def start(self, ends):
        copy = Copy(self, self.count, ends)
        self.count += 1
        self.open.append(copy)
        copy.make().start()
        return copy

    def drain(self):
        for copy in self.open:
            copy.make().wait_send()
        self.open = []


class Copy:
    def __init__(self, links, index, ends):
        self.links, self.index, self.ends = links, index, ends

    def make(self):
        src, dst, device = self.ends()
        return pltpu.make_async_remote_copy(
            src_ref=src,
            dst_ref=dst,
            send_sem=self.links.send.at[self.index],
            recv_sem=self.links.recv.at[self.index],
            device_id=device,
            device_id_type=MESH,
        )

    def wait_recv(self):
        self.make().wait_recv()


def gather_tensor(links, piece, ready=lambda dz, dx: None, between=lambda: None):
    s = links.slot
    put = links.put

    def pass_on(slot, lo, hi, dz, dx):
        ref = piece(slot, lo, hi)
        return put(ref, ref, dz, dx)

    me = s(0, 0)
    b_up = pass_on(me, 2, 4, 0, 1)
    b_down = pass_on(me, 2, 4, 0, 3)
    b_z = pass_on(me, 2, 4, 1, 0)
    between()
    a_z = pass_on(me, 0, 2, 1, 0)
    a_up = pass_on(me, 0, 2, 0, 1)
    a_down = pass_on(me, 0, 2, 0, 3)
    ready(0, 0)
    b_up.wait_recv()
    r2 = pass_on(s(0, 3), 2, 3, 0, 1)
    bz_lo = pass_on(s(0, 3), 2, 4, 1, 0)
    b_down.wait_recv()
    r3 = pass_on(s(0, 1), 3, 4, 0, 3)
    bz_hi = pass_on(s(0, 1), 2, 4, 1, 0)
    a_z.wait_recv()
    az_up = pass_on(s(1, 0), 0, 2, 0, 1)
    az_down = pass_on(s(1, 0), 0, 2, 0, 3)
    a_up.wait_recv()
    r0 = pass_on(s(0, 3), 0, 1, 0, 1)
    a_down.wait_recv()
    r1 = pass_on(s(0, 1), 1, 2, 0, 3)
    ready(0, 3)
    r2.wait_recv()
    bz_2 = pass_on(s(0, 2), 2, 3, 1, 0)
    r3.wait_recv()
    bz_3 = pass_on(s(0, 2), 3, 4, 1, 0)
    ready(0, 1)
    az_up.wait_recv()
    q0 = pass_on(s(1, 3), 0, 1, 0, 1)
    az_down.wait_recv()
    q1 = pass_on(s(1, 1), 1, 2, 0, 3)
    b_z.wait_recv()
    ready(1, 0)
    r0.wait_recv()
    r1.wait_recv()
    ready(0, 2)
    bz_lo.wait_recv()
    ready(1, 3)
    bz_hi.wait_recv()
    ready(1, 1)
    for copy in (bz_2, bz_3, q0, q1):
        copy.wait_recv()
    ready(1, 2)
    links.drain()


GATHER_COPIES = 18


def reduce_tensor(links, term, stage, rows, cols, make):
    quarter = cols // 4
    s = links.slot
    put = links.put

    def q(slot, lo, hi):
        return term.at[slot, :, lo * quarter : hi * quarter]

    def val(slot, lo, hi):
        return term[slot, :, lo * quarter : hi * quarter].astype(jnp.float32)

    def land(i, n):
        return stage.at[i, :, 0 : n * quarter]

    def got(i, lo, hi):
        return stage[i, :, lo * quarter : hi * quarter].astype(jnp.float32)

    def add_into(slot, lo, hi, *parts):
        total = val(slot, lo, hi)
        for part in parts:
            total = total + part
        term[slot, :, lo * quarter : hi * quarter] = total.astype(jnp.bfloat16)

    zb, fa, near = {}, {}, {}

    def cross(i, dx):
        zb[dx] = put(q(s(1, dx), 2, 4), land(i, 2), 1, 0)

    def far(j, dz):
        fa[dz, 0] = put(q(s(dz, 2), 0, 1), land(4 + j, 1), 0, 3)
        fa[dz, 1] = put(q(s(dz, 2), 1, 2), land(6 + j, 1), 0, 1)

    def relay(j, dz):
        fa[dz, 0].wait_recv()
        add_into(s(dz, 3), 0, 1, got(4 + j, 0, 1))
        near[dz, 3] = put(q(s(dz, 3), 0, 2), land(8 + j, 2), 0, 3)
        fa[dz, 1].wait_recv()
        add_into(s(dz, 1), 1, 2, got(6 + j, 0, 1))
        near[dz, 1] = put(q(s(dz, 1), 0, 2), land(10 + j, 2), 0, 1)

    make((1, 2), (0, 2))
    cross(0, 2)
    far(0, 1)
    far(1, 0)
    make((1, 1), (1, 3))
    cross(1, 1)
    cross(2, 3)
    relay(0, 1)
    make((0, 1), (0, 3))
    relay(1, 0)
    zb[2].wait_recv()
    add_into(s(0, 2), 2, 4, got(0, 0, 2))
    fb0 = put(q(s(0, 2), 2, 3), land(12, 1), 0, 3)
    fb1 = put(q(s(0, 2), 3, 4), land(13, 1), 0, 1)
    make((1, 0), (0, 0))
    cross(3, 0)
    zb[1].wait_recv()
    zb[3].wait_recv()
    near[1, 3].wait_recv()
    near[1, 1].wait_recv()
    add_into(s(1, 0), 0, 2, got(8, 0, 2), got(10, 0, 2))
    za = put(q(s(1, 0), 0, 2), land(14, 2), 1, 0)
    fb0.wait_recv()
    add_into(s(0, 3), 2, 3, got(2, 0, 1), got(12, 0, 1))
    add_into(s(0, 3), 3, 4, got(2, 1, 2))
    nb3 = put(q(s(0, 3), 2, 4), land(15, 2), 0, 3)
    fb1.wait_recv()
    add_into(s(0, 1), 3, 4, got(1, 1, 2), got(13, 0, 1))
    add_into(s(0, 1), 2, 3, got(1, 0, 1))
    nb1 = put(q(s(0, 1), 2, 4), land(16, 2), 0, 1)
    zb[0].wait_recv()
    nb3.wait_recv()
    nb1.wait_recv()
    second = val(s(0, 0), 2, 4) + got(3, 0, 2) + got(15, 0, 2) + got(16, 0, 2)

    def first():
        near[0, 3].wait_recv()
        near[0, 1].wait_recv()
        za.wait_recv()
        return val(s(0, 0), 0, 2) + got(9, 0, 2) + got(11, 0, 2) + got(14, 0, 2)

    return first, second


def tail_kernel(
    o_ref, w_out, tokens, gain, w_up, w_down, out_ref, every, mixed, post, term, stage, tok, wo, wu, wd, send, recv, local
):
    links = Links(send, recv)
    seq, me = links.seq, links.me
    y = lax.rem(seq // 2, 4)
    share, width = out_ref.shape[1], out_ref.shape[2]
    quarter = width // 4
    rows = tok.shape[0]
    loads = [
        pltpu.make_async_copy(src, dst, local.at[i])
        for i, (src, dst) in enumerate(((tokens, tok), (w_out, wo), (w_up, wu), (w_down, wd)))
    ]
    for load in loads:
        load.start()

    def at_y(dy):
        return ((seq // 8 * 4 + lax.rem(y + dy, 4)) * 2 + lax.rem(seq, 2), me)

    sem = pltpu.get_barrier_semaphore()
    for d in (1, 2, 3):
        pl.semaphore_signal(sem, inc=1, device_id=at_y(d), device_id_type=MESH)
    links.barrier(3)
    back = [links.start(lambda d=d: (o_ref.at[d], every.at[me, y], at_y(4 - d))) for d in (2, 1, 3)]
    every[me, y] = o_ref[0]
    loads[0].wait()
    mixed[0:rows, :] = tok[...].astype(jnp.float32)
    mixed[rows:, :] = jnp.zeros((PAD - rows, width), jnp.float32)
    loads[1].wait()
    for copy in back:
        copy.wait_recv()

    def project(dz, dx):
        slot = links.slot(dz, dx)

        def tile(i, _):
            at = pl.ds(pl.multiple_of(i * 256, 256), 256)
            left = every[slot, :, :, at].reshape(4 * HD, 256)
            mixed[at, :] += lax.dot_general(
                left, wo[slot], (((0,), (0,)), ((), ())), preferred_element_type=jnp.float32
            )
            return 0

        lax.fori_loop(0, PAD // 256, tile, 0)

    gather_tensor(links, lambda slot, lo, hi: every.at[slot, lo:hi], project)
    loads[2].wait()
    loads[3].wait()

    scale = wide_row(gain)

    def feed_forward(*pair):
        slots = [links.slot(*block) for block in pair]
        for k, slot in enumerate(slots):
            at = pl.ds(pl.multiple_of(slot * share, 32), share)
            post[k * share : (k + 1) * share, :] = layer_norm(mixed[at, :], scale).astype(jnp.bfloat16)
        up = jnp.dot(post[...], wu[...], preferred_element_type=jnp.float32)
        hidden = jax.nn.gelu(up, approximate=True).astype(jnp.bfloat16)
        for k in range(3):
            cols = slice(k * (width // 3), (k + 1) * (width // 3))
            down = jnp.dot(hidden, wd[:, cols], preferred_element_type=jnp.float32).astype(jnp.bfloat16)
            for i, slot in enumerate(slots):
                term[slot, :, cols] = down[i * share : (i + 1) * share]

    first, second = reduce_tensor(links, term, stage, share, width, feed_forward)
    at = pl.ds(pl.multiple_of(me * share, 32), share)
    out_ref[me, :, 2 * quarter :] = (mixed[at, 2 * quarter :] + second).astype(jnp.bfloat16)

    def rest():
        out_ref[me, :, 0 : 2 * quarter] = (mixed[at, 0 : 2 * quarter] + first()).astype(jnp.bfloat16)

    gather_tensor(links, lambda slot, lo, hi: out_ref.at[slot, :, lo * quarter : hi * quarter], between=rest)


def tail(o, w_out, tokens, gain, w_up, w_down):
    rows, cols = tokens.shape
    share = PAD // 8
    copies = 64
    bf16 = jnp.bfloat16
    anywhere = pl.BlockSpec(memory_space=pl.ANY)
    return pl.pallas_call(
        tail_kernel,
        out_shape=jax.ShapeDtypeStruct((8, share, cols), bf16),
        in_specs=[FULL, anywhere, anywhere, FULL, anywhere, anywhere],
        out_specs=FULL,
        scratch_shapes=[
            pltpu.VMEM((8,) + o.shape, bf16),
            pltpu.VMEM((PAD, cols), jnp.float32),
            pltpu.VMEM((2 * share, cols), bf16),
            pltpu.VMEM((8, share, cols), bf16),
            pltpu.VMEM((17, share, cols // 2), bf16),
            pltpu.VMEM(tokens.shape, bf16),
            pltpu.VMEM(w_out.shape, bf16),
            pltpu.VMEM(w_up.shape, bf16),
            pltpu.VMEM(w_down.shape, bf16),
            pltpu.SemaphoreType.DMA((copies,)),
            pltpu.SemaphoreType.DMA((copies,)),
            pltpu.SemaphoreType.DMA((4,)),
        ],
        compiler_params=pltpu.CompilerParams(collective_id=1, has_side_effects=True, vmem_limit_bytes=48 * 2**20),
        name="tail",
    )(o, w_out, tokens, gain, w_up, w_down)


def per_device(tokens, norm_gain, w_qkv, w_out, post_gain, w_up, w_down):
    rows, width = tokens.shape
    heads = w_qkv.shape[2] // HD
    o, w_out_all = attention(tokens, norm_gain, w_qkv, w_out)
    out = tail(o, w_out_all.reshape(8, heads * HD, width), tokens, post_gain.reshape(width // 128, 128), w_up, w_down)
    return out.reshape(PAD, width)[:rows]


def solution(mesh):
    placed = (
        P("seq", None),
        P(),
        P(None, None, "tensor"),
        P("tensor", None),
        P(),
        P(None, "tensor"),
        P("tensor", None),
    )
    return jax.shard_map(
        per_device, mesh=mesh, in_specs=placed, out_specs=P("seq", None), check_vma=False
    )
```

```python
import functools

import jax
import jax.numpy as jnp
from jax import lax
from jax.experimental import pallas as pl
from jax.experimental.pallas import tpu as pltpu
from jax.sharding import PartitionSpec as P

HD = 48
PAD = 768
WIDE = PAD
MESH = pl.DeviceIdType.MESH
LOG2E = 1.4426950408889634
LIMIT = 2.0**90
FLOOR = 2.0**-20
FULL = pl.BlockSpec(memory_space=pltpu.VMEM)


def layer_norm(values, gain):
    mean = jnp.mean(values, axis=-1, keepdims=True)
    centred = values - mean
    var = jnp.mean(centred * centred, axis=-1, keepdims=True)
    return centred * lax.rsqrt(var + 1e-05) * gain


def wide_row(ref):
    return jnp.concatenate([ref[k : k + 1, :] for k in range(ref.shape[0])], axis=1)


EARLY = [(b, c) for b in (0, 1, 2, 4, 5, 6, 3, 7) for c in range(3)] + [(b, 3) for b in range(8)]


def sweep(rows, queries, keys, vals, acc, probs, early, late):
    def scores(unit, slot):
        b, c = unit
        cols = slice(c * WIDE, (c + 1) * WIDE)
        cut = rows // 32 * 16
        for lo, hi in ((0, cut), (cut, rows)):
            s = jnp.dot(keys[b, lo:hi], queries[:, cols], preferred_element_type=jnp.float32)
            probs[slot, lo:hi, :] = jnp.exp2(s).astype(jnp.bfloat16)

    def product(unit, slot):
        b, c = unit
        cols = slice(c * WIDE, (c + 1) * WIDE)
        acc[:, cols] += jnp.dot(vals[b], probs[slot], preferred_element_type=jnp.float32)

    scores(EARLY[0], 0)
    order = EARLY + [(8, 0)]
    for n, pair in enumerate(EARLY):
        if n + 1 in early:
            early[n + 1]()
        scores(order[n + 1], (n + 1) % 2)
        product(pair, n % 2)

    def body(j, _):
        late(j)
        for c in range(4):
            scores((8 + j, c + 1) if c < 3 else (jnp.minimum(9 + j, 15), 0), (c + 1) % 2)
            product((8 + j, c), c % 2)
        return 0

    lax.fori_loop(0, 8, body, 0)


ORDER = (0, 1, 3, 2)


def load_keys(src, b, keys):
    one = (lax.broadcasted_iota(jnp.int32, (16, PAD), 0) == 0).astype(jnp.float32).astype(jnp.bfloat16)
    keys[b] = jnp.concatenate([src[...], one, jnp.zeros((64, PAD), jnp.bfloat16)], axis=0).T


def load_values(rows, src, b, vals):
    lane = lax.broadcasted_iota(jnp.int32, (16, PAD), 1)
    sub = lax.broadcasted_iota(jnp.int32, (16, PAD), 0)
    vals[b, 0:HD] = src[...]
    vals[b, HD : HD + 16] = ((sub == 0) & (lane < rows)).astype(jnp.float32).astype(jnp.bfloat16)


def load_block(rows, kv, b, keys, vals):
    load_keys(kv.at[0], b, keys)
    load_values(rows, kv.at[1], b, vals)


def attend_kernel(
    tokens, gain, w_in, w_ref, o_ref, totals, land_out, kvx_out, w_all,
    tok, wq, w_own, normed, qkv, land, kvx, queries, keys, vals, probs, acc, send, recv, local,
):
    rows = tok.shape[0]
    width = queries.shape[1]
    seq, me = lax.axis_index("seq"), lax.axis_index("tensor")
    z, y, core = seq // 8, lax.rem(seq // 2, 4), lax.rem(seq, 2)
    links = Links(send, recv)
    fetch = [
        pltpu.make_async_copy(src, dst, local.at[i])
        for i, (src, dst) in enumerate(((tokens, tok), (w_in, wq), (w_ref, w_own)))
    ]
    for copy in fetch:
        copy.start()

    def keep(i):
        src, dst = (
            (w_own, w_all.at[me]),
            (land, land_out),
            (kvx.at[0], kvx_out.at[0]),
            (kvx.at[1], kvx_out.at[1]),
            (kvx.at[2], kvx_out.at[2]),
        )[i]
        return pltpu.make_async_copy(src, dst, local.at[3 + i])


    def on_seq(dz, dy, dc):
        return ((lax.rem(z + dz, 2) * 4 + lax.rem(y + dy, 4)) * 2 + lax.rem(core + dc, 2), me)

    barrier = pltpu.get_barrier_semaphore()
    peers = [on_seq(0, d, 0) for d in (1, 2, 3)] + [on_seq(0, 0, 1), on_seq(1, 0, 0)]
    peers += [(seq, links.slot(1, 0)), (seq, links.slot(0, 1)), (seq, links.slot(0, 3))]
    for peer in peers:
        pl.semaphore_signal(barrier, inc=1, device_id=peer, device_id_type=MESH)

    step = rows // 5
    normed[rows:PAD, :] = jnp.zeros((PAD - rows, normed.shape[1]), jnp.bfloat16)
    fetch[0].wait()

    scale = wide_row(gain)

    def norm_rows(i, _):
        at = pl.ds(pl.multiple_of(i * step, 16), step)
        normed[at, :] = layer_norm(tok[at, :].astype(jnp.float32), scale).astype(jnp.bfloat16)
        return 0

    lax.fori_loop(0, 5, norm_rows, 0)
    fetch[1].wait()
    span = w_in.shape[0] // 3
    wide = lax.dot_general(wq[...], normed[...], (((1,), (1,)), ((), ())), preferred_element_type=jnp.float32)
    for p in range(3):
        part = wide[p * span : (p + 1) * span]
        if p == 0:
            part = part * (LOG2E / HD**0.5)
        qkv[p] = part.astype(jnp.bfloat16).reshape(4, HD, PAD)
    pl.semaphore_wait(barrier, 8)

    by_y = {}

    def send_y(d, lo, hi):
        by_y[d, lo] = links.start(
            lambda: (qkv.at[lo:hi, lax.rem(y + d, 4)], land.at[d, lo:hi], on_seq(0, d, 0))
        )

    for d, lo, hi in ((1, 0, 2), (3, 0, 2), (1, 2, 3), (3, 2, 3), (2, 0, 2), (2, 2, 3)):
        send_y(d, lo, hi)
    to_core, to_far, far_core, more = {}, {}, {}, {}
    to_core[0] = links.start(lambda: (qkv.at[1:3, y], kvx.at[0, 0], on_seq(0, 0, 1)))
    to_far[0] = links.start(lambda: (qkv.at[1:3, y], kvx.at[1, 0], on_seq(1, 0, 0)))

    fetch[2].wait()
    keep(0).start()
    w_cols = w_own.shape[2] // 2

    def tensor_at(dz, dx):
        return (seq, links.slot(dz, dx))

    def own_w(dz, dx):
        return links.start(lambda: (w_own.at[core], w_all.at[me, core], tensor_at(dz, dx)))

    def pass_w(slot, lo, hi, dz, dx):
        def ends():
            ref = w_all.at[links.slot(*slot), core, :, lo * w_cols : hi * w_cols]
            return ref, ref, tensor_at(dz, dx)

        return links.start(ends)

    def swap_w(slot):
        def ends():
            ref = w_all.at[links.slot(*slot), core]
            return ref, ref, on_seq(0, 0, 1)

        return links.start(ends)

    wz, wup, wdown = own_w(1, 0), own_w(0, 1), own_w(0, 3)

    def set_queries(i):
        cols = slice(i * PAD, (i + 1) * PAD)
        queries[0:HD, cols] = land[ORDER[i], 0]
        queries[HD:128, cols] = jnp.zeros((128 - HD, PAD), jnp.bfloat16)
        s = jnp.dot(keys[0, 0:rows], queries[:, cols], preferred_element_type=jnp.float32)
        top = jnp.max(s.reshape(rows // 8, 8, PAD), axis=0)
        top = jnp.max(top, axis=0, keepdims=True)
        first = lax.broadcasted_iota(jnp.int32, (16, PAD), 0) == 0
        shift = jnp.where(first, jnp.broadcast_to(-top, (16, PAD)), 0.0)
        queries[HD : HD + 16, cols] = shift.astype(jnp.bfloat16)

    def arrive(i):
        by_y[ORDER[i], 0].wait_recv()
        load_keys(land.at[ORDER[i], 1], i, keys)
        set_queries(i)

    def arrive_values(i):
        d = ORDER[i]
        by_y[d, 2].wait_recv()
        to_core[d] = links.start(lambda: (land.at[d, 1:3], kvx.at[0, d], on_seq(0, 0, 1)))
        to_far[d] = links.start(lambda: (land.at[d, 1:3], kvx.at[1, d], on_seq(1, 0, 0)))
        load_values(rows, land.at[d, 2], i, vals)

    def take(block):
        group, d = block // 4, ORDER[block % 4]
        if group == 1:
            to_core[d].wait_recv()
        elif group == 2:
            to_far[d].wait_recv()
            far_core[d] = links.start(lambda: (kvx.at[1, d], kvx.at[2, d], on_seq(0, 0, 1)))
        elif group == 3:
            far_core[d].wait_recv()
        load_block(rows, kvx.at[group - 1, d], block, keys, vals)

    others = [(0, 1), (0, 2), (0, 3), (1, 0), (1, 1), (1, 2), (1, 3)]

    def w_first():
        wz.wait_recv()
        more["zup"] = pass_w((1, 0), 0, 2, 0, 1)
        more["zdown"] = pass_w((1, 0), 0, 2, 0, 3)
        wup.wait_recv()
        more["r0"] = pass_w((0, 3), 0, 1, 0, 1)
        wdown.wait_recv()
        more["r1"] = pass_w((0, 1), 1, 2, 0, 3)

    def w_second():
        more["zup"].wait_recv()
        more["q0"] = pass_w((1, 3), 0, 1, 0, 1)
        more["zdown"].wait_recv()
        more["q1"] = pass_w((1, 1), 1, 2, 0, 3)

    def w_third():
        for name in ("r0", "r1", "q0", "q1"):
            more[name].wait_recv()
        for pair in others:
            more[pair] = swap_w(pair)

    def both(*steps):
        def run():
            for function, *args in steps:
                function(*args)

        return run

    def store(i):
        keep(i).start()

    early = {
        1: both((arrive, 1), (arrive, 2)),
        2: both((arrive_values, 1), (arrive_values, 2)),
        9: both((take, 4),),
        12: both((take, 5),),
        15: both((take, 6),),
        18: both((arrive, 3), (arrive_values, 3), (w_first,), (store, 1)),
        21: both((take, 7), (store, 2)),
        32: both((take, 8),),
    }

    def landed(block):
        group, d = block // 4, ORDER[block % 4]
        if group == 2:
            to_far[d].wait_recv()
            far_core[d] = links.start(lambda: (kvx.at[1, d], kvx.at[2, d], on_seq(0, 0, 1)))
        else:
            far_core[d].wait_recv()

    def late(j):
        for k in range(7):

            @pl.when(j == k)
            def _(k=k):
                landed(9 + k)
                if k == 2:
                    store(3)
                if k == 6:
                    store(4)
                if k == 1:
                    w_second()
                if k == 4:
                    w_third()

        block = jnp.minimum(9 + j, 15)
        far = (block >= 12).astype(jnp.int32)
        i = block - 8 - 4 * far
        d = i + (i == 2).astype(jnp.int32) - (i == 3).astype(jnp.int32)
        load_block(rows, kvx.at[1 + far, d], block, keys, vals)

    land[0] = qkv[:, y]
    load_block(rows, land.at[0, 1:3], 0, keys, vals)
    acc[...] = jnp.zeros_like(acc)
    probs[:, rows:PAD, :] = jnp.zeros((2, PAD - rows, WIDE), jnp.bfloat16)
    set_queries(0)
    sweep(rows, queries, keys, vals, acc, probs, early, late)
    attended(acc, o_ref)
    totals[...] = jnp.broadcast_to(acc[HD : HD + 1, :], totals.shape)
    for i in range(5):
        keep(i).wait()
    for pair in others:
        more[pair].wait_recv()
    links.drain()


def attended(sums, o_ref):
    for i, d in enumerate(ORDER):
        cols = slice(i * PAD, (i + 1) * PAD)
        o_ref[d] = (sums[0:HD, cols] / sums[HD : HD + 1, cols]).astype(jnp.bfloat16)


def settle_kernel(
    rows, o_in, totals, land_ref, kvx_ref, o_out, o_new, land, kvx, queries, keys, vals, probs, acc, local
):
    width = totals.shape[1]
    fits = jnp.where((totals[...] < LIMIT) & (totals[...] > FLOOR), 0.0, 1.0)

    @pl.when(jnp.max(fits) > 0.5)
    def _():
        loads = [
            pltpu.make_async_copy(land_ref, land, local.at[0]),
            pltpu.make_async_copy(kvx_ref, kvx, local.at[1]),
        ]
        for load in loads:
            load.start()
        for load in loads:
            load.wait()
        queries[HD:128, :] = jnp.zeros((128 - HD, width), jnp.bfloat16)
        for i, d in enumerate(ORDER):
            queries[0:HD, i * PAD : (i + 1) * PAD] = land[d, 0]
        probs[rows:PAD, :] = jnp.zeros((PAD - rows, 256), jnp.bfloat16)
        acc[...] = jnp.zeros_like(acc)

        def fill(d, _):
            load_block(rows, land.at[d, 1:3], d, keys, vals)
            for g in range(3):
                load_block(rows, kvx.at[g, d], 4 * g + 4 + d, keys, vals)
            return 0

        lax.fori_loop(0, 4, fill, 0)

        def chunk(c, _):
            cols = pl.ds(pl.multiple_of(c * 256, 256), 256)

            def block(b, carry):
                peak, sums = carry
                s = jnp.dot(keys[b, 0:rows], queries[:, cols], preferred_element_type=jnp.float32)
                fresh = jnp.maximum(peak, jnp.max(s, axis=0, keepdims=True))
                probs[0:rows, :] = jnp.exp2(s - fresh).astype(jnp.bfloat16)
                part = jnp.dot(vals[b], probs[...], preferred_element_type=jnp.float32)
                return fresh, sums * jnp.exp2(peak - fresh) + part

            start = (jnp.full((1, 256), -1e30, jnp.float32), jnp.zeros((HD + 16, 256), jnp.float32))
            _, sums = lax.fori_loop(0, 16, block, start)
            acc[:, cols] = sums
            return 0

        lax.fori_loop(0, width // 256, chunk, 0)
        attended(acc, o_new)
        store = pltpu.make_async_copy(o_new, o_out, local.at[2])
        store.start()
        store.wait()


def attention(tokens, gain, w_qkv, w_out):
    rows, features = tokens.shape
    width = 4 * PAD
    bf16 = jnp.bfloat16
    half, cols = w_out.shape[0] // 2, w_out.shape[1]
    n = 48
    tables = [
        pltpu.VMEM((128, width), bf16),
        pltpu.VMEM((16, PAD, 128), bf16),
        pltpu.VMEM((16, HD + 16, PAD), bf16),
    ]
    blocks = [pltpu.VMEM((4, 3, HD, PAD), bf16), pltpu.VMEM((3, 4, 2, HD, PAD), bf16)]
    anywhere = pl.BlockSpec(memory_space=pl.ANY)
    o, totals, land, kvx, w_all = pl.pallas_call(
        attend_kernel,
        out_shape=(
            jax.ShapeDtypeStruct((4, HD, PAD), bf16),
            jax.ShapeDtypeStruct((8, width), jnp.float32),
            jax.ShapeDtypeStruct((4, 3, HD, PAD), bf16),
            jax.ShapeDtypeStruct((3, 4, 2, HD, PAD), bf16),
            jax.ShapeDtypeStruct((8, 2, half, cols), bf16),
        ),
        in_specs=[anywhere, FULL, anywhere, anywhere],
        out_specs=(FULL, FULL, anywhere, anywhere, anywhere),
        scratch_shapes=[
            pltpu.VMEM(tokens.shape, bf16),
            pltpu.VMEM((3 * w_qkv.shape[2], features), bf16),
            pltpu.VMEM((2, half, cols), bf16),
            pltpu.VMEM((PAD, features), bf16),
            pltpu.VMEM((3, 4, HD, PAD), bf16),
        ]
        + blocks
        + tables
        + [
            pltpu.VMEM((2, PAD, WIDE), bf16),
            pltpu.VMEM((HD + 16, width), jnp.float32),
            pltpu.SemaphoreType.DMA((n,)),
            pltpu.SemaphoreType.DMA((n,)),
            pltpu.SemaphoreType.DMA((8,)),
        ],
        compiler_params=pltpu.CompilerParams(collective_id=0, has_side_effects=True, vmem_limit_bytes=54 * 2**20),
        name="attend",
    )(
        tokens,
        gain.reshape(features // 128, 128),
        jnp.transpose(w_qkv, (1, 2, 0)).reshape(3 * w_qkv.shape[2], features),
        w_out.reshape(2, half, cols),
    )
    o = pl.pallas_call(
        functools.partial(settle_kernel, rows),
        out_shape=jax.ShapeDtypeStruct((4, HD, PAD), bf16),
        in_specs=[anywhere, FULL, anywhere, anywhere],
        out_specs=anywhere,
        input_output_aliases={0: 0},
        scratch_shapes=[pltpu.VMEM((4, HD, PAD), bf16)]
        + blocks
        + tables
        + [
            pltpu.VMEM((PAD, 256), bf16),
            pltpu.VMEM((HD + 16, width), jnp.float32),
            pltpu.SemaphoreType.DMA((3,)),
        ],
        compiler_params=pltpu.CompilerParams(vmem_limit_bytes=61 * 2**20),
        name="settle",
    )(o, totals, land, kvx)
    return o, w_all.reshape(16 * half, cols)


class Links:
    def __init__(self, send, recv):
        me = lax.axis_index("tensor")
        self.seq = lax.axis_index("seq")
        self.z, self.x = me // 4, lax.rem(me, 4)
        self.me = me
        self.send, self.recv = send, recv
        self.count = 0
        self.open = []

    def slot(self, dz, dx):
        z = lax.rem(self.z + dz, 2)
        return z * 4 + lax.rem(self.x + dx, 4)

    def barrier(self, more=0):
        sem = pltpu.get_barrier_semaphore()
        for dz, dx in ((1, 0), (0, 1), (0, 3)):
            pl.semaphore_signal(sem, inc=1, device_id=(self.seq, self.slot(dz, dx)), device_id_type=MESH)
        pl.semaphore_wait(sem, 3 + more)

    def put(self, src, dst, dz, dx):
        device = (self.seq, self.slot(dz, dx))
        return self.start(lambda: (src, dst, device))

    def start(self, ends):
        copy = Copy(self, self.count, ends)
        self.count += 1
        self.open.append(copy)
        copy.make().start()
        return copy

    def drain(self):
        for copy in self.open:
            copy.make().wait_send()
        self.open = []


class Copy:
    def __init__(self, links, index, ends):
        self.links, self.index, self.ends = links, index, ends

    def make(self):
        src, dst, device = self.ends()
        return pltpu.make_async_remote_copy(
            src_ref=src,
            dst_ref=dst,
            send_sem=self.links.send.at[self.index],
            recv_sem=self.links.recv.at[self.index],
            device_id=device,
            device_id_type=MESH,
        )

    def wait_recv(self):
        self.make().wait_recv()


def gather_tensor(links, piece, ready=lambda dz, dx: None, between=lambda: None):
    s = links.slot
    put = links.put

    def pass_on(slot, lo, hi, dz, dx):
        ref = piece(slot, lo, hi)
        return put(ref, ref, dz, dx)

    me = s(0, 0)
    b_up = pass_on(me, 2, 4, 0, 1)
    b_down = pass_on(me, 2, 4, 0, 3)
    b_z = pass_on(me, 2, 4, 1, 0)
    between()
    a_z = pass_on(me, 0, 2, 1, 0)
    a_up = pass_on(me, 0, 2, 0, 1)
    a_down = pass_on(me, 0, 2, 0, 3)
    ready(0, 0)
    b_up.wait_recv()
    r2 = pass_on(s(0, 3), 2, 3, 0, 1)
    bz_lo = pass_on(s(0, 3), 2, 4, 1, 0)
    b_down.wait_recv()
    r3 = pass_on(s(0, 1), 3, 4, 0, 3)
    bz_hi = pass_on(s(0, 1), 2, 4, 1, 0)
    a_z.wait_recv()
    az_up = pass_on(s(1, 0), 0, 2, 0, 1)
    az_down = pass_on(s(1, 0), 0, 2, 0, 3)
    a_up.wait_recv()
    r0 = pass_on(s(0, 3), 0, 1, 0, 1)
    a_down.wait_recv()
    r1 = pass_on(s(0, 1), 1, 2, 0, 3)
    ready(0, 3)
    r2.wait_recv()
    bz_2 = pass_on(s(0, 2), 2, 3, 1, 0)
    r3.wait_recv()
    bz_3 = pass_on(s(0, 2), 3, 4, 1, 0)
    ready(0, 1)
    az_up.wait_recv()
    q0 = pass_on(s(1, 3), 0, 1, 0, 1)
    az_down.wait_recv()
    q1 = pass_on(s(1, 1), 1, 2, 0, 3)
    b_z.wait_recv()
    ready(1, 0)
    r0.wait_recv()
    r1.wait_recv()
    ready(0, 2)
    bz_lo.wait_recv()
    ready(1, 3)
    bz_hi.wait_recv()
    ready(1, 1)
    for copy in (bz_2, bz_3, q0, q1):
        copy.wait_recv()
    ready(1, 2)
    links.drain()


GATHER_COPIES = 18


def cuts(cols):
    return [cols // 12 * k for k in (0, 4, 7, 9, 12)]


def reduce_tensor(links, term, stage, rows, cols, make):
    at = cuts(cols)
    s = links.slot
    put = links.put

    def q(slot, lo, hi):
        return term.at[slot, :, at[lo] : at[hi]]

    def val(slot, lo, hi):
        return term[slot, :, at[lo] : at[hi]].astype(jnp.float32)

    def land(i, lo, hi):
        return stage.at[i, :, 0 : at[hi] - at[lo]]

    def got(i, base, lo, hi):
        return stage[i, :, at[lo] - at[base] : at[hi] - at[base]].astype(jnp.float32)

    def add_into(slot, lo, hi, *parts):
        total = val(slot, lo, hi)
        for part in parts:
            total = total + part
        term[slot, :, at[lo] : at[hi]] = total.astype(jnp.bfloat16)

    zb, fa, near = {}, {}, {}

    def cross(i, dx):
        zb[dx] = put(q(s(1, dx), 2, 4), land(i, 2, 4), 1, 0)

    def far(j, dz):
        fa[dz, 0] = put(q(s(dz, 2), 0, 1), land(4 + j, 0, 1), 0, 3)
        fa[dz, 1] = put(q(s(dz, 2), 1, 2), land(6 + j, 1, 2), 0, 1)

    def relay(j, dz):
        fa[dz, 0].wait_recv()
        add_into(s(dz, 3), 0, 1, got(4 + j, 0, 0, 1))
        near[dz, 3] = put(q(s(dz, 3), 0, 2), land(8 + j, 0, 2), 0, 3)
        fa[dz, 1].wait_recv()
        add_into(s(dz, 1), 1, 2, got(6 + j, 1, 1, 2))
        near[dz, 1] = put(q(s(dz, 1), 0, 2), land(10 + j, 0, 2), 0, 1)

    make((1, 2), (0, 2))
    cross(0, 2)
    far(0, 1)
    far(1, 0)
    make((1, 1), (1, 3))
    cross(1, 1)
    cross(2, 3)
    relay(0, 1)
    make((0, 1), (0, 3))
    relay(1, 0)
    zb[2].wait_recv()
    add_into(s(0, 2), 2, 4, got(0, 2, 2, 4))
    fb0 = put(q(s(0, 2), 2, 3), land(12, 2, 3), 0, 3)
    fb1 = put(q(s(0, 2), 3, 4), land(13, 3, 4), 0, 1)
    make((1, 0), (0, 0))
    cross(3, 0)
    zb[1].wait_recv()
    zb[3].wait_recv()
    near[1, 3].wait_recv()
    near[1, 1].wait_recv()
    add_into(s(1, 0), 0, 2, got(8, 0, 0, 2), got(10, 0, 0, 2))
    za = put(q(s(1, 0), 0, 2), land(14, 0, 2), 1, 0)
    fb0.wait_recv()
    add_into(s(0, 3), 2, 3, got(2, 2, 2, 3), got(12, 2, 2, 3))
    add_into(s(0, 3), 3, 4, got(2, 2, 3, 4))
    nb3 = put(q(s(0, 3), 2, 4), land(15, 2, 4), 0, 3)
    fb1.wait_recv()
    add_into(s(0, 1), 3, 4, got(1, 2, 3, 4), got(13, 3, 3, 4))
    add_into(s(0, 1), 2, 3, got(1, 2, 2, 3))
    nb1 = put(q(s(0, 1), 2, 4), land(16, 2, 4), 0, 1)
    zb[0].wait_recv()
    nb3.wait_recv()
    nb1.wait_recv()
    second = val(s(0, 0), 2, 4) + got(3, 2, 2, 4) + got(15, 2, 2, 4) + got(16, 2, 2, 4)

    def first():
        near[0, 3].wait_recv()
        near[0, 1].wait_recv()
        za.wait_recv()
        return val(s(0, 0), 0, 2) + got(9, 0, 0, 2) + got(11, 0, 0, 2) + got(14, 0, 0, 2)

    return first, second


def tail_kernel(
    o_ref, w_out, tokens, gain, w_up, w_down, out_ref, every, mixed, post, term, stage, tok, wo, wu, wd, send, recv, local
):
    links = Links(send, recv)
    seq, me = links.seq, links.me
    y = lax.rem(seq // 2, 4)
    share, width = out_ref.shape[1], out_ref.shape[2]
    cut = cuts(width)
    rows = tok.shape[0]
    loads = [
        pltpu.make_async_copy(src, dst, local.at[i])
        for i, (src, dst) in enumerate(((tokens, tok), (w_out, wo), (w_up, wu), (w_down, wd)))
    ]
    for load in loads:
        load.start()

    def at_y(dy):
        return ((seq // 8 * 4 + lax.rem(y + dy, 4)) * 2 + lax.rem(seq, 2), me)

    sem = pltpu.get_barrier_semaphore()
    for d in (1, 2, 3):
        pl.semaphore_signal(sem, inc=1, device_id=at_y(d), device_id_type=MESH)
    links.barrier(3)
    back = [links.start(lambda d=d: (o_ref.at[d], every.at[me, y], at_y(4 - d))) for d in (2, 1, 3)]
    every[me, y] = o_ref[0]
    loads[0].wait()
    mixed[0:rows, :] = tok[...].astype(jnp.float32)
    mixed[rows:, :] = jnp.zeros((PAD - rows, width), jnp.float32)
    loads[1].wait()
    for copy in back:
        copy.wait_recv()

    def project(dz, dx):
        slot = links.slot(dz, dx)

        def tile(i, _):
            at = pl.ds(pl.multiple_of(i * 256, 256), 256)
            left = every[slot, :, :, at].reshape(4 * HD, 256)
            mixed[at, :] += lax.dot_general(
                left, wo[slot], (((0,), (0,)), ((), ())), preferred_element_type=jnp.float32
            )
            return 0

        lax.fori_loop(0, PAD // 256, tile, 0)

    gather_tensor(links, lambda slot, lo, hi: every.at[slot, lo:hi], project)
    loads[2].wait()
    loads[3].wait()

    scale = wide_row(gain)

    def feed_forward(*pair):
        slots = [links.slot(*block) for block in pair]
        for k, slot in enumerate(slots):
            at = pl.ds(pl.multiple_of(slot * share, 32), share)
            post[k * share : (k + 1) * share, :] = layer_norm(mixed[at, :], scale).astype(jnp.bfloat16)
        up = jnp.dot(post[...], wu[...], preferred_element_type=jnp.float32)
        hidden = jax.nn.gelu(up, approximate=True).astype(jnp.bfloat16)
        for k in range(3):
            cols = slice(k * (width // 3), (k + 1) * (width // 3))
            down = jnp.dot(hidden, wd[:, cols], preferred_element_type=jnp.float32).astype(jnp.bfloat16)
            for i, slot in enumerate(slots):
                term[slot, :, cols] = down[i * share : (i + 1) * share]

    first, second = reduce_tensor(links, term, stage, share, width, feed_forward)
    at = pl.ds(pl.multiple_of(me * share, 32), share)
    out_ref[me, :, cut[2] :] = (mixed[at, cut[2] :] + second).astype(jnp.bfloat16)

    def rest():
        out_ref[me, :, 0 : cut[2]] = (mixed[at, 0 : cut[2]] + first()).astype(jnp.bfloat16)

    gather_tensor(links, lambda slot, lo, hi: out_ref.at[slot, :, cut[lo] : cut[hi]], between=rest)


def tail(o, w_out, tokens, gain, w_up, w_down):
    rows, cols = tokens.shape
    share = PAD // 8
    copies = 64
    bf16 = jnp.bfloat16
    anywhere = pl.BlockSpec(memory_space=pl.ANY)
    return pl.pallas_call(
        tail_kernel,
        out_shape=jax.ShapeDtypeStruct((8, share, cols), bf16),
        in_specs=[FULL, anywhere, anywhere, FULL, anywhere, anywhere],
        out_specs=FULL,
        scratch_shapes=[
            pltpu.VMEM((8,) + o.shape, bf16),
            pltpu.VMEM((PAD, cols), jnp.float32),
            pltpu.VMEM((2 * share, cols), bf16),
            pltpu.VMEM((8, share, cols), bf16),
            pltpu.VMEM((17, share, cols // 12 * 7), bf16),
            pltpu.VMEM(tokens.shape, bf16),
            pltpu.VMEM(w_out.shape, bf16),
            pltpu.VMEM(w_up.shape, bf16),
            pltpu.VMEM(w_down.shape, bf16),
            pltpu.SemaphoreType.DMA((copies,)),
            pltpu.SemaphoreType.DMA((copies,)),
            pltpu.SemaphoreType.DMA((4,)),
        ],
        compiler_params=pltpu.CompilerParams(collective_id=1, has_side_effects=True, vmem_limit_bytes=48 * 2**20),
        name="tail",
    )(o, w_out, tokens, gain, w_up, w_down)


def per_device(tokens, norm_gain, w_qkv, w_out, post_gain, w_up, w_down):
    rows, width = tokens.shape
    heads = w_qkv.shape[2] // HD
    o, w_out_all = attention(tokens, norm_gain, w_qkv, w_out)
    out = tail(o, w_out_all.reshape(8, heads * HD, width), tokens, post_gain.reshape(width // 128, 128), w_up, w_down)
    return out.reshape(PAD, width)[:rows]


def solution(mesh):
    placed = (
        P("seq", None),
        P(),
        P(None, None, "tensor"),
        P("tensor", None),
        P(),
        P(None, "tensor"),
        P("tensor", None),
    )
    return jax.shard_map(
        per_device, mesh=mesh, in_specs=placed, out_specs=P("seq", None), check_vma=False
    )
```

```python
import functools

import jax
import jax.numpy as jnp
from jax import lax
from jax.experimental import pallas as pl
from jax.experimental.pallas import tpu as pltpu
from jax.sharding import PartitionSpec as P

HD = 48
PAD = 768
WIDE = PAD
MESH = pl.DeviceIdType.MESH
LOG2E = 1.4426950408889634
LIMIT = 2.0**90
FLOOR = 2.0**-20
FULL = pl.BlockSpec(memory_space=pltpu.VMEM)


def layer_norm(values, gain):
    mean = jnp.mean(values, axis=-1, keepdims=True)
    centred = values - mean
    var = jnp.mean(centred * centred, axis=-1, keepdims=True)
    return centred * lax.rsqrt(var + 1e-05) * gain


def wide_row(ref):
    return jnp.concatenate([ref[k : k + 1, :] for k in range(ref.shape[0])], axis=1)


EARLY = [(b, c) for b in (0, 1, 2, 4, 5, 6, 3, 7) for c in range(3)] + [(b, 3) for b in range(8)]


def sweep(rows, queries, keys, vals, acc, probs, early, late):
    def scores(unit, slot):
        b, c = unit
        cols = slice(c * WIDE, (c + 1) * WIDE)
        cut = rows // 32 * 16
        for lo, hi in ((0, cut), (cut, rows)):
            s = jnp.dot(keys[b, lo:hi], queries[:, cols], preferred_element_type=jnp.float32)
            probs[slot, lo:hi, :] = jnp.exp2(s).astype(jnp.bfloat16)

    def product(unit, slot):
        b, c = unit
        cols = slice(c * WIDE, (c + 1) * WIDE)
        acc[:, cols] += jnp.dot(vals[b], probs[slot], preferred_element_type=jnp.float32)

    scores(EARLY[0], 0)
    order = EARLY + [(8, 0)]
    for n, pair in enumerate(EARLY):
        if n + 1 in early:
            early[n + 1]()
        scores(order[n + 1], (n + 1) % 2)
        product(pair, n % 2)

    def body(j, _):
        late(j)
        for c in range(4):
            scores((8 + j, c + 1) if c < 3 else (jnp.minimum(9 + j, 15), 0), (c + 1) % 2)
            product((8 + j, c), c % 2)
        return 0

    lax.fori_loop(0, 8, body, 0)


ORDER = (0, 1, 3, 2)


def load_keys(src, b, keys):
    one = (lax.broadcasted_iota(jnp.int32, (16, PAD), 0) == 0).astype(jnp.float32).astype(jnp.bfloat16)
    keys[b] = jnp.concatenate([src[...], one, jnp.zeros((64, PAD), jnp.bfloat16)], axis=0).T


def load_values(rows, src, b, vals):
    lane = lax.broadcasted_iota(jnp.int32, (16, PAD), 1)
    sub = lax.broadcasted_iota(jnp.int32, (16, PAD), 0)
    vals[b, 0:HD] = src[...]
    vals[b, HD : HD + 16] = ((sub == 0) & (lane < rows)).astype(jnp.float32).astype(jnp.bfloat16)


def load_block(rows, kv, b, keys, vals):
    load_keys(kv.at[0], b, keys)
    load_values(rows, kv.at[1], b, vals)


def attend_kernel(
    tokens, gain, w_in, w_ref, o_ref, totals, land_out, kvx_out, w_all,
    tok, wq, w_own, normed, qkv, land, kvx, queries, keys, vals, probs, acc, send, recv, local,
):
    rows = tok.shape[0]
    width = queries.shape[1]
    seq, me = lax.axis_index("seq"), lax.axis_index("tensor")
    z, y, core = seq // 8, lax.rem(seq // 2, 4), lax.rem(seq, 2)
    links = Links(send, recv)
    fetch = [
        pltpu.make_async_copy(src, dst, local.at[i])
        for i, (src, dst) in enumerate(((tokens, tok), (w_in, wq), (w_ref, w_own)))
    ]
    for copy in fetch:
        copy.start()

    def keep(i):
        src, dst = (
            (w_own, w_all.at[me]),
            (land, land_out),
            (kvx.at[0], kvx_out.at[0]),
            (kvx.at[1], kvx_out.at[1]),
            (kvx.at[2], kvx_out.at[2]),
        )[i]
        return pltpu.make_async_copy(src, dst, local.at[3 + i])


    def on_seq(dz, dy, dc):
        return ((lax.rem(z + dz, 2) * 4 + lax.rem(y + dy, 4)) * 2 + lax.rem(core + dc, 2), me)

    barrier = pltpu.get_barrier_semaphore()
    peers = [on_seq(0, d, 0) for d in (1, 2, 3)] + [on_seq(0, 0, 1), on_seq(1, 0, 0)]
    peers += [(seq, links.slot(1, 0)), (seq, links.slot(0, 1)), (seq, links.slot(0, 3))]
    for peer in peers:
        pl.semaphore_signal(barrier, inc=1, device_id=peer, device_id_type=MESH)

    step = rows // 5
    normed[rows:PAD, :] = jnp.zeros((PAD - rows, normed.shape[1]), jnp.bfloat16)
    fetch[0].wait()

    scale = wide_row(gain)

    def norm_rows(i, _):
        at = pl.ds(pl.multiple_of(i * step, 16), step)
        normed[at, :] = layer_norm(tok[at, :].astype(jnp.float32), scale).astype(jnp.bfloat16)
        return 0

    lax.fori_loop(0, 5, norm_rows, 0)
    fetch[1].wait()
    span = w_in.shape[0] // 3
    wide = lax.dot_general(wq[...], normed[...], (((1,), (1,)), ((), ())), preferred_element_type=jnp.float32)
    for p in range(3):
        part = wide[p * span : (p + 1) * span]
        if p == 0:
            part = part * (LOG2E / HD**0.5)
        qkv[p] = part.astype(jnp.bfloat16).reshape(4, HD, PAD)
    pl.semaphore_wait(barrier, 8)

    by_y = {}

    def send_y(d, lo, hi):
        by_y[d, lo] = links.start(
            lambda: (qkv.at[lo:hi, lax.rem(y + d, 4)], land.at[d, lo:hi], on_seq(0, d, 0))
        )

    for d, lo, hi in ((1, 0, 2), (3, 0, 2), (1, 2, 3), (3, 2, 3), (2, 0, 2), (2, 2, 3)):
        send_y(d, lo, hi)
    to_core, to_far, far_core, more = {}, {}, {}, {}
    to_core[0] = links.start(lambda: (qkv.at[1:3, y], kvx.at[0, 0], on_seq(0, 0, 1)))
    to_far[0] = links.start(lambda: (qkv.at[1:3, y], kvx.at[1, 0], on_seq(1, 0, 0)))

    fetch[2].wait()
    keep(0).start()
    w_cols = w_own.shape[2] // 2

    def tensor_at(dz, dx):
        return (seq, links.slot(dz, dx))

    def own_w(dz, dx):
        return links.start(lambda: (w_own.at[core], w_all.at[me, core], tensor_at(dz, dx)))

    def pass_w(slot, lo, hi, dz, dx):
        def ends():
            ref = w_all.at[links.slot(*slot), core, :, lo * w_cols : hi * w_cols]
            return ref, ref, tensor_at(dz, dx)

        return links.start(ends)

    def swap_w(slot):
        def ends():
            ref = w_all.at[links.slot(*slot), core]
            return ref, ref, on_seq(0, 0, 1)

        return links.start(ends)

    wz, wup, wdown = own_w(1, 0), own_w(0, 1), own_w(0, 3)

    def set_queries(i):
        cols = slice(i * PAD, (i + 1) * PAD)
        queries[0:HD, cols] = land[ORDER[i], 0]
        queries[HD:128, cols] = jnp.zeros((128 - HD, PAD), jnp.bfloat16)
        s = jnp.dot(keys[0, 0:rows], queries[:, cols], preferred_element_type=jnp.float32)
        top = jnp.max(s.reshape(rows // 8, 8, PAD), axis=0)
        top = jnp.max(top, axis=0, keepdims=True)
        first = lax.broadcasted_iota(jnp.int32, (16, PAD), 0) == 0
        shift = jnp.where(first, jnp.broadcast_to(-top, (16, PAD)), 0.0)
        queries[HD : HD + 16, cols] = shift.astype(jnp.bfloat16)

    def arrive(i):
        by_y[ORDER[i], 0].wait_recv()
        load_keys(land.at[ORDER[i], 1], i, keys)
        set_queries(i)

    def arrive_values(i):
        d = ORDER[i]
        by_y[d, 2].wait_recv()
        to_core[d] = links.start(lambda: (land.at[d, 1:3], kvx.at[0, d], on_seq(0, 0, 1)))
        to_far[d] = links.start(lambda: (land.at[d, 1:3], kvx.at[1, d], on_seq(1, 0, 0)))
        load_values(rows, land.at[d, 2], i, vals)

    def take(block):
        group, d = block // 4, ORDER[block % 4]
        if group == 1:
            to_core[d].wait_recv()
        elif group == 2:
            to_far[d].wait_recv()
            far_core[d] = links.start(lambda: (kvx.at[1, d], kvx.at[2, d], on_seq(0, 0, 1)))
        elif group == 3:
            far_core[d].wait_recv()
        load_block(rows, kvx.at[group - 1, d], block, keys, vals)

    others = [(0, 1), (0, 2), (0, 3), (1, 0), (1, 1), (1, 2), (1, 3)]

    def w_first():
        wz.wait_recv()
        more["zup"] = pass_w((1, 0), 0, 2, 0, 1)
        more["zdown"] = pass_w((1, 0), 0, 2, 0, 3)
        wup.wait_recv()
        more["r0"] = pass_w((0, 3), 0, 1, 0, 1)
        wdown.wait_recv()
        more["r1"] = pass_w((0, 1), 1, 2, 0, 3)

    def w_second():
        more["zup"].wait_recv()
        more["q0"] = pass_w((1, 3), 0, 1, 0, 1)
        more["zdown"].wait_recv()
        more["q1"] = pass_w((1, 1), 1, 2, 0, 3)

    def w_third():
        for name in ("r0", "r1", "q0", "q1"):
            more[name].wait_recv()
        for pair in others:
            more[pair] = swap_w(pair)

    def both(*steps):
        def run():
            for function, *args in steps:
                function(*args)

        return run

    def store(i):
        keep(i).start()

    early = {
        1: both((arrive, 1), (arrive, 2)),
        2: both((arrive_values, 1), (arrive_values, 2)),
        9: both((take, 4),),
        12: both((take, 5),),
        15: both((take, 6),),
        18: both((arrive, 3), (arrive_values, 3), (w_first,), (store, 1)),
        21: both((take, 7), (store, 2)),
        32: both((take, 8),),
    }

    def landed(block):
        group, d = block // 4, ORDER[block % 4]
        if group == 2:
            to_far[d].wait_recv()
            far_core[d] = links.start(lambda: (kvx.at[1, d], kvx.at[2, d], on_seq(0, 0, 1)))
        else:
            far_core[d].wait_recv()

    def late(j):
        for k in range(7):

            @pl.when(j == k)
            def _(k=k):
                landed(9 + k)
                if k == 2:
                    store(3)
                if k == 6:
                    store(4)
                if k == 1:
                    w_second()
                if k == 4:
                    w_third()

        block = jnp.minimum(9 + j, 15)
        far = (block >= 12).astype(jnp.int32)
        i = block - 8 - 4 * far
        d = i + (i == 2).astype(jnp.int32) - (i == 3).astype(jnp.int32)
        load_block(rows, kvx.at[1 + far, d], block, keys, vals)

    land[0] = qkv[:, y]
    load_block(rows, land.at[0, 1:3], 0, keys, vals)
    acc[...] = jnp.zeros_like(acc)
    probs[:, rows:PAD, :] = jnp.zeros((2, PAD - rows, WIDE), jnp.bfloat16)
    set_queries(0)
    sweep(rows, queries, keys, vals, acc, probs, early, late)
    attended(acc, o_ref)
    totals[...] = jnp.broadcast_to(acc[HD : HD + 1, :], totals.shape)
    for i in range(5):
        keep(i).wait()
    for pair in others:
        more[pair].wait_recv()
    links.drain()


def attended(sums, o_ref):
    for i, d in enumerate(ORDER):
        cols = slice(i * PAD, (i + 1) * PAD)
        o_ref[d] = (sums[0:HD, cols] / sums[HD : HD + 1, cols]).astype(jnp.bfloat16)


def settle_kernel(
    rows, o_in, totals, land_ref, kvx_ref, o_out, o_new, land, kvx, queries, keys, vals, probs, acc, local
):
    width = totals.shape[1]
    fits = jnp.where((totals[...] < LIMIT) & (totals[...] > FLOOR), 0.0, 1.0)

    @pl.when(jnp.max(fits) > 0.5)
    def _():
        loads = [
            pltpu.make_async_copy(land_ref, land, local.at[0]),
            pltpu.make_async_copy(kvx_ref, kvx, local.at[1]),
        ]
        for load in loads:
            load.start()
        for load in loads:
            load.wait()
        queries[HD:128, :] = jnp.zeros((128 - HD, width), jnp.bfloat16)
        for i, d in enumerate(ORDER):
            queries[0:HD, i * PAD : (i + 1) * PAD] = land[d, 0]
        probs[rows:PAD, :] = jnp.zeros((PAD - rows, 256), jnp.bfloat16)
        acc[...] = jnp.zeros_like(acc)

        def fill(d, _):
            load_block(rows, land.at[d, 1:3], d, keys, vals)
            for g in range(3):
                load_block(rows, kvx.at[g, d], 4 * g + 4 + d, keys, vals)
            return 0

        lax.fori_loop(0, 4, fill, 0)

        def chunk(c, _):
            cols = pl.ds(pl.multiple_of(c * 256, 256), 256)

            def block(b, carry):
                peak, sums = carry
                s = jnp.dot(keys[b, 0:rows], queries[:, cols], preferred_element_type=jnp.float32)
                fresh = jnp.maximum(peak, jnp.max(s, axis=0, keepdims=True))
                probs[0:rows, :] = jnp.exp2(s - fresh).astype(jnp.bfloat16)
                part = jnp.dot(vals[b], probs[...], preferred_element_type=jnp.float32)
                return fresh, sums * jnp.exp2(peak - fresh) + part

            start = (jnp.full((1, 256), -1e30, jnp.float32), jnp.zeros((HD + 16, 256), jnp.float32))
            _, sums = lax.fori_loop(0, 16, block, start)
            acc[:, cols] = sums
            return 0

        lax.fori_loop(0, width // 256, chunk, 0)
        attended(acc, o_new)
        store = pltpu.make_async_copy(o_new, o_out, local.at[2])
        store.start()
        store.wait()


def attention(tokens, gain, w_qkv, w_out):
    rows, features = tokens.shape
    width = 4 * PAD
    bf16 = jnp.bfloat16
    half, cols = w_out.shape[0] // 2, w_out.shape[1]
    n = 48
    tables = [
        pltpu.VMEM((128, width), bf16),
        pltpu.VMEM((16, PAD, 128), bf16),
        pltpu.VMEM((16, HD + 16, PAD), bf16),
    ]
    blocks = [pltpu.VMEM((4, 3, HD, PAD), bf16), pltpu.VMEM((3, 4, 2, HD, PAD), bf16)]
    anywhere = pl.BlockSpec(memory_space=pl.ANY)
    o, totals, land, kvx, w_all = pl.pallas_call(
        attend_kernel,
        out_shape=(
            jax.ShapeDtypeStruct((4, HD, PAD), bf16),
            jax.ShapeDtypeStruct((8, width), jnp.float32),
            jax.ShapeDtypeStruct((4, 3, HD, PAD), bf16),
            jax.ShapeDtypeStruct((3, 4, 2, HD, PAD), bf16),
            jax.ShapeDtypeStruct((8, 2, half, cols), bf16),
        ),
        in_specs=[anywhere, FULL, anywhere, anywhere],
        out_specs=(FULL, FULL, anywhere, anywhere, anywhere),
        scratch_shapes=[
            pltpu.VMEM(tokens.shape, bf16),
            pltpu.VMEM((3 * w_qkv.shape[2], features), bf16),
            pltpu.VMEM((2, half, cols), bf16),
            pltpu.VMEM((PAD, features), bf16),
            pltpu.VMEM((3, 4, HD, PAD), bf16),
        ]
        + blocks
        + tables
        + [
            pltpu.VMEM((2, PAD, WIDE), bf16),
            pltpu.VMEM((HD + 16, width), jnp.float32),
            pltpu.SemaphoreType.DMA((n,)),
            pltpu.SemaphoreType.DMA((n,)),
            pltpu.SemaphoreType.DMA((8,)),
        ],
        compiler_params=pltpu.CompilerParams(collective_id=0, has_side_effects=True, vmem_limit_bytes=54 * 2**20),
        name="attend",
    )(
        tokens,
        gain.reshape(features // 128, 128),
        jnp.transpose(w_qkv, (1, 2, 0)).reshape(3 * w_qkv.shape[2], features),
        w_out.reshape(2, half, cols),
    )
    o = pl.pallas_call(
        functools.partial(settle_kernel, rows),
        out_shape=jax.ShapeDtypeStruct((4, HD, PAD), bf16),
        in_specs=[anywhere, FULL, anywhere, anywhere],
        out_specs=anywhere,
        input_output_aliases={0: 0},
        scratch_shapes=[pltpu.VMEM((4, HD, PAD), bf16)]
        + blocks
        + tables
        + [
            pltpu.VMEM((PAD, 256), bf16),
            pltpu.VMEM((HD + 16, width), jnp.float32),
            pltpu.SemaphoreType.DMA((3,)),
        ],
        compiler_params=pltpu.CompilerParams(vmem_limit_bytes=61 * 2**20),
        name="settle",
    )(o, totals, land, kvx)
    return o, w_all.reshape(16 * half, cols)


class Links:
    def __init__(self, send, recv):
        me = lax.axis_index("tensor")
        self.seq = lax.axis_index("seq")
        self.z, self.x = me // 4, lax.rem(me, 4)
        self.me = me
        self.send, self.recv = send, recv
        self.count = 0
        self.open = []

    def slot(self, dz, dx):
        z = lax.rem(self.z + dz, 2)
        return z * 4 + lax.rem(self.x + dx, 4)

    def barrier(self, more=0):
        sem = pltpu.get_barrier_semaphore()
        for dz, dx in ((1, 0), (0, 1), (0, 3)):
            pl.semaphore_signal(sem, inc=1, device_id=(self.seq, self.slot(dz, dx)), device_id_type=MESH)
        pl.semaphore_wait(sem, 3 + more)

    def put(self, src, dst, dz, dx):
        device = (self.seq, self.slot(dz, dx))
        return self.start(lambda: (src, dst, device))

    def start(self, ends):
        copy = Copy(self, self.count, ends)
        self.count += 1
        self.open.append(copy)
        copy.make().start()
        return copy

    def drain(self):
        for copy in self.open:
            copy.make().wait_send()
        self.open = []


class Copy:
    def __init__(self, links, index, ends):
        self.links, self.index, self.ends = links, index, ends

    def make(self):
        src, dst, device = self.ends()
        return pltpu.make_async_remote_copy(
            src_ref=src,
            dst_ref=dst,
            send_sem=self.links.send.at[self.index],
            recv_sem=self.links.recv.at[self.index],
            device_id=device,
            device_id_type=MESH,
        )

    def wait_recv(self):
        self.make().wait_recv()


def gather_tensor(links, piece, ready=lambda dz, dx: None, between=lambda: None):
    s = links.slot
    put = links.put

    def pass_on(slot, lo, hi, dz, dx):
        ref = piece(slot, lo, hi)
        return put(ref, ref, dz, dx)

    me = s(0, 0)
    b_up = pass_on(me, 2, 4, 0, 1)
    b_down = pass_on(me, 2, 4, 0, 3)
    between()
    a_z = pass_on(me, 0, 2, 1, 0)
    b_z = pass_on(me, 2, 4, 1, 0)
    a_up = pass_on(me, 0, 2, 0, 1)
    a_down = pass_on(me, 0, 2, 0, 3)
    ready(0, 0)
    b_up.wait_recv()
    r2 = pass_on(s(0, 3), 2, 3, 0, 1)
    bz_lo = pass_on(s(0, 3), 2, 4, 1, 0)
    b_down.wait_recv()
    r3 = pass_on(s(0, 1), 3, 4, 0, 3)
    bz_hi = pass_on(s(0, 1), 2, 4, 1, 0)
    a_z.wait_recv()
    az_up = pass_on(s(1, 0), 0, 2, 0, 1)
    az_down = pass_on(s(1, 0), 0, 2, 0, 3)
    a_up.wait_recv()
    r0 = pass_on(s(0, 3), 0, 1, 0, 1)
    a_down.wait_recv()
    r1 = pass_on(s(0, 1), 1, 2, 0, 3)
    ready(0, 3)
    r2.wait_recv()
    bz_2 = pass_on(s(0, 2), 2, 3, 1, 0)
    r3.wait_recv()
    bz_3 = pass_on(s(0, 2), 3, 4, 1, 0)
    ready(0, 1)
    az_up.wait_recv()
    q0 = pass_on(s(1, 3), 0, 1, 0, 1)
    az_down.wait_recv()
    q1 = pass_on(s(1, 1), 1, 2, 0, 3)
    b_z.wait_recv()
    ready(1, 0)
    r0.wait_recv()
    r1.wait_recv()
    ready(0, 2)
    bz_lo.wait_recv()
    ready(1, 3)
    bz_hi.wait_recv()
    ready(1, 1)
    for copy in (bz_2, bz_3, q0, q1):
        copy.wait_recv()
    ready(1, 2)
    links.drain()


GATHER_COPIES = 18


def cuts(cols):
    return [cols // 12 * k for k in (0, 3, 6, 9, 12)]


def reduce_tensor(links, term, stage, rows, cols, make):
    at = cuts(cols)
    s = links.slot
    put = links.put

    def q(slot, lo, hi):
        return term.at[slot, :, at[lo] : at[hi]]

    def val(slot, lo, hi):
        return term[slot, :, at[lo] : at[hi]].astype(jnp.float32)

    def land(i, lo, hi):
        return stage.at[i, :, 0 : at[hi] - at[lo]]

    def got(i, base, lo, hi):
        return stage[i, :, at[lo] - at[base] : at[hi] - at[base]].astype(jnp.float32)

    def add_into(slot, lo, hi, *parts):
        total = val(slot, lo, hi)
        for part in parts:
            total = total + part
        term[slot, :, at[lo] : at[hi]] = total.astype(jnp.bfloat16)

    zb, fa, near = {}, {}, {}

    def cross(i, dx):
        zb[dx] = put(q(s(1, dx), 2, 4), land(i, 2, 4), 1, 0)

    def far(j, dz):
        fa[dz, 0] = put(q(s(dz, 2), 0, 1), land(4 + j, 0, 1), 0, 3)
        fa[dz, 1] = put(q(s(dz, 2), 1, 2), land(6 + j, 1, 2), 0, 1)

    def relay(j, dz):
        fa[dz, 0].wait_recv()
        add_into(s(dz, 3), 0, 1, got(4 + j, 0, 0, 1))
        near[dz, 3] = put(q(s(dz, 3), 0, 2), land(8 + j, 0, 2), 0, 3)
        fa[dz, 1].wait_recv()
        add_into(s(dz, 1), 1, 2, got(6 + j, 1, 1, 2))
        near[dz, 1] = put(q(s(dz, 1), 0, 2), land(10 + j, 0, 2), 0, 1)

    make((1, 2), (0, 2))
    cross(0, 2)
    far(0, 1)
    far(1, 0)
    make((1, 1), (1, 3))
    cross(1, 1)
    cross(2, 3)
    relay(0, 1)
    make((0, 1), (0, 3))
    relay(1, 0)
    zb[2].wait_recv()
    add_into(s(0, 2), 2, 4, got(0, 2, 2, 4))
    fb0 = put(q(s(0, 2), 2, 3), land(12, 2, 3), 0, 3)
    fb1 = put(q(s(0, 2), 3, 4), land(13, 3, 4), 0, 1)
    make((1, 0), (0, 0))
    cross(3, 0)
    zb[1].wait_recv()
    zb[3].wait_recv()
    near[1, 3].wait_recv()
    near[1, 1].wait_recv()
    add_into(s(1, 0), 0, 2, got(8, 0, 0, 2), got(10, 0, 0, 2))
    za = put(q(s(1, 0), 0, 2), land(14, 0, 2), 1, 0)
    fb0.wait_recv()
    add_into(s(0, 3), 2, 3, got(2, 2, 2, 3), got(12, 2, 2, 3))
    add_into(s(0, 3), 3, 4, got(2, 2, 3, 4))
    nb3 = put(q(s(0, 3), 2, 4), land(15, 2, 4), 0, 3)
    fb1.wait_recv()
    add_into(s(0, 1), 3, 4, got(1, 2, 3, 4), got(13, 3, 3, 4))
    add_into(s(0, 1), 2, 3, got(1, 2, 2, 3))
    nb1 = put(q(s(0, 1), 2, 4), land(16, 2, 4), 0, 1)
    zb[0].wait_recv()
    nb3.wait_recv()
    nb1.wait_recv()
    second = val(s(0, 0), 2, 4) + got(3, 2, 2, 4) + got(15, 2, 2, 4) + got(16, 2, 2, 4)

    def first():
        near[0, 3].wait_recv()
        near[0, 1].wait_recv()
        za.wait_recv()
        return val(s(0, 0), 0, 2) + got(9, 0, 0, 2) + got(11, 0, 0, 2) + got(14, 0, 0, 2)

    return first, second


def tail_kernel(
    o_ref, w_out, tokens, gain, w_up, w_down, out_ref, every, mixed, post, term, stage, tok, wo, wu, wd, send, recv, local
):
    links = Links(send, recv)
    seq, me = links.seq, links.me
    y = lax.rem(seq // 2, 4)
    share, width = out_ref.shape[1], out_ref.shape[2]
    cut = cuts(width)
    rows = tok.shape[0]
    loads = [
        pltpu.make_async_copy(src, dst, local.at[i])
        for i, (src, dst) in enumerate(((tokens, tok), (w_out, wo), (w_up, wu), (w_down, wd)))
    ]
    for load in loads:
        load.start()

    def at_y(dy):
        return ((seq // 8 * 4 + lax.rem(y + dy, 4)) * 2 + lax.rem(seq, 2), me)

    sem = pltpu.get_barrier_semaphore()
    for d in (1, 2, 3):
        pl.semaphore_signal(sem, inc=1, device_id=at_y(d), device_id_type=MESH)
    links.barrier(3)
    back = [links.start(lambda d=d: (o_ref.at[d], every.at[me, y], at_y(4 - d))) for d in (2, 1, 3)]
    every[me, y] = o_ref[0]
    loads[0].wait()
    mixed[0:rows, :] = tok[...].astype(jnp.float32)
    mixed[rows:, :] = jnp.zeros((PAD - rows, width), jnp.float32)
    loads[1].wait()
    for copy in back:
        copy.wait_recv()

    def project(dz, dx):
        slot = links.slot(dz, dx)

        def tile(i, _):
            at = pl.ds(pl.multiple_of(i * 256, 256), 256)
            left = every[slot, :, :, at].reshape(4 * HD, 256)
            mixed[at, :] += lax.dot_general(
                left, wo[slot], (((0,), (0,)), ((), ())), preferred_element_type=jnp.float32
            )
            return 0

        lax.fori_loop(0, PAD // 256, tile, 0)

    gather_tensor(links, lambda slot, lo, hi: every.at[slot, lo:hi], project)
    loads[2].wait()
    loads[3].wait()

    scale = wide_row(gain)

    def feed_forward(*pair):
        slots = [links.slot(*block) for block in pair]
        for k, slot in enumerate(slots):
            at = pl.ds(pl.multiple_of(slot * share, 32), share)
            post[k * share : (k + 1) * share, :] = layer_norm(mixed[at, :], scale).astype(jnp.bfloat16)
        up = jnp.dot(post[...], wu[...], preferred_element_type=jnp.float32)
        hidden = jax.nn.gelu(up, approximate=True).astype(jnp.bfloat16)
        for k in range(3):
            cols = slice(k * (width // 3), (k + 1) * (width // 3))
            down = jnp.dot(hidden, wd[:, cols], preferred_element_type=jnp.float32).astype(jnp.bfloat16)
            for i, slot in enumerate(slots):
                term[slot, :, cols] = down[i * share : (i + 1) * share]

    first, second = reduce_tensor(links, term, stage, share, width, feed_forward)
    at = pl.ds(pl.multiple_of(me * share, 32), share)
    out_ref[me, :, cut[2] :] = (mixed[at, cut[2] :] + second).astype(jnp.bfloat16)

    def rest():
        out_ref[me, :, 0 : cut[2]] = (mixed[at, 0 : cut[2]] + first()).astype(jnp.bfloat16)

    gather_tensor(links, lambda slot, lo, hi: out_ref.at[slot, :, cut[lo] : cut[hi]], between=rest)


def tail(o, w_out, tokens, gain, w_up, w_down):
    rows, cols = tokens.shape
    share = PAD // 8
    copies = 64
    bf16 = jnp.bfloat16
    anywhere = pl.BlockSpec(memory_space=pl.ANY)
    return pl.pallas_call(
        tail_kernel,
        out_shape=jax.ShapeDtypeStruct((8, share, cols), bf16),
        in_specs=[FULL, anywhere, anywhere, FULL, anywhere, anywhere],
        out_specs=FULL,
        scratch_shapes=[
            pltpu.VMEM((8,) + o.shape, bf16),
            pltpu.VMEM((PAD, cols), jnp.float32),
            pltpu.VMEM((2 * share, cols), bf16),
            pltpu.VMEM((8, share, cols), bf16),
            pltpu.VMEM((17, share, cols // 2), bf16),
            pltpu.VMEM(tokens.shape, bf16),
            pltpu.VMEM(w_out.shape, bf16),
            pltpu.VMEM(w_up.shape, bf16),
            pltpu.VMEM(w_down.shape, bf16),
            pltpu.SemaphoreType.DMA((copies,)),
            pltpu.SemaphoreType.DMA((copies,)),
            pltpu.SemaphoreType.DMA((4,)),
        ],
        compiler_params=pltpu.CompilerParams(collective_id=1, has_side_effects=True, vmem_limit_bytes=48 * 2**20),
        name="tail",
    )(o, w_out, tokens, gain, w_up, w_down)


def per_device(tokens, norm_gain, w_qkv, w_out, post_gain, w_up, w_down):
    rows, width = tokens.shape
    heads = w_qkv.shape[2] // HD
    o, w_out_all = attention(tokens, norm_gain, w_qkv, w_out)
    out = tail(o, w_out_all.reshape(8, heads * HD, width), tokens, post_gain.reshape(width // 128, 128), w_up, w_down)
    return out.reshape(PAD, width)[:rows]


def solution(mesh):
    placed = (
        P("seq", None),
        P(),
        P(None, None, "tensor"),
        P("tensor", None),
        P(),
        P(None, "tensor"),
        P("tensor", None),
    )
    return jax.shard_map(
        per_device, mesh=mesh, in_specs=placed, out_specs=P("seq", None), check_vma=False
    )
```
